32 devices in a mesh: dp: 2 (over y), fsdp: 16 (over z, x, core).
Axes of the slice: x: 2, y: 2, z: 4, core: 2. Of those that a mesh axis runs over, the one named last changes fastest.
Arguments:
- queries: bfloat16 [6144, 2560], P(('dp', 'fsdp')), may hold values from -8 to 8
- keys: bfloat16 [6144, 2560], P(('dp', 'fsdp')), may hold values from -8 to 8
- values: bfloat16 [6144, 2560], P(('dp', 'fsdp')), may hold values from -6 to 6
- lengths: int32 [16, 2, 4], P('fsdp'), may hold values from 0 to 192, as said below
- normalized_weight: bfloat16 [2560, 5120], P(None, 'fsdp'), may hold values from -1 to 1
- block_scale_codes: int32 [40, 5120], P(None, 'fsdp'), may hold values from 0 to 255
- scale_group_factor: float32 [5, 5120], P(None, 'fsdp'), may hold values from 0.01 to 0.03
- scale_group_offset: float32 [5, 5120], P(None, 'fsdp'), may hold values from 0.005 to 0.015
- adapter_down_weight: bfloat16 [64, 2560], P(None, 'fsdp'), may hold values from -0.125 to 0.125
- adapter_up_weight: bfloat16 [64, 5120], P(None, 'fsdp'), may hold values from -0.75 to 0.75
- cotangent: bfloat16 [6144, 5120], P(('dp', 'fsdp')), may hold values from -6 to 6
Outputs:
- projection_output: bfloat16 [6144, 5120], P(('dp', 'fsdp'))
- attention_gradient: bfloat16 [6144, 2560], P(('dp', 'fsdp'))
- down_grad: float32 [64, 2560], P(None, 'fsdp')
- adapter_up_gradient: float32 [64, 5120], P(None, 'fsdp')
The draws below stay inside these ranges and needn't reach their ends.
Inputs may be any that keep to these rules, and one draw needn't show every extreme that they name: The 4 lengths of each block sum to 192; zero lengths, if any, come last; some block is a single document of 192 tokens.
All inputs are finite; a program needn't handle non-finite values.
Results may differ from the reference program's by a relative error of at most 0.0059.
Values may be sent and summed in bfloat16 or wider, within the bound.
A program may use at most 192 MiB of HBM per device.

```python
import math
import jax
import jax.numpy as jnp
from jax import lax

MODEL_WIDTH = 5120
HEADS = 20
HEAD_SIZE = 128
ADAPTER_RANK = 64
QBLOCK = 64
SCALE_GROUP = 8
DOCS = 4
TOK_DEV = 192
HEAD_FEATURES = 2560
TOKENS = 6144
N_DP = 2
N_FSDP = 16


def draw_queries(key, part):
    noise = jax.random.normal(jax.random.fold_in(key, 11), (TOKENS, HEADS, HEAD_SIZE), jnp.float32)
    result = jnp.clip(noise, -6.0, 6.0)
    return result.reshape(TOKENS, HEAD_FEATURES).astype(jnp.bfloat16)


def draw_keys(key, part):
    noise = jax.random.normal(jax.random.fold_in(key, 12), (TOKENS, HEADS, HEAD_SIZE), jnp.float32)
    result = jnp.clip(noise, -6.0, 6.0)
    return result.reshape(TOKENS, HEAD_FEATURES).astype(jnp.bfloat16)


def draw_lengths(key, part):
    blocks = N_FSDP * N_DP
    doc_count = jax.random.randint(jax.random.fold_in(key, 21), (blocks,), 1, DOCS + 1)
    single = jax.random.randint(jax.random.fold_in(key, 22), (), 0, blocks)
    doc_count = jnp.where(jnp.arange(blocks) == single, 1, doc_count)
    scores = jax.random.randint(jax.random.fold_in(key, 23), (blocks, TOK_DEV - 1), 0, 2 ** 20) * TOK_DEV + jnp.arange(1, TOK_DEV, dtype=jnp.int32)[None, :]
    order = jnp.argsort(scores, axis=-1)
    picks = order[:, :DOCS - 1].astype(jnp.int32) + 1
    usable = jnp.arange(DOCS - 1, dtype=jnp.int32)[None, :] < doc_count[:, None] - 1
    cuts = jnp.sort(jnp.where(usable, picks, TOK_DEV), axis=-1)
    edges = jnp.concatenate([jnp.zeros((blocks, 1), jnp.int32), cuts.astype(jnp.int32), jnp.full((blocks, 1), TOK_DEV, jnp.int32)], axis=1)
    doc_lengths = edges[:, 1:] - edges[:, :-1]
    return doc_lengths.reshape(N_FSDP, N_DP, DOCS).astype(jnp.int32)


def set_ends(values, stream_key, least, largest):
    dims = values.shape
    place = [jax.random.randint(jax.random.fold_in(stream_key, axis), (), 0, dims[axis]) for axis in range(len(dims))]
    values = values.at[tuple(place)].set(least)
    longest = dims.index(max(dims))
    place[longest] = (place[longest] + 1) % dims[longest]
    return values.at[tuple(place)].set(largest)


def strengthened(entries, key, source, target, shards_of, factor):
    owner, partner = [(jnp.arange(entries.shape[dim]) // (entries.shape[dim] // shards_of)).reshape([-1 if axis == dim else 1 for axis in range(entries.ndim)]) for dim in (source, target)]
    chosen = jax.random.permutation(key, shards_of)[partner]
    strong = (owner == chosen) | (owner == (partner + shards_of // 2) % shards_of)
    return jnp.where(strong, factor * entries, entries)


def shard_levels(key, shape, split, smallest, largest):
    level = 1.0
    for dim, blocks in split:
        heights = jax.random.uniform(jax.random.fold_in(jax.random.fold_in(key, 6), dim), (blocks,), jnp.float32, smallest / len(split), largest / len(split))
        level = level * jnp.repeat(jnp.exp(heights), shape[dim] // blocks).reshape((-1,) + (1,) * (len(shape) - 1 - dim))
    return level


def scatter_about(own_key, shape, deviation, bound, split=(), kind=jnp.bfloat16):
    level = shard_levels(own_key, shape, split, -0.22, 0.18) if split else 1.0
    drawn = jax.random.normal(own_key, shape, jnp.float32) * deviation * level
    return jnp.minimum(jnp.maximum(drawn, -bound), bound).astype(kind)


def bell_draw_with(rng, extent, width, most, cuts, heavy, kind=jnp.bfloat16):
    array = width * jax.random.normal(rng, extent, jnp.float32)
    if cuts:
        array = array * shard_levels(rng, extent, cuts, -0.22, 0.18)
    return jnp.clip(strengthened(array, jax.random.fold_in(rng, 3), *heavy), -most, most).astype(kind)


def setup_inputs(seed: int = 0) -> dict:
    key_list = jax.random.split(jax.random.key(seed), 12)
    return {
        "queries": draw_queries(jax.random.fold_in(key_list[11], 71), 0),
        "keys": draw_keys(jax.random.fold_in(key_list[11], 71), 0),
        "values": scatter_about(key_list[2], (TOKENS, HEAD_FEATURES), 1.0, 6.0, ((0, 32),)),
        "lengths": draw_lengths(jax.random.fold_in(key_list[11], 71), 0),
        "normalized_weight": jnp.clip(jax.random.uniform(key_list[4], (HEAD_FEATURES, MODEL_WIDTH), jnp.float32, -1.0, 1.0) * shard_levels(key_list[4], (HEAD_FEATURES, MODEL_WIDTH), ((1, 16),), -0.4, 0.0), -1.0, 1.0).astype(jnp.bfloat16),
        "block_scale_codes": set_ends(jax.random.randint(key_list[5], (HEAD_FEATURES // QBLOCK, MODEL_WIDTH), 0, 256), jax.random.fold_in(key_list[5], 1), 0, 255).astype(jnp.int32),
        "scale_group_factor": jnp.clip(jnp.exp(math.log(0.03) - 1.0986123 * jax.random.uniform(key_list[6], (HEAD_FEATURES // (QBLOCK * SCALE_GROUP), MODEL_WIDTH), jnp.float32) ** shard_levels(key_list[6], (HEAD_FEATURES // (QBLOCK * SCALE_GROUP), MODEL_WIDTH), ((1, 16),), -0.2, 0.2)), 0.01, 0.03),
        "scale_group_offset": jnp.clip(jnp.exp(math.log(0.015) - 1.0986123 * jax.random.uniform(key_list[7], (HEAD_FEATURES // (QBLOCK * SCALE_GROUP), MODEL_WIDTH), jnp.float32) ** shard_levels(key_list[7], (HEAD_FEATURES // (QBLOCK * SCALE_GROUP), MODEL_WIDTH), ((1, 16),), -0.2, 0.2)), 0.005, 0.015),
        "adapter_down_weight": scatter_about(key_list[8], (ADAPTER_RANK, HEAD_FEATURES), HEAD_FEATURES ** -0.5, 0.125, ((1, 16),)),
        "adapter_up_weight": scatter_about(key_list[9], (ADAPTER_RANK, MODEL_WIDTH), ADAPTER_RANK ** -0.5, 0.75, ((1, 16),)),
        "cotangent": bell_draw_with(key_list[10], (TOKENS, MODEL_WIDTH), 1.0, 6.0, ((0, 32),), (0, 1, 32, 2.75)),
    }


adapter_scale = 0.25


def dequantize(normalized_weight, block_scale_codes, scale_group_factor, scale_group_offset):
    spread_scale = jnp.repeat(scale_group_factor, SCALE_GROUP, axis=0)
    spread_offset = jnp.repeat(scale_group_offset, SCALE_GROUP, axis=0)
    absmax = spread_scale * (block_scale_codes.astype(jnp.float32) + 1.0) / 256.0 + spread_offset
    return (normalized_weight.astype(jnp.float32) * jnp.repeat(absmax, QBLOCK, axis=0)).astype(jnp.bfloat16)


def attend_block(operands):
    queries, keys, values, doc_lengths = operands
    doc_ends = jnp.cumsum(doc_lengths)
    places = jnp.arange(TOK_DEV, dtype=jnp.int32)
    segment = jnp.sum((doc_ends[None, :] <= places[:, None]).astype(jnp.int32), axis=1)
    allowed = (segment[:, None] == segment[None, :]) & (places[None, :] <= places[:, None])
    query_heads = queries.reshape(TOK_DEV, HEADS, HEAD_SIZE).astype(jnp.float32)
    key_heads = keys.reshape(TOK_DEV, HEADS, HEAD_SIZE).astype(jnp.float32)
    value_heads = values.reshape(TOK_DEV, HEADS, HEAD_SIZE).astype(jnp.float32)
    scores = jnp.einsum("qhe,khe->hqk", query_heads, key_heads) * (HEAD_SIZE ** -0.5)
    scores = jnp.where(allowed[None], scores, -jnp.inf)
    row_max = jnp.max(scores, axis=-1, keepdims=True)
    weights = jnp.exp(scores - row_max)
    total = jnp.sum(weights, axis=-1)
    rounded = lax.optimization_barrier(weights.astype(jnp.bfloat16)).astype(jnp.float32)
    mixed = jnp.einsum("hqk,khe->qhe", rounded, value_heads) / jnp.transpose(total)[:, :, None]
    return mixed.astype(jnp.bfloat16).reshape(TOK_DEV, HEAD_FEATURES)


def reference(queries, keys, values, lengths, normalized_weight, block_scale_codes, scale_group_factor, scale_group_offset, adapter_down_weight, adapter_up_weight, cotangent):
    blocks = N_DP * N_FSDP
    block_lengths = jnp.transpose(lengths, (1, 0, 2)).reshape(blocks, DOCS)
    attention_output = lax.map(attend_block, (queries.reshape(blocks, TOK_DEV, HEAD_FEATURES), keys.reshape(blocks, TOK_DEV, HEAD_FEATURES), values.reshape(blocks, TOK_DEV, HEAD_FEATURES), block_lengths))
    attention_output = attention_output.reshape(TOKENS, HEAD_FEATURES)
    frozen_output = dequantize(normalized_weight, block_scale_codes, scale_group_factor, scale_group_offset)
    reduced_activation = jnp.dot(attention_output, adapter_down_weight.T, preferred_element_type=jnp.float32).astype(jnp.bfloat16)
    projection_output = (jnp.dot(attention_output, frozen_output, preferred_element_type=jnp.float32) + adapter_scale * jnp.dot(reduced_activation, adapter_up_weight, preferred_element_type=jnp.float32)).astype(jnp.bfloat16)
    reduced_gradient = (adapter_scale * jnp.dot(cotangent, adapter_up_weight.T, preferred_element_type=jnp.float32)).astype(jnp.bfloat16)
    attention_gradient = (jnp.dot(cotangent, frozen_output.T, preferred_element_type=jnp.float32) + jnp.dot(reduced_gradient, adapter_down_weight, preferred_element_type=jnp.float32)).astype(jnp.bfloat16)
    down_grad = jnp.dot(reduced_gradient.T, attention_output, preferred_element_type=jnp.float32)
    adapter_up_gradient = adapter_scale * jnp.dot(reduced_activation.T, cotangent, preferred_element_type=jnp.float32)
    return projection_output, attention_gradient, down_grad, adapter_up_gradient
```

```python
import functools

import jax
import jax.numpy as jnp
from jax import lax
from jax.experimental import pallas as pl
from jax.experimental.pallas import tpu as pltpu
from jax.sharding import PartitionSpec as P

HEAD_SIZE = 128
QBLOCK = 64
SCALE_GROUP = 8


adapter_scale = 0.25


def dequantize_kernel(weight, absmax, out):
    rows, features = out.shape
    lane = lax.broadcasted_iota(jnp.int32, (rows, 2 * QBLOCK), 1)
    for i in range(features // (2 * QBLOCK)):
        columns = slice(2 * QBLOCK * i, 2 * QBLOCK * (i + 1))
        scale = jnp.where(
            lane < QBLOCK, absmax[:, 2 * i : 2 * i + 1], absmax[:, 2 * i + 1 : 2 * i + 2]
        )
        out[:, columns] = (weight[:, columns].astype(jnp.float32) * scale).astype(out.dtype)


def dequantize(normalized_weight, block_scale_codes, scale_group_factor, scale_group_offset):
    spread_scale = jnp.repeat(scale_group_factor, SCALE_GROUP, axis=0)
    spread_offset = jnp.repeat(scale_group_offset, SCALE_GROUP, axis=0)
    absmax = spread_scale * (block_scale_codes.astype(jnp.float32) + 1.0) / 256.0 + spread_offset
    weight = normalized_weight.T
    return pl.pallas_call(
        dequantize_kernel,
        out_shape=jax.ShapeDtypeStruct(weight.shape, jnp.bfloat16),
        compiler_params=pltpu.CompilerParams(vmem_limit_bytes=16 * 2**20),
    )(weight, absmax.T)


def attend(queries, keys, values, doc_lengths):
    tokens = queries.shape[0]
    head_count = queries.shape[1] // HEAD_SIZE
    query_heads = queries.reshape(tokens, head_count, HEAD_SIZE)
    key_heads = keys.reshape(tokens, head_count, HEAD_SIZE)
    value_heads = values.reshape(tokens, head_count, HEAD_SIZE)
    doc_ends = jnp.cumsum(doc_lengths)
    places = jnp.arange(tokens, dtype=jnp.int32)
    segment = jnp.sum((doc_ends[None, :] <= places[:, None]).astype(jnp.int32), axis=1)
    allowed = (segment[:, None] == segment[None, :]) & (places[None, :] <= places[:, None])
    scores = jnp.einsum(
        "qhe,khe->hqk", query_heads, key_heads, preferred_element_type=jnp.float32
    ) * HEAD_SIZE ** (-0.5)
    scores = jnp.where(allowed[None], scores, -jnp.inf)
    row_max = jnp.max(scores, axis=-1, keepdims=True)
    weights = jnp.exp(scores - row_max)
    total = jnp.sum(weights, axis=-1)
    summed = jnp.einsum(
        "hqk,khe->qhe",
        weights.astype(jnp.bfloat16),
        value_heads,
        preferred_element_type=jnp.float32,
    )
    return (
        (summed / jnp.transpose(total)[:, :, None])
        .astype(jnp.bfloat16)
        .reshape(tokens, head_count * HEAD_SIZE)
    )


MESH = pl.DeviceIdType.MESH


def ring_kernel(scatter, third, *refs):
    if scatter:
        block, parts, out, mine, sems, ring_send, ring_recv, row_send, row_recv = refs[:9]
        core_send, core_recv, part_send, part_recv = refs[9:]
    else:
        block, out, sems, ring_send, ring_recv, row_send, row_recv, core_send, core_recv = refs
    n = lax.axis_size("fsdp")
    chips = n // 2
    half = chips // 2
    row = lax.axis_index("dp")
    me = lax.axis_index("fsdp")
    chip, core = me // 2, me % 2
    place = jnp.where(chip % 2 == 0, chip // 2, chips - 1 - chip // 2)

    def device_at(where):
        where = (where + chips) % chips
        there = jnp.where(where < half, 2 * where, 2 * (chips - 1 - where) + 1)
        return 2 * there + core

    neighbour = (device_at(place + 1), device_at(place - 1))
    twin = 2 * chip + 1 - core
    other_row = row + 1 - 2 * (row % 2)
    parity = row % 2
    size = block.shape[0]
    own = (pl.ds(pl.multiple_of(parity * third, 16), third))
    others = (pl.ds(pl.multiple_of((1 - parity) * third, 16), third))
    rest = pl.ds(2 * third, size - 2 * third)
    segments = (own, rest)

    barrier = pltpu.get_barrier_semaphore()
    if scatter:
        for k in range(1, n):
            pl.semaphore_signal(barrier, inc=1, device_id={"fsdp": (me + k) % n}, device_id_type=MESH)
        pl.semaphore_signal(barrier, inc=1, device_id={"dp": other_row}, device_id_type=MESH)
        pl.semaphore_wait(barrier, n)
    else:
        for peer in (*neighbour, twin):
            pl.semaphore_signal(barrier, inc=1, device_id={"fsdp": peer}, device_id_type=MESH)
        pl.semaphore_signal(barrier, inc=1, device_id={"dp": other_row}, device_id_type=MESH)
        pl.semaphore_wait(barrier, 4)

    sent = []

    def send(src, dst, send_sem, recv_sem, target):
        copy = pltpu.make_async_remote_copy(
            src_ref=src, dst_ref=dst, send_sem=send_sem, recv_sem=recv_sem,
            device_id=target, device_id_type=MESH,
        )
        copy.start()
        sent.append(copy)

    def arrived(dst, recv_sem, send_sem):
        pltpu.make_async_remote_copy(
            src_ref=dst, dst_ref=dst, send_sem=send_sem, recv_sem=recv_sem,
            device_id={"fsdp": twin}, device_id_type=MESH,
        ).wait_recv()

    hops = ((half, half - 1), (half - 1, half))

    def ring(src, origin, way, seg, step):
        send(
            src, out.at[origin, segments[seg]], ring_send.at[way, seg, step],
            ring_recv.at[way, seg, step], {"fsdp": neighbour[way]},
        )

    for seg in range(2):
        for way in range(2):
            if hops[way][seg] >= 1:
                ring(block.at[segments[seg]], me, way, seg, 0)
    send(block, out.at[me], core_send.at[0, 0, 2], core_recv.at[0, 0, 2], {"fsdp": twin})
    if scatter:
        for k in range(1, n):
            to = (me + k) % n
            send(parts.at[to], mine.at[me], part_send.at[k], part_recv.at[k], {"fsdp": to})
    keep = pltpu.make_async_copy(block, out.at[me], sems.at[0])
    keep.start()
    if scatter:
        keep_part = pltpu.make_async_copy(parts.at[me], mine.at[me], sems.at[1])
        keep_part.start()

    def origin_of(way, step):
        return device_at(place - step if way == 0 else place + step)

    def to_twin(origin, rows, way, step, kind):
        send(
            out.at[origin, rows], out.at[origin, rows], core_send.at[way, step, kind],
            core_recv.at[way, step, kind], {"fsdp": twin},
        )

    def from_row(way, step):
        origin = origin_of(way, step)
        arrived(out.at[origin, others], row_recv.at[way, step], row_send.at[way, step])
        to_twin(origin, others, way, step, 2)

    for step in range(1, half + 1):
        for seg in range(2):
            for way in range(2):
                if step <= hops[way][seg]:
                    origin = origin_of(way, step)
                    rows = segments[seg]
                    view = out.at[origin, rows]
                    arrived(view, ring_recv.at[way, seg, step - 1], ring_send.at[way, seg, step - 1])
                    if step < hops[way][seg]:
                        ring(view, origin, way, seg, step)
                    if seg == 0:
                        send(
                            view, view, row_send.at[way, step], row_recv.at[way, step],
                            {"dp": other_row},
                        )
                    to_twin(origin, rows, way, step, seg)
        for way in range(2):
            if 1 <= step - 1 <= hops[way][0]:
                from_row(way, step - 1)
    for way in range(2):
        if 1 <= half <= hops[way][0]:
            from_row(way, half)

    arrived(out.at[twin], core_recv.at[0, 0, 2], core_send.at[0, 0, 2])
    for way in range(2):
        for step in range(1, half + 1):
            there = origin_of(way, step)
            origin = there + 1 - 2 * core
            for seg in range(2):
                if step <= hops[way][seg]:
                    arrived(
                        out.at[origin, segments[seg]], core_recv.at[way, step, seg],
                        core_send.at[way, step, seg],
                    )
            if step <= hops[way][0]:
                arrived(out.at[origin, others], core_recv.at[way, step, 2], core_send.at[way, step, 2])
    if scatter:
        for k in range(1, n):
            arrived(mine.at[(me + n - k) % n], part_recv.at[k], part_send.at[k])
        keep_part.wait()
    keep.wait()
    for copy in sent:
        copy.wait_send()


def ring_gather(block, collective_id, parts=None):
    n = lax.axis_size("fsdp")
    half = n // 4
    rows, width = block.shape
    third = (rows // 16 + 2) // 3 * 16
    scatter = parts is not None
    out_shape = [jax.ShapeDtypeStruct((n, rows, width), block.dtype)]
    any_spec = pl.BlockSpec(memory_space=pl.ANY)
    dma = pltpu.SemaphoreType.DMA
    scratch = [
        dma((2,)),
        dma((2, 2, half + 1)), dma((2, 2, half + 1)),
        dma((2, half + 1)), dma((2, half + 1)),
        dma((2, half + 1, 3)), dma((2, half + 1, 3)),
    ]
    operands = [block]
    if scatter:
        out_shape.append(jax.ShapeDtypeStruct(parts.shape, parts.dtype))
        scratch += [dma((n,)), dma((n,))]
        operands.append(parts)
    return pl.pallas_call(
        functools.partial(ring_kernel, scatter, third),
        out_shape=out_shape,
        in_specs=[pl.BlockSpec(memory_space=pltpu.VMEM)] * len(operands),
        out_specs=[any_spec] * len(out_shape),
        scratch_shapes=scratch,
        compiler_params=pltpu.CompilerParams(
            collective_id=collective_id, has_side_effects=True, vmem_limit_bytes=24 * 2**20
        ),
    )(*operands)


def row_sum_kernel(rows, share, out, landed, send_sems, recv_sems):
    me = lax.axis_index("dp")
    barrier = pltpu.get_barrier_semaphore()
    for k in range(1, rows):
        pl.semaphore_signal(barrier, inc=1, device_id={"dp": (me + k) % rows}, device_id_type=MESH)
    pl.semaphore_wait(barrier, rows - 1)
    copies = []
    for k in range(1, rows):
        copy = pltpu.make_async_remote_copy(
            src_ref=share, dst_ref=landed.at[me], send_sem=send_sems.at[k],
            recv_sem=recv_sems.at[k], device_id={"dp": (me + k) % rows}, device_id_type=MESH,
        )
        copy.start()
        copies.append(copy)
    keep = pltpu.make_async_copy(share, landed.at[me], send_sems.at[0])
    keep.start()
    for k in range(1, rows):
        pltpu.make_async_remote_copy(
            src_ref=share, dst_ref=landed.at[(me + rows - k) % rows], send_sem=send_sems.at[k],
            recv_sem=recv_sems.at[k], device_id={"dp": (me + k) % rows}, device_id_type=MESH,
        ).wait_recv()
    keep.wait()
    for copy in copies:
        copy.wait_send()
    total = landed[0]
    for k in range(1, rows):
        total = total + landed[k]
    out[...] = total


def sum_over_rows(share):
    rows = lax.axis_size("dp")
    vmem = pl.BlockSpec(memory_space=pltpu.VMEM)
    return pl.pallas_call(
        functools.partial(row_sum_kernel, rows),
        out_shape=jax.ShapeDtypeStruct(share.shape, share.dtype),
        in_specs=[vmem],
        out_specs=vmem,
        scratch_shapes=[
            pltpu.VMEM((rows, *share.shape), share.dtype),
            pltpu.SemaphoreType.DMA((rows,)),
            pltpu.SemaphoreType.DMA((rows,)),
        ],
        compiler_params=pltpu.CompilerParams(
            collective_id=2, has_side_effects=True, vmem_limit_bytes=16 * 2**20
        ),
    )(share)


def general_per_device(
    queries,
    keys,
    values,
    lengths,
    normalized_weight,
    block_scale_codes,
    scale_group_factor,
    scale_group_offset,
    adapter_down_weight,
    adapter_up_weight,
    cotangent,
):
    n = lax.axis_size("fsdp")
    row_index = lax.axis_index("dp")
    rank, down_width = adapter_down_weight.shape
    up_width = adapter_up_weight.shape[1]
    own_rows = down_width + up_width
    packed_rows = own_rows * rank // 128
    padded_rows = -(-packed_rows // 16) * 16

    def pack(x):
        x = x.reshape(*x.shape[:-2], packed_rows, 128)
        pad = [(0, 0)] * (x.ndim - 2) + [(0, padded_rows - packed_rows), (0, 0)]
        return jnp.pad(x, pad)

    def unpack(x):
        return x[..., :packed_rows, :].reshape(*x.shape[:-2], own_rows, rank)

    own_lengths = lax.dynamic_index_in_dim(lengths[0], row_index, 0, keepdims=False)
    own_adapters = jnp.concatenate([adapter_up_weight.T, adapter_down_weight.T], axis=0)
    (adapters,) = ring_gather(pack(own_adapters), 0)
    adapters = unpack(adapters)
    up_rows = adapters[:, :up_width].reshape(n * up_width, rank)
    down_rows = adapters[:, up_width:].reshape(n * down_width, rank)

    attention_output = attend(queries, keys, values, own_lengths)
    reduced_activation = jnp.dot(
        attention_output, down_rows, preferred_element_type=jnp.float32
    ).astype(jnp.bfloat16)
    reduced_gradient = (
        adapter_scale * jnp.dot(cotangent, up_rows, preferred_element_type=jnp.float32)
    ).astype(jnp.bfloat16)
    down_part = jnp.dot(attention_output.T, reduced_gradient, preferred_element_type=jnp.float32)
    up_part = adapter_scale * jnp.dot(
        cotangent.T, reduced_activation, preferred_element_type=jnp.float32
    )
    parts = jnp.concatenate(
        [up_part.reshape(n, up_width, rank), down_part.reshape(n, down_width, rank)], axis=1
    ).astype(jnp.bfloat16)

    local_base = dequantize(
        normalized_weight, block_scale_codes, scale_group_factor, scale_group_offset
    )
    gathered, shares = ring_gather(local_base, 1, pack(parts))
    base_rows = gathered.reshape(-1, gathered.shape[2])
    share = unpack(sum_over_rows(jnp.sum(shares.astype(jnp.float32), axis=0)))

    product = lax.dot_general(
        attention_output, base_rows, (((1,), (1,)), ((), ())), preferred_element_type=jnp.float32
    )
    projection_output = (
        product
        + adapter_scale
        * lax.dot_general(
            reduced_activation, up_rows, (((1,), (1,)), ((), ())),
            preferred_element_type=jnp.float32,
        )
    ).astype(jnp.bfloat16)
    attention_gradient = (
        jnp.dot(cotangent, base_rows, preferred_element_type=jnp.float32)
        + lax.dot_general(
            reduced_gradient, down_rows, (((1,), (1,)), ((), ())),
            preferred_element_type=jnp.float32,
        )
    ).astype(jnp.bfloat16)
    return (projection_output, attention_gradient, share[up_width:].T, share[:up_width].T)


LANES = 128
TILE = 256
A, RA, RB, AD, Y = range(5)


def dot(a, b, contract):
    return lax.dot_general(
        a, b, ((contract[:1], contract[1:]), ((), ())), preferred_element_type=jnp.float32
    )


def fused_kernel(
    lengths, weight, codes, factor, offset, down, up, queries, keys, values, cotangent_hbm,
    projection_output, attention_gradient, up_out, down_out,
    base, adapters, down_rows, q, k, v, cot, attended, absmax, scaled, bias, mixed, low_rank,
    low_grad, product, gradient, part, part_twin, part_row, landed_row, part_chip, landed_chip,
    final, local_sem, ring_send, ring_recv, row_send, row_recv, twin_send, twin_recv, sum_send,
    sum_recv,
):
    n = lax.axis_size("fsdp")
    chips = n // 2
    half = chips // 2
    row = lax.axis_index("dp")
    me = lax.axis_index("fsdp")
    chip, core = me // 2, me % 2
    tokens, features = attended.shape
    model = cot.shape[1]
    rank, width = up.shape
    down_width = down.shape[1]
    pair = 2 * width
    quad = 4 * down_width
    block = pair + quad
    tiles = features // TILE
    a_tiles = 3 * tiles // 10
    r_tiles = (tiles - 2 * a_tiles) // 2
    place = jnp.where(chip % 2 == 0, chip // 2, chips - 1 - chip // 2)
    twin = 2 * chip + 1 - core
    other_row = 1 - row
    way_dir = (1 - 2 * core, 2 * core - 1)

    def device_at(where):
        where = (where + 2 * chips) % chips
        there = jnp.where(where < half, 2 * where, 2 * (chips - 1 - where) + 1)
        return 2 * there + core

    def origin_of(way, step):
        return device_at(place - way_dir[way] * step)

    neighbour = tuple(device_at(place + way_dir[way]) for way in range(2))

    barrier = pltpu.get_barrier_semaphore()
    for d in range(1, chips):
        pl.semaphore_signal(
            barrier, inc=1, device_id={"fsdp": 2 * ((chip + d) % chips) + core}, device_id_type=MESH
        )
    pl.semaphore_signal(barrier, inc=1, device_id={"fsdp": twin}, device_id_type=MESH)
    pl.semaphore_signal(barrier, inc=1, device_id={"dp": other_row}, device_id_type=MESH)
    pl.semaphore_signal(
        barrier, inc=1, device_id={"dp": other_row, "fsdp": twin}, device_id_type=MESH
    )

    loads = [
        pltpu.make_async_copy(src, dst, local_sem.at[i])
        for i, (src, dst) in enumerate(
            ((queries, q), (keys, k), (values, v), (cotangent_hbm, cot))
        )
    ]
    for load in loads:
        load.start()

    sent = []

    def send(src, dst, send_sem, recv_sem, target):
        copy = pltpu.make_async_remote_copy(
            src_ref=src, dst_ref=dst, send_sem=send_sem, recv_sem=recv_sem,
            device_id=target, device_id_type=MESH,
        )
        copy.start()
        sent.append(copy)

    def arrived(dst, send_sem, recv_sem):
        pltpu.make_async_remote_copy(
            src_ref=dst, dst_ref=dst, send_sem=send_sem, recv_sem=recv_sem,
            device_id={"fsdp": twin}, device_id_type=MESH,
        ).wait_recv()

    def rows_of(origin):
        return pl.ds(pl.multiple_of(origin * width, 64), width)

    def tiles_of(kind):
        if kind == A:
            return row * a_tiles, a_tiles
        if kind == Y:
            return (1 - row) * a_tiles, a_tiles
        if kind == RA:
            return 2 * a_tiles, r_tiles
        return 2 * a_tiles + r_tiles, tiles - 2 * a_tiles - r_tiles

    def piece(origin, kind):
        if kind == AD:
            return adapters.at[rows_of(origin)]
        first, count = tiles_of(kind)
        return base.at[rows_of(origin), pl.ds(pl.multiple_of(first * TILE, TILE), count * TILE)]

    def ring(way, step, kind):
        view = piece(me if step == 1 else origin_of(way, step - 1), kind)
        send(
            view, view, ring_send.at[way, step, kind], ring_recv.at[way, step, kind],
            {"fsdp": neighbour[way]},
        )

    def ring_in(way, step, kind):
        view = piece(origin_of(way, step), kind)
        arrived(view, ring_send.at[way, step, kind], ring_recv.at[way, step, kind])
        send(
            view, view, twin_send.at[way, step, kind], twin_recv.at[way, step, kind],
            {"fsdp": twin},
        )
        if kind == A:
            send(
                view, view, row_send.at[way, step], row_recv.at[way, step], {"dp": other_row}
            )

    def row_in(way, step):
        view = piece(origin_of(way, step), Y)
        arrived(view, row_send.at[way, step], row_recv.at[way, step])
        send(view, view, twin_send.at[way, step, Y], twin_recv.at[way, step, Y], {"fsdp": twin})

    def twin_in(way, step, kind):
        origin = origin_of(1 - way, step) + 1 - 2 * core
        arrived(
            piece(origin, kind), twin_send.at[way, step, kind], twin_recv.at[way, step, kind]
        )

    def eye(rows, columns):
        return (
            lax.broadcasted_iota(jnp.int32, (rows, columns), 0)
            == lax.broadcasted_iota(jnp.int32, (rows, columns), 1)
        ).astype(jnp.bfloat16)

    square = eye(width, width)
    own_rows = rows_of(me)
    up_low = jnp.concatenate([up[...], jnp.zeros((LANES - rank, width), up.dtype)], axis=0)
    down_high = jnp.concatenate(
        [jnp.zeros((LANES - rank, down_width), down.dtype), down[...]], axis=0
    )
    adapters[own_rows, :] = (
        dot(square, up_low, (1, 1)) + dot(eye(width, down_width), down_high, (1, 1))
    ).astype(adapters.dtype)

    groups = factor.shape[0]
    for g in range(groups):
        eight = slice(SCALE_GROUP * g, SCALE_GROUP * (g + 1))
        absmax[eight, :] = (
            factor[g : g + 1, :] * (codes[eight, :].astype(jnp.float32) + 1.0) / 256.0
            + offset[g : g + 1, :]
        )
    span = SCALE_GROUP * QBLOCK

    @pl.loop(0, groups)
    def _(g):
        scales = absmax[pl.ds(pl.multiple_of(SCALE_GROUP * g, SCALE_GROUP), SCALE_GROUP), :]
        for j in range(SCALE_GROUP):
            rows = weight[pl.ds(pl.multiple_of(span * g + QBLOCK * j, QBLOCK), QBLOCK), :]
            scaled[QBLOCK * j : QBLOCK * (j + 1), :] = (
                rows.astype(jnp.float32) * scales[j : j + 1, :]
            ).astype(scaled.dtype)
        base[own_rows, pl.ds(pl.multiple_of(span * g, span), span)] = dot(
            square, scaled[...], (1, 1)
        ).astype(base.dtype)

    pl.semaphore_wait(barrier, chips + 2)
    for way in range(2):
        ring(way, 1, AD)
    for way in range(2):
        ring(way, 1, A)
    for way in range(2):
        ring(way, 1, RA)
    own_ad, own_base = adapters.at[own_rows], base.at[own_rows]
    send(own_ad, own_ad, twin_send.at[0, 0, AD], twin_recv.at[0, 0, AD], {"fsdp": twin})
    send(own_base, own_base, twin_send.at[0, 0, A], twin_recv.at[0, 0, A], {"fsdp": twin})

    ends = []
    for j in range(lengths.shape[2]):
        ends.append(lengths[0, row, j] + (ends[-1] if ends else 0))
    at = lax.broadcasted_iota(jnp.int32, (tokens, tokens), 0)
    to = lax.broadcasted_iota(jnp.int32, (tokens, tokens), 1)
    segment_at = sum((at >= end).astype(jnp.int32) for end in ends)
    segment_to = sum((to >= end).astype(jnp.int32) for end in ends)
    bias[...] = jnp.where((segment_at == segment_to) & (to <= at), 0.0, -jnp.inf)
    for load in loads[:3]:
        load.wait()

    head_count = features // HEAD_SIZE
    per_loop = 2

    def heads(first, count):
        @pl.loop(first // per_loop, (first + count) // per_loop)
        def _(i):
            for j in range(per_loop):
                columns = pl.ds(
                    pl.multiple_of((i * per_loop + j) * HEAD_SIZE, HEAD_SIZE), HEAD_SIZE
                )
                scores = dot(q[:, columns], k[:, columns], (1, 1)) * HEAD_SIZE ** (-0.5)
                scores = scores + bias[...]
                weights = jnp.exp(scores - jnp.max(scores, axis=-1, keepdims=True))
                total = jnp.sum(weights, axis=-1, keepdims=True)
                summed = dot(weights.astype(jnp.bfloat16), v[:, columns], (1, 0))
                attended[:, columns] = (summed / total).astype(attended.dtype)

    def accumulate(way, step, *kinds, origin=None):
        there = (origin_of(way, step) if origin is None else origin) // 2
        columns = pl.ds(pl.multiple_of(there * pair, LANES), pair)
        for first, count in kinds:
            @pl.loop(first, first + count)
            def _(i):
                some = pl.ds(pl.multiple_of(i * TILE, TILE), TILE)
                rows = base[pl.ds(pl.multiple_of(there * pair, LANES), pair), some]
                gradient[:, some] += dot(cot[:, columns], rows, (1, 0))
                product[:, columns] += dot(attended[:, some], rows, (1, 1))

    share = head_count // 10 * 2
    heads(0, 2 * share)
    for way in range(2):
        ring_in(way, 1, AD)
        ring(way, 2, AD)
    heads(2 * share, share)
    for way in range(2):
        ring_in(way, 1, A)
        ring(way, 2, A)
        ring(way, 1, RB)
    for way in range(2):
        ring_in(way, 2, AD)
        ring(way, 3, AD)
    heads(3 * share, share)
    for way in range(2):
        ring_in(way, 3, AD)
    ring(0, 4, AD)
    heads(4 * share, head_count - 4 * share)
    for way in range(2):
        ring_in(way, 1, RA)
    ring_in(0, 4, AD)
    arrived(
        adapters.at[rows_of(twin)], twin_send.at[0, 0, AD], twin_recv.at[0, 0, AD]
    )
    for step in range(1, half + 1):
        for way in range(2 if step < half else 1):
            twin_in(way, step, AD)
    loads[3].wait()

    for f in range(n):
        down_rows[f * down_width : (f + 1) * down_width, :] = adapters[
            f * width : f * width + down_width, :
        ]
    lane = lax.broadcasted_iota(jnp.int32, (tokens, LANES), 1)
    activation = dot(attended[...], down_rows[...], (1, 0))
    grads = adapter_scale * dot(cot[...], adapters[...], (1, 0))
    both = jnp.where(lane < rank, pltpu.roll(activation, rank, 1), pltpu.roll(grads, rank, 1))
    both = both.astype(jnp.bfloat16)
    mixed[...] = both
    nothing = jnp.zeros_like(both)
    low_rank[...] = jnp.where(lane < rank, both * jnp.bfloat16(adapter_scale), nothing)
    low_grad[...] = jnp.where(lane < rank, nothing, both)
    chunk = pair

    @pl.loop(0, model // chunk)
    def _(i):
        columns = pl.ds(pl.multiple_of(i * chunk, LANES), chunk)
        both = mixed[...]
        part[:, columns] = (
            adapter_scale * dot(both, cot[:, columns], (0, 0))[:rank]
        ).astype(part.dtype)

    @pl.loop(0, features // chunk)
    def _(i):
        columns = pl.ds(pl.multiple_of(i * chunk, LANES), chunk)
        there = pl.ds(pl.multiple_of(model + i * chunk, LANES), chunk)
        both = mixed[...]
        part[:, there] = dot(both, attended[:, columns], (0, 0))[rank:].astype(part.dtype)

    per_core = rank // 2
    per_row = per_core // 2
    theirs = pl.ds(pl.multiple_of((1 - core) * per_core, per_core), per_core)
    send(part.at[theirs], part_twin, sum_send.at[0], sum_recv.at[0], {"fsdp": twin})

    for way in range(2):
        ring_in(way, 2, A)
        ring(way, 3, A)
        ring(way, 2, RA)
        row_in(way, 1)

    @pl.loop(0, model // pair)
    def _(i):
        columns = pl.ds(pl.multiple_of(i * pair, LANES), pair)
        product[:, columns] = dot(low_rank[...], adapters[columns, :], (1, 1))

    @pl.loop(0, tiles)
    def _(i):
        some = pl.ds(pl.multiple_of(i * TILE, TILE), TILE)
        gradient[:, some] = dot(low_grad[...], down_rows[some, :], (1, 1))

    arrived(part_twin, sum_send.at[0], sum_recv.at[0])
    away = pl.ds(pl.multiple_of(core * per_core + (1 - row) * per_row, per_row), per_row)
    away_twin = pl.ds(pl.multiple_of((1 - row) * per_row, per_row), per_row)
    kept = pl.ds(pl.multiple_of(core * per_core + row * per_row, per_row), per_row)
    kept_twin = pl.ds(pl.multiple_of(row * per_row, per_row), per_row)

    @pl.loop(0, (model + features) // chunk)
    def _(i):
        columns = pl.ds(pl.multiple_of(i * chunk, LANES), chunk)
        part_row[:, columns] = (
            part[away, columns].astype(jnp.float32)
            + part_twin[away_twin, columns].astype(jnp.float32)
        ).astype(part_row.dtype)

    send(part_row, landed_row, sum_send.at[1], sum_recv.at[1], {"dp": other_row})

    arrived(base.at[rows_of(twin)], twin_send.at[0, 0, A], twin_recv.at[0, 0, A])
    accumulate(0, 0, (0, tiles), origin=me)
    for way in range(2):
        ring_in(way, 1, RB)
    for way in range(2):
        for kind in (A, RA, RB, Y):
            twin_in(1 - way, 1, kind)
        accumulate(way, 1, (0, tiles))

    arrived(landed_row, sum_send.at[1], sum_recv.at[1])

    def row_sum(columns):
        return (
            part[kept, columns].astype(jnp.float32)
            + part_twin[kept_twin, columns].astype(jnp.float32)
            + landed_row[:, columns].astype(jnp.float32)
        ).astype(part_chip.dtype)

    @pl.loop(0, chips)
    def _(i):
        part_chip[i, :, :pair] = row_sum(pl.ds(pl.multiple_of(i * pair, LANES), pair))
        part_chip[i, :, pair:] = row_sum(
            pl.ds(pl.multiple_of(model + i // 2 * quad, LANES), quad)
        )

    for d in range(1, chips):
        there = (chip + d) % chips
        send(
            part_chip.at[there], landed_chip.at[d], sum_send.at[1 + d], sum_recv.at[1 + d],
            {"fsdp": 2 * there + core},
        )

    for way in range(2):
        ring_in(way, 3, A)
    ring(0, 4, A)
    for way in range(2):
        ring(way, 2, RB)
    for way in range(2):
        ring_in(way, 2, RA)
    ring(1, 3, RA)
    for way in range(2):
        row_in(way, 2)
    for way in range(2):
        for kind in (A, RA, Y):
            twin_in(1 - way, 2, kind)
        accumulate(way, 2, (0, 2 * a_tiles + r_tiles))
    ring_in(0, 4, A)
    ring(0, 3, RA)
    for way in range(2):
        ring_in(way, 2, RB)
        ring(way, 3, RB)

    total = part_chip[chip].astype(jnp.float32)
    for d in range(1, chips):
        arrived(landed_chip.at[d], sum_send.at[1 + d], sum_recv.at[1 + d])
        total = total + landed_chip[d].astype(jnp.float32)
    own = 2 * core + row
    final[own] = total
    targets = ({"fsdp": twin}, {"dp": other_row}, {"dp": other_row, "fsdp": twin})
    for i, target in enumerate(targets):
        send(
            final.at[own], final.at[own], sum_send.at[1 + chips + i],
            sum_recv.at[1 + chips + i], target,
        )

    for way in range(2):
        twin_in(1 - way, 2, RB)
        accumulate(way, 2, tiles_of(RB))
    for way in range(2):
        row_in(way, 3)
        ring_in(way, 3, RA)
    ring(1, 4, RA)
    for way in range(2):
        for kind in (A, RA, Y):
            twin_in(1 - way, 3, kind)
        accumulate(way, 3, (0, 2 * a_tiles + r_tiles))
    for way in range(2):
        ring_in(way, 3, RB)
    ring(1, 4, RB)
    for way in range(2):
        twin_in(1 - way, 3, RB)
        accumulate(way, 3, tiles_of(RB))
    ring_in(1, 4, RA)
    twin_in(0, 4, A)
    twin_in(1, 4, RA)
    accumulate(0, 4, tiles_of(A), tiles_of(RA))
    row_in(0, 4)
    twin_in(0, 4, Y)
    accumulate(0, 4, tiles_of(Y))

    owners = (2 * (1 - core) + row, 2 * core + 1 - row, 2 * (1 - core) + 1 - row)
    for i, owner in enumerate(owners):
        arrived(final.at[owner], sum_send.at[1 + chips + i], sum_recv.at[1 + chips + i])
    ranks = final[...].reshape(rank, block)
    up_cols, down_cols = ranks[:, :pair], ranks[:, pair:]
    up_cols = jnp.where(core == 0, up_cols, pltpu.roll(up_cols, pair - width, 1))
    up_out[...] = up_cols[:, :width]
    turned = down_cols
    for j in range(1, 4):
        turned = jnp.where(me % 4 == j, pltpu.roll(down_cols, quad - j * down_width, 1), turned)
    down_out[...] = turned[:, :down_width]

    ring_in(1, 4, RB)
    twin_in(1, 4, RB)
    accumulate(0, 4, tiles_of(RB))

    @pl.loop(0, model // pair)
    def _(i):
        columns = pl.ds(pl.multiple_of(i * pair, LANES), pair)
        projection_output[:, columns] = product[:, columns].astype(projection_output.dtype)

    @pl.loop(0, features // chunk)
    def _(i):
        columns = pl.ds(pl.multiple_of(i * chunk, LANES), chunk)
        attention_gradient[:, columns] = gradient[:, columns].astype(attention_gradient.dtype)

    for copy in sent:
        copy.wait_send()


def fused_per_device(
    queries,
    keys,
    values,
    lengths,
    normalized_weight,
    block_scale_codes,
    scale_group_factor,
    scale_group_offset,
    adapter_down_weight,
    adapter_up_weight,
    cotangent,
):
    n = lax.axis_size("fsdp")
    chips = n // 2
    half = chips // 2
    tokens, features = queries.shape
    model = cotangent.shape[1]
    rank, width = adapter_up_weight.shape
    down_width = adapter_down_weight.shape[1]
    block = 2 * width + 4 * down_width
    low, full = jnp.bfloat16, jnp.float32
    dma = pltpu.SemaphoreType.DMA
    vmem = pl.BlockSpec(memory_space=pltpu.VMEM)
    hbm = pl.BlockSpec(memory_space=pl.ANY)
    shapes = lambda *s: pltpu.VMEM(s[:-1], s[-1])
    sums = 1 + chips + 3
    return tuple(
        pl.pallas_call(
            fused_kernel,
            out_shape=[
                jax.ShapeDtypeStruct((tokens, model), low),
                jax.ShapeDtypeStruct((tokens, features), low),
                jax.ShapeDtypeStruct((rank, width), full),
                jax.ShapeDtypeStruct((rank, down_width), full),
            ],
            in_specs=[pl.BlockSpec(memory_space=pltpu.SMEM)] + [vmem] * 6 + [hbm] * 4,
            out_specs=[vmem] * 4,
            scratch_shapes=[
                shapes(n * width, features, low),
                shapes(n * width, LANES, low),
                shapes(features, LANES, low),
                shapes(tokens, features, low),
                shapes(tokens, features, low),
                shapes(tokens, features, low),
                shapes(tokens, model, low),
                shapes(tokens, features, low),
                shapes(features // QBLOCK, width, full),
                shapes(SCALE_GROUP * QBLOCK, width, low),
                shapes(tokens, tokens, full),
                shapes(tokens, LANES, low),
                shapes(tokens, LANES, low),
                shapes(tokens, LANES, low),
                shapes(tokens, model, full),
                shapes(tokens, features, full),
                shapes(rank, model + features, low),
                shapes(rank // 2, model + features, low),
                shapes(rank // 4, model + features, low),
                shapes(rank // 4, model + features, low),
                shapes(chips, rank // 4, block, low),
                shapes(chips, rank // 4, block, low),
                shapes(4, rank // 4, block, full),
                dma((4,)),
                dma((2, half + 1, 4)),
                dma((2, half + 1, 4)),
                dma((2, half + 1)),
                dma((2, half + 1)),
                dma((2, half + 1, 5)),
                dma((2, half + 1, 5)),
                dma((sums,)),
                dma((sums,)),
            ],
            compiler_params=pltpu.CompilerParams(
                collective_id=3, has_side_effects=True, vmem_limit_bytes=60 * 2**20
            ),
        )(
            lengths, normalized_weight, block_scale_codes, scale_group_factor,
            scale_group_offset, adapter_down_weight, adapter_up_weight, queries, keys, values,
            cotangent,
        )
    )


def per_device(*operands):
    projection_output, attention_gradient, up_gradient, down_gradient = fused_per_device(*operands)
    return projection_output, attention_gradient, down_gradient, up_gradient


def fused_fits(mesh):
    return mesh.shape["dp"] == 2 and mesh.shape["fsdp"] == 16


def solution(mesh):
    return jax.shard_map(
        per_device if fused_fits(mesh) else general_per_device,
        mesh=mesh,
        in_specs=(
            P(("dp", "fsdp"), None),
            P(("dp", "fsdp"), None),
            P(("dp", "fsdp"), None),
            P("fsdp", None, None),
            P(None, "fsdp"),
            P(None, "fsdp"),
            P(None, "fsdp"),
            P(None, "fsdp"),
            P(None, "fsdp"),
            P(None, "fsdp"),
            P(("dp", "fsdp"), None),
        ),
        out_specs=(
            P(("dp", "fsdp"), None),
            P(("dp", "fsdp"), None),
            P(None, "fsdp"),
            P(None, "fsdp"),
        ),
        check_vma=False,
    )
```

```python
import functools

import jax
import jax.numpy as jnp
from jax import lax
from jax.experimental import pallas as pl
from jax.experimental.pallas import tpu as pltpu
from jax.sharding import PartitionSpec as P

HEAD_SIZE = 128
QBLOCK = 64
SCALE_GROUP = 8


adapter_scale = 0.25


def dequantize_kernel(weight, absmax, out):
    rows, features = out.shape
    lane = lax.broadcasted_iota(jnp.int32, (rows, 2 * QBLOCK), 1)
    for i in range(features // (2 * QBLOCK)):
        columns = slice(2 * QBLOCK * i, 2 * QBLOCK * (i + 1))
        scale = jnp.where(
            lane < QBLOCK, absmax[:, 2 * i : 2 * i + 1], absmax[:, 2 * i + 1 : 2 * i + 2]
        )
        out[:, columns] = (weight[:, columns].astype(jnp.float32) * scale).astype(out.dtype)


def dequantize(normalized_weight, block_scale_codes, scale_group_factor, scale_group_offset):
    spread_scale = jnp.repeat(scale_group_factor, SCALE_GROUP, axis=0)
    spread_offset = jnp.repeat(scale_group_offset, SCALE_GROUP, axis=0)
    absmax = spread_scale * (block_scale_codes.astype(jnp.float32) + 1.0) / 256.0 + spread_offset
    weight = normalized_weight.T
    return pl.pallas_call(
        dequantize_kernel,
        out_shape=jax.ShapeDtypeStruct(weight.shape, jnp.bfloat16),
        compiler_params=pltpu.CompilerParams(vmem_limit_bytes=16 * 2**20),
    )(weight, absmax.T)


def attend(queries, keys, values, doc_lengths):
    tokens = queries.shape[0]
    head_count = queries.shape[1] // HEAD_SIZE
    query_heads = queries.reshape(tokens, head_count, HEAD_SIZE)
    key_heads = keys.reshape(tokens, head_count, HEAD_SIZE)
    value_heads = values.reshape(tokens, head_count, HEAD_SIZE)
    doc_ends = jnp.cumsum(doc_lengths)
    places = jnp.arange(tokens, dtype=jnp.int32)
    segment = jnp.sum((doc_ends[None, :] <= places[:, None]).astype(jnp.int32), axis=1)
    allowed = (segment[:, None] == segment[None, :]) & (places[None, :] <= places[:, None])
    scores = jnp.einsum(
        "qhe,khe->hqk", query_heads, key_heads, preferred_element_type=jnp.float32
    ) * HEAD_SIZE ** (-0.5)
    scores = jnp.where(allowed[None], scores, -jnp.inf)
    row_max = jnp.max(scores, axis=-1, keepdims=True)
    weights = jnp.exp(scores - row_max)
    total = jnp.sum(weights, axis=-1)
    summed = jnp.einsum(
        "hqk,khe->qhe",
        weights.astype(jnp.bfloat16),
        value_heads,
        preferred_element_type=jnp.float32,
    )
    return (
        (summed / jnp.transpose(total)[:, :, None])
        .astype(jnp.bfloat16)
        .reshape(tokens, head_count * HEAD_SIZE)
    )


MESH = pl.DeviceIdType.MESH


def ring_kernel(scatter, third, *refs):
    if scatter:
        block, parts, out, mine, sems, ring_send, ring_recv, row_send, row_recv = refs[:9]
        core_send, core_recv, part_send, part_recv = refs[9:]
    else:
        block, out, sems, ring_send, ring_recv, row_send, row_recv, core_send, core_recv = refs
    n = lax.axis_size("fsdp")
    chips = n // 2
    half = chips // 2
    row = lax.axis_index("dp")
    me = lax.axis_index("fsdp")
    chip, core = me // 2, me % 2
    place = jnp.where(chip % 2 == 0, chip // 2, chips - 1 - chip // 2)

    def device_at(where):
        where = (where + chips) % chips
        there = jnp.where(where < half, 2 * where, 2 * (chips - 1 - where) + 1)
        return 2 * there + core

    neighbour = (device_at(place + 1), device_at(place - 1))
    twin = 2 * chip + 1 - core
    other_row = row + 1 - 2 * (row % 2)
    parity = row % 2
    size = block.shape[0]
    own = (pl.ds(pl.multiple_of(parity * third, 16), third))
    others = (pl.ds(pl.multiple_of((1 - parity) * third, 16), third))
    rest = pl.ds(2 * third, size - 2 * third)
    segments = (own, rest)

    barrier = pltpu.get_barrier_semaphore()
    if scatter:
        for k in range(1, n):
            pl.semaphore_signal(barrier, inc=1, device_id={"fsdp": (me + k) % n}, device_id_type=MESH)
        pl.semaphore_signal(barrier, inc=1, device_id={"dp": other_row}, device_id_type=MESH)
        pl.semaphore_wait(barrier, n)
    else:
        for peer in (*neighbour, twin):
            pl.semaphore_signal(barrier, inc=1, device_id={"fsdp": peer}, device_id_type=MESH)
        pl.semaphore_signal(barrier, inc=1, device_id={"dp": other_row}, device_id_type=MESH)
        pl.semaphore_wait(barrier, 4)

    sent = []

    def send(src, dst, send_sem, recv_sem, target):
        copy = pltpu.make_async_remote_copy(
            src_ref=src, dst_ref=dst, send_sem=send_sem, recv_sem=recv_sem,
            device_id=target, device_id_type=MESH,
        )
        copy.start()
        sent.append(copy)

    def arrived(dst, recv_sem, send_sem):
        pltpu.make_async_remote_copy(
            src_ref=dst, dst_ref=dst, send_sem=send_sem, recv_sem=recv_sem,
            device_id={"fsdp": twin}, device_id_type=MESH,
        ).wait_recv()

    hops = ((half, half - 1), (half - 1, half))

    def ring(src, origin, way, seg, step):
        send(
            src, out.at[origin, segments[seg]], ring_send.at[way, seg, step],
            ring_recv.at[way, seg, step], {"fsdp": neighbour[way]},
        )

    for seg in range(2):
        for way in range(2):
            if hops[way][seg] >= 1:
                ring(block.at[segments[seg]], me, way, seg, 0)
    send(block, out.at[me], core_send.at[0, 0, 2], core_recv.at[0, 0, 2], {"fsdp": twin})
    if scatter:
        for k in range(1, n):
            to = (me + k) % n
            send(parts.at[to], mine.at[me], part_send.at[k], part_recv.at[k], {"fsdp": to})
    keep = pltpu.make_async_copy(block, out.at[me], sems.at[0])
    keep.start()
    if scatter:
        keep_part = pltpu.make_async_copy(parts.at[me], mine.at[me], sems.at[1])
        keep_part.start()

    def origin_of(way, step):
        return device_at(place - step if way == 0 else place + step)

    def to_twin(origin, rows, way, step, kind):
        send(
            out.at[origin, rows], out.at[origin, rows], core_send.at[way, step, kind],
            core_recv.at[way, step, kind], {"fsdp": twin},
        )

    def from_row(way, step):
        origin = origin_of(way, step)
        arrived(out.at[origin, others], row_recv.at[way, step], row_send.at[way, step])
        to_twin(origin, others, way, step, 2)

    for step in range(1, half + 1):
        for seg in range(2):
            for way in range(2):
                if step <= hops[way][seg]:
                    origin = origin_of(way, step)
                    rows = segments[seg]
                    view = out.at[origin, rows]
                    arrived(view, ring_recv.at[way, seg, step - 1], ring_send.at[way, seg, step - 1])
                    if step < hops[way][seg]:
                        ring(view, origin, way, seg, step)
                    if seg == 0:
                        send(
                            view, view, row_send.at[way, step], row_recv.at[way, step],
                            {"dp": other_row},
                        )
                    to_twin(origin, rows, way, step, seg)
        for way in range(2):
            if 1 <= step - 1 <= hops[way][0]:
                from_row(way, step - 1)
    for way in range(2):
        if 1 <= half <= hops[way][0]:
            from_row(way, half)

    arrived(out.at[twin], core_recv.at[0, 0, 2], core_send.at[0, 0, 2])
    for way in range(2):
        for step in range(1, half + 1):
            there = origin_of(way, step)
            origin = there + 1 - 2 * core
            for seg in range(2):
                if step <= hops[way][seg]:
                    arrived(
                        out.at[origin, segments[seg]], core_recv.at[way, step, seg],
                        core_send.at[way, step, seg],
                    )
            if step <= hops[way][0]:
                arrived(out.at[origin, others], core_recv.at[way, step, 2], core_send.at[way, step, 2])
    if scatter:
        for k in range(1, n):
            arrived(mine.at[(me + n - k) % n], part_recv.at[k], part_send.at[k])
        keep_part.wait()
    keep.wait()
    for copy in sent:
        copy.wait_send()


def ring_gather(block, collective_id, parts=None):
    n = lax.axis_size("fsdp")
    half = n // 4
    rows, width = block.shape
    third = (rows // 16 + 2) // 3 * 16
    scatter = parts is not None
    out_shape = [jax.ShapeDtypeStruct((n, rows, width), block.dtype)]
    any_spec = pl.BlockSpec(memory_space=pl.ANY)
    dma = pltpu.SemaphoreType.DMA
    scratch = [
        dma((2,)),
        dma((2, 2, half + 1)), dma((2, 2, half + 1)),
        dma((2, half + 1)), dma((2, half + 1)),
        dma((2, half + 1, 3)), dma((2, half + 1, 3)),
    ]
    operands = [block]
    if scatter:
        out_shape.append(jax.ShapeDtypeStruct(parts.shape, parts.dtype))
        scratch += [dma((n,)), dma((n,))]
        operands.append(parts)
    return pl.pallas_call(
        functools.partial(ring_kernel, scatter, third),
        out_shape=out_shape,
        in_specs=[pl.BlockSpec(memory_space=pltpu.VMEM)] * len(operands),
        out_specs=[any_spec] * len(out_shape),
        scratch_shapes=scratch,
        compiler_params=pltpu.CompilerParams(
            collective_id=collective_id, has_side_effects=True, vmem_limit_bytes=24 * 2**20
        ),
    )(*operands)


def row_sum_kernel(rows, share, out, landed, send_sems, recv_sems):
    me = lax.axis_index("dp")
    barrier = pltpu.get_barrier_semaphore()
    for k in range(1, rows):
        pl.semaphore_signal(barrier, inc=1, device_id={"dp": (me + k) % rows}, device_id_type=MESH)
    pl.semaphore_wait(barrier, rows - 1)
    copies = []
    for k in range(1, rows):
        copy = pltpu.make_async_remote_copy(
            src_ref=share, dst_ref=landed.at[me], send_sem=send_sems.at[k],
            recv_sem=recv_sems.at[k], device_id={"dp": (me + k) % rows}, device_id_type=MESH,
        )
        copy.start()
        copies.append(copy)
    keep = pltpu.make_async_copy(share, landed.at[me], send_sems.at[0])
    keep.start()
    for k in range(1, rows):
        pltpu.make_async_remote_copy(
            src_ref=share, dst_ref=landed.at[(me + rows - k) % rows], send_sem=send_sems.at[k],
            recv_sem=recv_sems.at[k], device_id={"dp": (me + k) % rows}, device_id_type=MESH,
        ).wait_recv()
    keep.wait()
    for copy in copies:
        copy.wait_send()
    total = landed[0]
    for k in range(1, rows):
        total = total + landed[k]
    out[...] = total


def sum_over_rows(share):
    rows = lax.axis_size("dp")
    vmem = pl.BlockSpec(memory_space=pltpu.VMEM)
    return pl.pallas_call(
        functools.partial(row_sum_kernel, rows),
        out_shape=jax.ShapeDtypeStruct(share.shape, share.dtype),
        in_specs=[vmem],
        out_specs=vmem,
        scratch_shapes=[
            pltpu.VMEM((rows, *share.shape), share.dtype),
            pltpu.SemaphoreType.DMA((rows,)),
            pltpu.SemaphoreType.DMA((rows,)),
        ],
        compiler_params=pltpu.CompilerParams(
            collective_id=2, has_side_effects=True, vmem_limit_bytes=16 * 2**20
        ),
    )(share)


def general_per_device(
    queries,
    keys,
    values,
    lengths,
    normalized_weight,
    block_scale_codes,
    scale_group_factor,
    scale_group_offset,
    adapter_down_weight,
    adapter_up_weight,
    cotangent,
):
    n = lax.axis_size("fsdp")
    row_index = lax.axis_index("dp")
    rank, down_width = adapter_down_weight.shape
    up_width = adapter_up_weight.shape[1]
    own_rows = down_width + up_width
    packed_rows = own_rows * rank // 128
    padded_rows = -(-packed_rows // 16) * 16

    def pack(x):
        x = x.reshape(*x.shape[:-2], packed_rows, 128)
        pad = [(0, 0)] * (x.ndim - 2) + [(0, padded_rows - packed_rows), (0, 0)]
        return jnp.pad(x, pad)

    def unpack(x):
        return x[..., :packed_rows, :].reshape(*x.shape[:-2], own_rows, rank)

    own_lengths = lax.dynamic_index_in_dim(lengths[0], row_index, 0, keepdims=False)
    own_adapters = jnp.concatenate([adapter_up_weight.T, adapter_down_weight.T], axis=0)
    (adapters,) = ring_gather(pack(own_adapters), 0)
    adapters = unpack(adapters)
    up_rows = adapters[:, :up_width].reshape(n * up_width, rank)
    down_rows = adapters[:, up_width:].reshape(n * down_width, rank)

    attention_output = attend(queries, keys, values, own_lengths)
    reduced_activation = jnp.dot(
        attention_output, down_rows, preferred_element_type=jnp.float32
    ).astype(jnp.bfloat16)
    reduced_gradient = (
        adapter_scale * jnp.dot(cotangent, up_rows, preferred_element_type=jnp.float32)
    ).astype(jnp.bfloat16)
    down_part = jnp.dot(attention_output.T, reduced_gradient, preferred_element_type=jnp.float32)
    up_part = adapter_scale * jnp.dot(
        cotangent.T, reduced_activation, preferred_element_type=jnp.float32
    )
    parts = jnp.concatenate(
        [up_part.reshape(n, up_width, rank), down_part.reshape(n, down_width, rank)], axis=1
    ).astype(jnp.bfloat16)

    local_base = dequantize(
        normalized_weight, block_scale_codes, scale_group_factor, scale_group_offset
    )
    gathered, shares = ring_gather(local_base, 1, pack(parts))
    base_rows = gathered.reshape(-1, gathered.shape[2])
    share = unpack(sum_over_rows(jnp.sum(shares.astype(jnp.float32), axis=0)))

    product = lax.dot_general(
        attention_output, base_rows, (((1,), (1,)), ((), ())), preferred_element_type=jnp.float32
    )
    projection_output = (
        product
        + adapter_scale
        * lax.dot_general(
            reduced_activation, up_rows, (((1,), (1,)), ((), ())),
            preferred_element_type=jnp.float32,
        )
    ).astype(jnp.bfloat16)
    attention_gradient = (
        jnp.dot(cotangent, base_rows, preferred_element_type=jnp.float32)
        + lax.dot_general(
            reduced_gradient, down_rows, (((1,), (1,)), ((), ())),
            preferred_element_type=jnp.float32,
        )
    ).astype(jnp.bfloat16)
    return (projection_output, attention_gradient, share[up_width:].T, share[:up_width].T)


LANES = 128
TILE = 256
A, RA, RB, AD, Y = range(5)
WHOLE = A


def dot(a, b, contract):
    return lax.dot_general(
        a, b, ((contract[:1], contract[1:]), ((), ())), preferred_element_type=jnp.float32
    )


def fused_kernel(
    lengths, weight, codes, factor, offset, down, up, queries, keys, values, cotangent_hbm,
    projection_output, attention_gradient, up_out, down_out,
    base, adapters, down_rows, q, k, v, cot, attended, bias, mixed, low_rank,
    low_grad, product, gradient, part, part_twin, part_row, landed_row, part_chip, landed_chip,
    final, local_sem, ring_send, ring_recv, row_send, row_recv, twin_send, twin_recv, sum_send,
    sum_recv,
):
    n = lax.axis_size("fsdp")
    chips = n // 2
    half = chips // 2
    row = lax.axis_index("dp")
    me = lax.axis_index("fsdp")
    chip, core = me // 2, me % 2
    tokens, features = attended.shape
    model = cot.shape[1]
    rank, width = up.shape
    down_width = down.shape[1]
    pair = 2 * width
    quad = 4 * down_width
    block = pair + quad
    tiles = features // TILE
    a_tiles = 3 * tiles // 10
    r_tiles = (tiles - 2 * a_tiles) // 2
    place = jnp.where(chip % 2 == 0, chip // 2, chips - 1 - chip // 2)
    twin = 2 * chip + 1 - core
    other_row = 1 - row
    sense = 1 - 2 * core

    def chip_at(where):
        where = (where + 2 * chips) % chips
        return jnp.where(where < half, 2 * where, 2 * (chips - 1 - where) + 1)

    def behind(step):
        return chip_at(place - sense * step)

    def ahead(step):
        return chip_at(place + sense * step)

    barrier = pltpu.get_barrier_semaphore()
    for d in range(1, chips):
        pl.semaphore_signal(
            barrier, inc=1, device_id={"fsdp": 2 * ((chip + d) % chips) + core}, device_id_type=MESH
        )
    pl.semaphore_signal(barrier, inc=1, device_id={"fsdp": twin}, device_id_type=MESH)
    pl.semaphore_signal(barrier, inc=1, device_id={"dp": other_row}, device_id_type=MESH)
    pl.semaphore_signal(
        barrier, inc=1, device_id={"dp": other_row, "fsdp": twin}, device_id_type=MESH
    )

    loads = [
        pltpu.make_async_copy(src, dst, local_sem.at[i])
        for i, (src, dst) in enumerate(
            ((queries, q), (keys, k), (values, v), (cotangent_hbm, cot))
        )
    ]
    for load in loads:
        load.start()

    sent = []

    def send(src, dst, send_sem, recv_sem, target):
        copy = pltpu.make_async_remote_copy(
            src_ref=src, dst_ref=dst, send_sem=send_sem, recv_sem=recv_sem,
            device_id=target, device_id_type=MESH,
        )
        copy.start()
        sent.append(copy)

    def arrived(dst, send_sem, recv_sem):
        pltpu.make_async_remote_copy(
            src_ref=dst, dst_ref=dst, send_sem=send_sem, recv_sem=recv_sem,
            device_id={"fsdp": twin}, device_id_type=MESH,
        ).wait_recv()

    def rows_of(origin):
        return pl.ds(pl.multiple_of(origin * width, 64), width)

    def tiles_of(kind):
        if kind == A:
            return row * a_tiles, a_tiles
        if kind == Y:
            return (1 - row) * a_tiles, a_tiles
        if kind == RA:
            return 2 * a_tiles, r_tiles
        return 2 * a_tiles + r_tiles, tiles - 2 * a_tiles - r_tiles

    def piece(origin, kind):
        if kind == AD:
            return adapters.at[rows_of(origin)]
        first, count = tiles_of(kind)
        return base.at[rows_of(origin), pl.ds(pl.multiple_of(first * TILE, TILE), count * TILE)]

    def shard(origin_chip, side):
        return 2 * origin_chip + (core if side == 0 else 1 - core)

    def ring(step, kind, sides=(0, 1)):
        far = (ahead if kind == AD else behind)(step - 1)
        to = (behind if kind == AD else ahead)(1)
        for side in sides:
            view = piece(shard(far, side), kind)
            send(
                view, view, ring_send.at[step, kind, side], ring_recv.at[step, kind, side],
                {"fsdp": 2 * to + core},
            )

    def to_twin(view, step, kind, side):
        send(
            view, view, twin_send.at[step, kind, side], twin_recv.at[step, kind, side],
            {"fsdp": twin},
        )

    def ring_in(step, kind, sides=(0, 1)):
        for side in sides:
            view = piece(shard((ahead if kind == AD else behind)(step), side), kind)
            arrived(view, ring_send.at[step, kind, side], ring_recv.at[step, kind, side])
            to_twin(view, step, kind, side)
            if kind == A:
                send(
                    view, view, row_send.at[step, side], row_recv.at[step, side],
                    {"dp": other_row},
                )

    def row_in(step, sides=(0, 1)):
        for side in sides:
            view = piece(shard(behind(step), side), Y)
            arrived(view, row_send.at[step, side], row_recv.at[step, side])
            to_twin(view, step, Y, side)

    def twin_in(step, *kinds, sides=(0, 1)):
        for kind in kinds:
            for side in sides:
                far = (behind if kind == AD else ahead)(step) if step else chip
                arrived(
                    piece(shard(far, 1 - side), kind), twin_send.at[step, kind, side],
                    twin_recv.at[step, kind, side],
                )

    def eye(rows, columns):
        return (
            lax.broadcasted_iota(jnp.int32, (rows, columns), 0)
            == lax.broadcasted_iota(jnp.int32, (rows, columns), 1)
        ).astype(jnp.bfloat16)

    square = eye(width, width)
    own_rows = rows_of(me)
    up_low = jnp.concatenate([up[...], jnp.zeros((LANES - rank, width), up.dtype)], axis=0)
    down_high = jnp.concatenate(
        [jnp.zeros((LANES - rank, down_width), down.dtype), down[...]], axis=0
    )
    adapters[own_rows, :] = (
        dot(square, up_low, (1, 1)) + dot(eye(width, down_width), down_high, (1, 1))
    ).astype(adapters.dtype)

    groups = factor.shape[0]
    span = SCALE_GROUP * QBLOCK
    shape = (3 * SCALE_GROUP, span)
    spread = (
        lax.broadcasted_iota(jnp.int32, shape, 0) % SCALE_GROUP
        == lax.broadcasted_iota(jnp.int32, shape, 1) // QBLOCK
    ).astype(jnp.bfloat16)
    for g in range(groups):
        eight = slice(SCALE_GROUP * g, SCALE_GROUP * (g + 1))
        absmax = (
            factor[g : g + 1, :] * (codes[eight, :].astype(jnp.float32) + 1.0) / 256.0
            + offset[g : g + 1, :]
        )
        high = absmax.astype(jnp.bfloat16).astype(jnp.float32)
        middle = (absmax - high).astype(jnp.bfloat16).astype(jnp.float32)
        parts = jnp.concatenate([high, middle, absmax - high - middle], axis=0)
        columns = slice(span * g, span * (g + 1))
        base[own_rows, columns] = (
            weight[:, columns].astype(jnp.float32)
            * dot(parts.astype(jnp.bfloat16), spread, (0, 0))
        ).astype(base.dtype)

    own_ad, own_base = adapters.at[own_rows], base.at[own_rows]
    pl.semaphore_wait(barrier, chips + 2)
    ring(1, AD, (0,))
    ring(1, A, (0,))
    to_twin(own_ad, 0, AD, 0)
    to_twin(own_base, 0, WHOLE, 0)

    ends = []
    for j in range(lengths.shape[2]):
        ends.append(lengths[0, row, j] + (ends[-1] if ends else 0))
    at = lax.broadcasted_iota(jnp.int32, (tokens, tokens), 0)
    to = lax.broadcasted_iota(jnp.int32, (tokens, tokens), 1)
    segment_at = sum((at >= end).astype(jnp.int32) for end in ends)
    segment_to = sum((to >= end).astype(jnp.int32) for end in ends)
    bias[...] = jnp.where((segment_at == segment_to) & (to <= at), 0.0, -jnp.inf)
    for load in loads[:3]:
        load.wait()

    head_count = features // HEAD_SIZE
    per_loop = 2

    def heads(first, count):
        @pl.loop(first // per_loop, (first + count) // per_loop)
        def _(i):
            for j in range(per_loop):
                columns = pl.ds(
                    pl.multiple_of((i * per_loop + j) * HEAD_SIZE, HEAD_SIZE), HEAD_SIZE
                )
                scores = dot(q[:, columns], k[:, columns], (1, 1)) * HEAD_SIZE ** (-0.5)
                scores = scores + bias[...]
                weights = jnp.exp(scores - jnp.max(scores, axis=-1, keepdims=True))
                total = jnp.sum(weights, axis=-1, keepdims=True)
                summed = dot(weights.astype(jnp.bfloat16), v[:, columns], (1, 0))
                attended[:, columns] = (summed / total).astype(attended.dtype)

    def accumulate(there, *kinds):
        columns = pl.ds(pl.multiple_of(there * pair, LANES), pair)
        for first, count in kinds:
            @pl.loop(first, first + count)
            def _(i):
                some = pl.ds(pl.multiple_of(i * TILE, TILE), TILE)
                rows = base[columns, some]
                gradient[:, some] += dot(cot[:, columns], rows, (1, 0))
                product[:, columns] += dot(attended[:, some], rows, (1, 1))

    share = head_count // 10 * 2
    arrived(adapters.at[rows_of(twin)], twin_send.at[0, AD, 0], twin_recv.at[0, AD, 0])
    ring(1, AD, (1,))
    arrived(base.at[rows_of(twin)], twin_send.at[0, WHOLE, 0], twin_recv.at[0, WHOLE, 0])
    ring(1, A, (1,))
    ring(1, RA)
    heads(0, share)
    ring_in(1, AD)
    ring(2, AD)
    heads(share, share)
    ring_in(1, A)
    ring(2, A)
    ring(1, RB)
    ring_in(2, AD)
    ring(3, AD)
    heads(2 * share, share)
    ring_in(3, AD)
    ring(4, AD, (0,))
    heads(3 * share, head_count - 3 * share)
    ring_in(1, RA)
    ring_in(4, AD, (0,))
    for step in range(1, half):
        twin_in(step, AD)
    twin_in(half, AD, sides=(0,))
    loads[3].wait()

    for f in range(n):
        down_rows[f * down_width : (f + 1) * down_width, :] = adapters[
            f * width : f * width + down_width, :
        ]
    lane = lax.broadcasted_iota(jnp.int32, (tokens, LANES), 1)
    activation = dot(attended[...], down_rows[...], (1, 0))
    grads = adapter_scale * dot(cot[...], adapters[...], (1, 0))
    both = jnp.where(lane < rank, pltpu.roll(activation, rank, 1), pltpu.roll(grads, rank, 1))
    both = both.astype(jnp.bfloat16)
    mixed[...] = both
    nothing = jnp.zeros_like(both)
    low_rank[...] = jnp.where(lane < rank, both * jnp.bfloat16(adapter_scale), nothing)
    low_grad[...] = jnp.where(lane < rank, nothing, both)
    chunk = pair

    @pl.loop(0, model // chunk)
    def _(i):
        columns = pl.ds(pl.multiple_of(i * chunk, LANES), chunk)
        both = mixed[...]
        part[:, columns] = (
            adapter_scale * dot(both, cot[:, columns], (0, 0))[:rank]
        ).astype(part.dtype)

    @pl.loop(0, features // chunk)
    def _(i):
        columns = pl.ds(pl.multiple_of(i * chunk, LANES), chunk)
        there = pl.ds(pl.multiple_of(model + i * chunk, LANES), chunk)
        both = mixed[...]
        part[:, there] = dot(both, attended[:, columns], (0, 0))[rank:].astype(part.dtype)

    per_core = rank // 2
    per_row = per_core // 2
    theirs = pl.ds(pl.multiple_of((1 - core) * per_core, per_core), per_core)
    send(part.at[theirs], part_twin, sum_send.at[0], sum_recv.at[0], {"fsdp": twin})

    ring_in(2, A)
    ring(3, A)
    ring(2, RA)
    row_in(1)

    @pl.loop(0, model // pair)
    def _(i):
        columns = pl.ds(pl.multiple_of(i * pair, LANES), pair)
        product[:, columns] = dot(low_rank[...], adapters[columns, :], (1, 1))

    @pl.loop(0, tiles)
    def _(i):
        some = pl.ds(pl.multiple_of(i * TILE, TILE), TILE)
        gradient[:, some] = dot(low_grad[...], down_rows[some, :], (1, 1))

    arrived(part_twin, sum_send.at[0], sum_recv.at[0])
    away = pl.ds(pl.multiple_of(core * per_core + (1 - row) * per_row, per_row), per_row)
    away_twin = pl.ds(pl.multiple_of((1 - row) * per_row, per_row), per_row)
    kept = pl.ds(pl.multiple_of(core * per_core + row * per_row, per_row), per_row)
    kept_twin = pl.ds(pl.multiple_of(row * per_row, per_row), per_row)

    @pl.loop(0, (model + features) // chunk)
    def _(i):
        columns = pl.ds(pl.multiple_of(i * chunk, LANES), chunk)
        part_row[:, columns] = (
            part[away, columns].astype(jnp.float32)
            + part_twin[away_twin, columns].astype(jnp.float32)
        ).astype(part_row.dtype)

    send(part_row, landed_row, sum_send.at[1], sum_recv.at[1], {"dp": other_row})

    accumulate(chip, (0, tiles))
    ring_in(1, RB)
    accumulate(behind(1), (0, tiles))
    twin_in(1, A, RA, RB, Y)
    accumulate(ahead(1), (0, tiles))

    arrived(landed_row, sum_send.at[1], sum_recv.at[1])

    def row_sum(columns):
        return (
            part[kept, columns].astype(jnp.float32)
            + part_twin[kept_twin, columns].astype(jnp.float32)
            + landed_row[:, columns].astype(jnp.float32)
        ).astype(part_chip.dtype)

    @pl.loop(0, chips)
    def _(i):
        part_chip[i, :, :pair] = row_sum(pl.ds(pl.multiple_of(i * pair, LANES), pair))
        part_chip[i, :, pair:] = row_sum(
            pl.ds(pl.multiple_of(model + i // 2 * quad, LANES), quad)
        )

    for d in range(1, chips):
        there = (chip + d) % chips
        send(
            part_chip.at[there], landed_chip.at[d], sum_send.at[1 + d], sum_recv.at[1 + d],
            {"fsdp": 2 * there + core},
        )

    ring_in(3, A)
    ring(4, A, (0,))
    ring(2, RB)
    ring_in(2, RA)
    ring(3, RA)
    row_in(2)
    most = (0, 2 * a_tiles + r_tiles)
    accumulate(behind(2), most)
    twin_in(2, A, RA, Y)
    accumulate(ahead(2), most)
    ring_in(4, A, (0,))
    ring_in(2, RB)
    ring(3, RB)

    total = part_chip[chip].astype(jnp.float32)
    for d in range(1, chips):
        arrived(landed_chip.at[d], sum_send.at[1 + d], sum_recv.at[1 + d])
        total = total + landed_chip[d].astype(jnp.float32)
    own = 2 * core + row
    final[own] = total
    targets = ({"fsdp": twin}, {"dp": other_row}, {"dp": other_row, "fsdp": twin})
    for i, target in enumerate(targets):
        send(
            final.at[own], final.at[own], sum_send.at[1 + chips + i],
            sum_recv.at[1 + chips + i], target,
        )

    accumulate(behind(2), tiles_of(RB))
    twin_in(2, RB)
    accumulate(ahead(2), tiles_of(RB))
    ring_in(3, RA)
    ring(4, RA, (0,))
    row_in(3)
    accumulate(behind(3), most)
    twin_in(3, A, RA, Y)
    accumulate(ahead(3), most)
    ring_in(3, RB)
    ring(4, RB, (0,))
    accumulate(behind(3), tiles_of(RB))
    twin_in(3, RB)
    accumulate(ahead(3), tiles_of(RB))
    row_in(4, (0,))
    ring_in(4, RA, (0,))
    twin_in(4, A, Y, RA, sides=(0,))
    accumulate(behind(4), most)

    owners = (2 * (1 - core) + row, 2 * core + 1 - row, 2 * (1 - core) + 1 - row)
    for i, owner in enumerate(owners):
        arrived(final.at[owner], sum_send.at[1 + chips + i], sum_recv.at[1 + chips + i])
    ranks = final[...].reshape(rank, block)
    up_cols, down_cols = ranks[:, :pair], ranks[:, pair:]
    up_cols = jnp.where(core == 0, up_cols, pltpu.roll(up_cols, pair - width, 1))
    up_out[...] = up_cols[:, :width]
    turned = down_cols
    for j in range(1, 4):
        turned = jnp.where(me % 4 == j, pltpu.roll(down_cols, quad - j * down_width, 1), turned)
    down_out[...] = turned[:, :down_width]

    ring_in(4, RB, (0,))
    twin_in(4, RB, sides=(0,))
    accumulate(behind(4), tiles_of(RB))

    @pl.loop(0, model // pair)
    def _(i):
        columns = pl.ds(pl.multiple_of(i * pair, LANES), pair)
        projection_output[:, columns] = product[:, columns].astype(projection_output.dtype)

    @pl.loop(0, features // chunk)
    def _(i):
        columns = pl.ds(pl.multiple_of(i * chunk, LANES), chunk)
        attention_gradient[:, columns] = gradient[:, columns].astype(attention_gradient.dtype)

    for copy in sent:
        copy.wait_send()


def fused_per_device(
    queries,
    keys,
    values,
    lengths,
    normalized_weight,
    block_scale_codes,
    scale_group_factor,
    scale_group_offset,
    adapter_down_weight,
    adapter_up_weight,
    cotangent,
):
    n = lax.axis_size("fsdp")
    chips = n // 2
    half = chips // 2
    tokens, features = queries.shape
    model = cotangent.shape[1]
    rank, width = adapter_up_weight.shape
    down_width = adapter_down_weight.shape[1]
    block = 2 * width + 4 * down_width
    low, full = jnp.bfloat16, jnp.float32
    dma = pltpu.SemaphoreType.DMA
    vmem = pl.BlockSpec(memory_space=pltpu.VMEM)
    hbm = pl.BlockSpec(memory_space=pltpu.HBM)
    shapes = lambda *s: pltpu.VMEM(s[:-1], s[-1])
    sums = 1 + chips + 3
    return tuple(
        pl.pallas_call(
            fused_kernel,
            out_shape=[
                jax.ShapeDtypeStruct((tokens, model), low),
                jax.ShapeDtypeStruct((tokens, features), low),
                jax.ShapeDtypeStruct((rank, width), full),
                jax.ShapeDtypeStruct((rank, down_width), full),
            ],
            in_specs=[pl.BlockSpec(memory_space=pltpu.SMEM)] + [vmem] * 6 + [hbm] * 4,
            out_specs=[vmem] * 4,
            scratch_shapes=[
                shapes(n * width, features, low),
                shapes(n * width, LANES, low),
                shapes(features, LANES, low),
                shapes(tokens, features, low),
                shapes(tokens, features, low),
                shapes(tokens, features, low),
                shapes(tokens, model, low),
                shapes(tokens, features, low),
                shapes(tokens, tokens, full),
                shapes(tokens, LANES, low),
                shapes(tokens, LANES, low),
                shapes(tokens, LANES, low),
                shapes(tokens, model, full),
                shapes(tokens, features, full),
                shapes(rank, model + features, low),
                shapes(rank // 2, model + features, low),
                shapes(rank // 4, model + features, low),
                shapes(rank // 4, model + features, low),
                shapes(chips, rank // 4, block, low),
                shapes(chips, rank // 4, block, low),
                shapes(4, rank // 4, block, full),
                dma((4,)),
                dma((half + 1, 4, 2)),
                dma((half + 1, 4, 2)),
                dma((half + 1, 2)),
                dma((half + 1, 2)),
                dma((half + 1, 5, 2)),
                dma((half + 1, 5, 2)),
                dma((sums,)),
                dma((sums,)),
            ],
            compiler_params=pltpu.CompilerParams(
                collective_id=3, has_side_effects=True, vmem_limit_bytes=60 * 2**20
            ),
        )(
            lengths, normalized_weight.T, block_scale_codes, scale_group_factor,
            scale_group_offset, adapter_down_weight, adapter_up_weight, queries, keys, values,
            cotangent,
        )
    )


def per_device(*operands):
    projection_output, attention_gradient, up_gradient, down_gradient = fused_per_device(*operands)
    return projection_output, attention_gradient, down_gradient, up_gradient


def fused_fits(mesh):
    return mesh.shape["dp"] == 2 and mesh.shape["fsdp"] == 16


def solution(mesh):
    return jax.shard_map(
        per_device if fused_fits(mesh) else general_per_device,
        mesh=mesh,
        in_specs=(
            P(("dp", "fsdp"), None),
            P(("dp", "fsdp"), None),
            P(("dp", "fsdp"), None),
            P("fsdp", None, None),
            P(None, "fsdp"),
            P(None, "fsdp"),
            P(None, "fsdp"),
            P(None, "fsdp"),
            P(None, "fsdp"),
            P(None, "fsdp"),
            P(("dp", "fsdp"), None),
        ),
        out_specs=(
            P(("dp", "fsdp"), None),
            P(("dp", "fsdp"), None),
            P(None, "fsdp"),
            P(None, "fsdp"),
        ),
        check_vma=False,
    )
```

```python
import functools

import jax
import jax.numpy as jnp
from jax import lax
from jax.experimental import pallas as pl
from jax.experimental.pallas import tpu as pltpu
from jax.sharding import PartitionSpec as P

HEAD_SIZE = 128
QBLOCK = 64
SCALE_GROUP = 8


adapter_scale = 0.25


def dequantize_kernel(weight, absmax, out):
    rows, features = out.shape
    lane = lax.broadcasted_iota(jnp.int32, (rows, 2 * QBLOCK), 1)
    for i in range(features // (2 * QBLOCK)):
        columns = slice(2 * QBLOCK * i, 2 * QBLOCK * (i + 1))
        scale = jnp.where(
            lane < QBLOCK, absmax[:, 2 * i : 2 * i + 1], absmax[:, 2 * i + 1 : 2 * i + 2]
        )
        out[:, columns] = (weight[:, columns].astype(jnp.float32) * scale).astype(out.dtype)


def dequantize(normalized_weight, block_scale_codes, scale_group_factor, scale_group_offset):
    spread_scale = jnp.repeat(scale_group_factor, SCALE_GROUP, axis=0)
    spread_offset = jnp.repeat(scale_group_offset, SCALE_GROUP, axis=0)
    absmax = spread_scale * (block_scale_codes.astype(jnp.float32) + 1.0) / 256.0 + spread_offset
    weight = normalized_weight.T
    return pl.pallas_call(
        dequantize_kernel,
        out_shape=jax.ShapeDtypeStruct(weight.shape, jnp.bfloat16),
        compiler_params=pltpu.CompilerParams(vmem_limit_bytes=16 * 2**20),
    )(weight, absmax.T)


def attend(queries, keys, values, doc_lengths):
    tokens = queries.shape[0]
    head_count = queries.shape[1] // HEAD_SIZE
    query_heads = queries.reshape(tokens, head_count, HEAD_SIZE)
    key_heads = keys.reshape(tokens, head_count, HEAD_SIZE)
    value_heads = values.reshape(tokens, head_count, HEAD_SIZE)
    doc_ends = jnp.cumsum(doc_lengths)
    places = jnp.arange(tokens, dtype=jnp.int32)
    segment = jnp.sum((doc_ends[None, :] <= places[:, None]).astype(jnp.int32), axis=1)
    allowed = (segment[:, None] == segment[None, :]) & (places[None, :] <= places[:, None])
    scores = jnp.einsum(
        "qhe,khe->hqk", query_heads, key_heads, preferred_element_type=jnp.float32
    ) * HEAD_SIZE ** (-0.5)
    scores = jnp.where(allowed[None], scores, -jnp.inf)
    row_max = jnp.max(scores, axis=-1, keepdims=True)
    weights = jnp.exp(scores - row_max)
    total = jnp.sum(weights, axis=-1)
    summed = jnp.einsum(
        "hqk,khe->qhe",
        weights.astype(jnp.bfloat16),
        value_heads,
        preferred_element_type=jnp.float32,
    )
    return (
        (summed / jnp.transpose(total)[:, :, None])
        .astype(jnp.bfloat16)
        .reshape(tokens, head_count * HEAD_SIZE)
    )


MESH = pl.DeviceIdType.MESH


def ring_kernel(scatter, third, *refs):
    if scatter:
        block, parts, out, mine, sems, ring_send, ring_recv, row_send, row_recv = refs[:9]
        core_send, core_recv, part_send, part_recv = refs[9:]
    else:
        block, out, sems, ring_send, ring_recv, row_send, row_recv, core_send, core_recv = refs
    n = lax.axis_size("fsdp")
    chips = n // 2
    half = chips // 2
    row = lax.axis_index("dp")
    me = lax.axis_index("fsdp")
    chip, core = me // 2, me % 2
    place = jnp.where(chip % 2 == 0, chip // 2, chips - 1 - chip // 2)

    def device_at(where):
        where = (where + chips) % chips
        there = jnp.where(where < half, 2 * where, 2 * (chips - 1 - where) + 1)
        return 2 * there + core

    neighbour = (device_at(place + 1), device_at(place - 1))
    twin = 2 * chip + 1 - core
    other_row = row + 1 - 2 * (row % 2)
    parity = row % 2
    size = block.shape[0]
    own = (pl.ds(pl.multiple_of(parity * third, 16), third))
    others = (pl.ds(pl.multiple_of((1 - parity) * third, 16), third))
    rest = pl.ds(2 * third, size - 2 * third)
    segments = (own, rest)

    barrier = pltpu.get_barrier_semaphore()
    if scatter:
        for k in range(1, n):
            pl.semaphore_signal(barrier, inc=1, device_id={"fsdp": (me + k) % n}, device_id_type=MESH)
        pl.semaphore_signal(barrier, inc=1, device_id={"dp": other_row}, device_id_type=MESH)
        pl.semaphore_wait(barrier, n)
    else:
        for peer in (*neighbour, twin):
            pl.semaphore_signal(barrier, inc=1, device_id={"fsdp": peer}, device_id_type=MESH)
        pl.semaphore_signal(barrier, inc=1, device_id={"dp": other_row}, device_id_type=MESH)
        pl.semaphore_wait(barrier, 4)

    sent = []

    def send(src, dst, send_sem, recv_sem, target):
        copy = pltpu.make_async_remote_copy(
            src_ref=src, dst_ref=dst, send_sem=send_sem, recv_sem=recv_sem,
            device_id=target, device_id_type=MESH,
        )
        copy.start()
        sent.append(copy)

    def arrived(dst, recv_sem, send_sem):
        pltpu.make_async_remote_copy(
            src_ref=dst, dst_ref=dst, send_sem=send_sem, recv_sem=recv_sem,
            device_id={"fsdp": twin}, device_id_type=MESH,
        ).wait_recv()

    hops = ((half, half - 1), (half - 1, half))

    def ring(src, origin, way, seg, step):
        send(
            src, out.at[origin, segments[seg]], ring_send.at[way, seg, step],
            ring_recv.at[way, seg, step], {"fsdp": neighbour[way]},
        )

    for seg in range(2):
        for way in range(2):
            if hops[way][seg] >= 1:
                ring(block.at[segments[seg]], me, way, seg, 0)
    send(block, out.at[me], core_send.at[0, 0, 2], core_recv.at[0, 0, 2], {"fsdp": twin})
    if scatter:
        for k in range(1, n):
            to = (me + k) % n
            send(parts.at[to], mine.at[me], part_send.at[k], part_recv.at[k], {"fsdp": to})
    keep = pltpu.make_async_copy(block, out.at[me], sems.at[0])
    keep.start()
    if scatter:
        keep_part = pltpu.make_async_copy(parts.at[me], mine.at[me], sems.at[1])
        keep_part.start()

    def origin_of(way, step):
        return device_at(place - step if way == 0 else place + step)

    def to_twin(origin, rows, way, step, kind):
        send(
            out.at[origin, rows], out.at[origin, rows], core_send.at[way, step, kind],
            core_recv.at[way, step, kind], {"fsdp": twin},
        )

    def from_row(way, step):
        origin = origin_of(way, step)
        arrived(out.at[origin, others], row_recv.at[way, step], row_send.at[way, step])
        to_twin(origin, others, way, step, 2)

    for step in range(1, half + 1):
        for seg in range(2):
            for way in range(2):
                if step <= hops[way][seg]:
                    origin = origin_of(way, step)
                    rows = segments[seg]
                    view = out.at[origin, rows]
                    arrived(view, ring_recv.at[way, seg, step - 1], ring_send.at[way, seg, step - 1])
                    if step < hops[way][seg]:
                        ring(view, origin, way, seg, step)
                    if seg == 0:
                        send(
                            view, view, row_send.at[way, step], row_recv.at[way, step],
                            {"dp": other_row},
                        )
                    to_twin(origin, rows, way, step, seg)
        for way in range(2):
            if 1 <= step - 1 <= hops[way][0]:
                from_row(way, step - 1)
    for way in range(2):
        if 1 <= half <= hops[way][0]:
            from_row(way, half)

    arrived(out.at[twin], core_recv.at[0, 0, 2], core_send.at[0, 0, 2])
    for way in range(2):
        for step in range(1, half + 1):
            there = origin_of(way, step)
            origin = there + 1 - 2 * core
            for seg in range(2):
                if step <= hops[way][seg]:
                    arrived(
                        out.at[origin, segments[seg]], core_recv.at[way, step, seg],
                        core_send.at[way, step, seg],
                    )
            if step <= hops[way][0]:
                arrived(out.at[origin, others], core_recv.at[way, step, 2], core_send.at[way, step, 2])
    if scatter:
        for k in range(1, n):
            arrived(mine.at[(me + n - k) % n], part_recv.at[k], part_send.at[k])
        keep_part.wait()
    keep.wait()
    for copy in sent:
        copy.wait_send()


def ring_gather(block, collective_id, parts=None):
    n = lax.axis_size("fsdp")
    half = n // 4
    rows, width = block.shape
    third = (rows // 16 + 2) // 3 * 16
    scatter = parts is not None
    out_shape = [jax.ShapeDtypeStruct((n, rows, width), block.dtype)]
    any_spec = pl.BlockSpec(memory_space=pl.ANY)
    dma = pltpu.SemaphoreType.DMA
    scratch = [
        dma((2,)),
        dma((2, 2, half + 1)), dma((2, 2, half + 1)),
        dma((2, half + 1)), dma((2, half + 1)),
        dma((2, half + 1, 3)), dma((2, half + 1, 3)),
    ]
    operands = [block]
    if scatter:
        out_shape.append(jax.ShapeDtypeStruct(parts.shape, parts.dtype))
        scratch += [dma((n,)), dma((n,))]
        operands.append(parts)
    return pl.pallas_call(
        functools.partial(ring_kernel, scatter, third),
        out_shape=out_shape,
        in_specs=[pl.BlockSpec(memory_space=pltpu.VMEM)] * len(operands),
        out_specs=[any_spec] * len(out_shape),
        scratch_shapes=scratch,
        compiler_params=pltpu.CompilerParams(
            collective_id=collective_id, has_side_effects=True, vmem_limit_bytes=24 * 2**20
        ),
    )(*operands)


def row_sum_kernel(rows, share, out, landed, send_sems, recv_sems):
    me = lax.axis_index("dp")
    barrier = pltpu.get_barrier_semaphore()
    for k in range(1, rows):
        pl.semaphore_signal(barrier, inc=1, device_id={"dp": (me + k) % rows}, device_id_type=MESH)
    pl.semaphore_wait(barrier, rows - 1)
    copies = []
    for k in range(1, rows):
        copy = pltpu.make_async_remote_copy(
            src_ref=share, dst_ref=landed.at[me], send_sem=send_sems.at[k],
            recv_sem=recv_sems.at[k], device_id={"dp": (me + k) % rows}, device_id_type=MESH,
        )
        copy.start()
        copies.append(copy)
    keep = pltpu.make_async_copy(share, landed.at[me], send_sems.at[0])
    keep.start()
    for k in range(1, rows):
        pltpu.make_async_remote_copy(
            src_ref=share, dst_ref=landed.at[(me + rows - k) % rows], send_sem=send_sems.at[k],
            recv_sem=recv_sems.at[k], device_id={"dp": (me + k) % rows}, device_id_type=MESH,
        ).wait_recv()
    keep.wait()
    for copy in copies:
        copy.wait_send()
    total = landed[0]
    for k in range(1, rows):
        total = total + landed[k]
    out[...] = total


def sum_over_rows(share):
    rows = lax.axis_size("dp")
    vmem = pl.BlockSpec(memory_space=pltpu.VMEM)
    return pl.pallas_call(
        functools.partial(row_sum_kernel, rows),
        out_shape=jax.ShapeDtypeStruct(share.shape, share.dtype),
        in_specs=[vmem],
        out_specs=vmem,
        scratch_shapes=[
            pltpu.VMEM((rows, *share.shape), share.dtype),
            pltpu.SemaphoreType.DMA((rows,)),
            pltpu.SemaphoreType.DMA((rows,)),
        ],
        compiler_params=pltpu.CompilerParams(
            collective_id=2, has_side_effects=True, vmem_limit_bytes=16 * 2**20
        ),
    )(share)


def general_per_device(
    queries,
    keys,
    values,
    lengths,
    normalized_weight,
    block_scale_codes,
    scale_group_factor,
    scale_group_offset,
    adapter_down_weight,
    adapter_up_weight,
    cotangent,
):
    n = lax.axis_size("fsdp")
    row_index = lax.axis_index("dp")
    rank, down_width = adapter_down_weight.shape
    up_width = adapter_up_weight.shape[1]
    own_rows = down_width + up_width
    packed_rows = own_rows * rank // 128
    padded_rows = -(-packed_rows // 16) * 16

    def pack(x):
        x = x.reshape(*x.shape[:-2], packed_rows, 128)
        pad = [(0, 0)] * (x.ndim - 2) + [(0, padded_rows - packed_rows), (0, 0)]
        return jnp.pad(x, pad)

    def unpack(x):
        return x[..., :packed_rows, :].reshape(*x.shape[:-2], own_rows, rank)

    own_lengths = lax.dynamic_index_in_dim(lengths[0], row_index, 0, keepdims=False)
    own_adapters = jnp.concatenate([adapter_up_weight.T, adapter_down_weight.T], axis=0)
    (adapters,) = ring_gather(pack(own_adapters), 0)
    adapters = unpack(adapters)
    up_rows = adapters[:, :up_width].reshape(n * up_width, rank)
    down_rows = adapters[:, up_width:].reshape(n * down_width, rank)

    attention_output = attend(queries, keys, values, own_lengths)
    reduced_activation = jnp.dot(
        attention_output, down_rows, preferred_element_type=jnp.float32
    ).astype(jnp.bfloat16)
    reduced_gradient = (
        adapter_scale * jnp.dot(cotangent, up_rows, preferred_element_type=jnp.float32)
    ).astype(jnp.bfloat16)
    down_part = jnp.dot(attention_output.T, reduced_gradient, preferred_element_type=jnp.float32)
    up_part = adapter_scale * jnp.dot(
        cotangent.T, reduced_activation, preferred_element_type=jnp.float32
    )
    parts = jnp.concatenate(
        [up_part.reshape(n, up_width, rank), down_part.reshape(n, down_width, rank)], axis=1
    ).astype(jnp.bfloat16)

    local_base = dequantize(
        normalized_weight, block_scale_codes, scale_group_factor, scale_group_offset
    )
    gathered, shares = ring_gather(local_base, 1, pack(parts))
    base_rows = gathered.reshape(-1, gathered.shape[2])
    share = unpack(sum_over_rows(jnp.sum(shares.astype(jnp.float32), axis=0)))

    product = lax.dot_general(
        attention_output, base_rows, (((1,), (1,)), ((), ())), preferred_element_type=jnp.float32
    )
    projection_output = (
        product
        + adapter_scale
        * lax.dot_general(
            reduced_activation, up_rows, (((1,), (1,)), ((), ())),
            preferred_element_type=jnp.float32,
        )
    ).astype(jnp.bfloat16)
    attention_gradient = (
        jnp.dot(cotangent, base_rows, preferred_element_type=jnp.float32)
        + lax.dot_general(
            reduced_gradient, down_rows, (((1,), (1,)), ((), ())),
            preferred_element_type=jnp.float32,
        )
    ).astype(jnp.bfloat16)
    return (projection_output, attention_gradient, share[up_width:].T, share[:up_width].T)


LANES = 128
TILE = 256
A, RA, RB, AD, Y = range(5)
WHOLE = A


def dot(a, b, contract):
    return lax.dot_general(
        a, b, ((contract[:1], contract[1:]), ((), ())), preferred_element_type=jnp.float32
    )


def fused_kernel(
    lengths, weight_hbm, codes_hbm, factor_hbm, offset_hbm, down_hbm, up_hbm, queries, keys,
    values, cotangent_hbm,
    projection_hbm, gradient_hbm, up_hbm_out, down_hbm_out,
    base, adapters, down_rows, weight, codes, factor, offset, down, up, q, k, v, cot, attended, bias, mixed, low_rank,
    low_grad, product, gradient, part, part_twin, part_row, landed_row, part_chip,
    landed_side, part_line, landed_line, projection_output, attention_gradient, up_out, down_out,
    final, local_sem, out_sem, ring_send, ring_recv, row_send, row_recv, twin_send, twin_recv, sum_send,
    sum_recv,
):
    n = lax.axis_size("fsdp")
    chips = n // 2
    half = chips // 2
    row = lax.axis_index("dp")
    me = lax.axis_index("fsdp")
    chip, core = me // 2, me % 2
    tokens, features = attended.shape
    model = cot.shape[1]
    rank, width = up.shape
    down_width = down.shape[1]
    pair = 2 * width
    quad = 4 * down_width
    block = pair + quad
    tiles = features // TILE
    a_tiles = 3 * tiles // 10
    r_tiles = (tiles - 2 * a_tiles) // 2
    place = jnp.where(chip % 2 == 0, chip // 2, chips - 1 - chip // 2)
    twin = 2 * chip + 1 - core
    other_row = 1 - row
    sense = 1 - 2 * core

    def chip_at(where):
        where = (where + 2 * chips) % chips
        return jnp.where(where < half, 2 * where, 2 * (chips - 1 - where) + 1)

    def behind(step):
        return chip_at(place - sense * step)

    def ahead(step):
        return chip_at(place + sense * step)

    barrier = pltpu.get_barrier_semaphore()
    peers = (
        {"fsdp": 2 * ahead(1) + core}, {"fsdp": 2 * behind(1) + core}, {"fsdp": twin},
        {"dp": other_row},
    )
    for peer in peers:
        pl.semaphore_signal(barrier, inc=1, device_id=peer, device_id_type=MESH)

    loads = [
        pltpu.make_async_copy(src, dst, local_sem.at[i])
        for i, (src, dst) in enumerate(
            (
                (codes_hbm, codes), (factor_hbm, factor), (offset_hbm, offset),
                (weight_hbm, weight), (up_hbm, up), (down_hbm, down), (queries, q), (keys, k),
                (values, v), (cotangent_hbm, cot),
            )
        )
    ]
    for load in loads:
        load.start()

    sent = []

    def send(src, dst, send_sem, recv_sem, target):
        copy = pltpu.make_async_remote_copy(
            src_ref=src, dst_ref=dst, send_sem=send_sem, recv_sem=recv_sem,
            device_id=target, device_id_type=MESH,
        )
        copy.start()
        sent.append(copy)

    def arrived(dst, send_sem, recv_sem):
        pltpu.make_async_remote_copy(
            src_ref=dst, dst_ref=dst, send_sem=send_sem, recv_sem=recv_sem,
            device_id={"fsdp": twin}, device_id_type=MESH,
        ).wait_recv()

    def rows_of(origin):
        return pl.ds(pl.multiple_of(origin * width, 64), width)

    def tiles_of(kind):
        if kind == A:
            return row * a_tiles, a_tiles
        if kind == Y:
            return (1 - row) * a_tiles, a_tiles
        if kind == RA:
            return 2 * a_tiles, r_tiles
        return 2 * a_tiles + r_tiles, tiles - 2 * a_tiles - r_tiles

    def piece(origin, kind):
        if kind == AD:
            return adapters.at[rows_of(origin)]
        first, count = tiles_of(kind)
        return base.at[rows_of(origin), pl.ds(pl.multiple_of(first * TILE, TILE), count * TILE)]

    def shard(origin_chip, side):
        return 2 * origin_chip + (core if side == 0 else 1 - core)

    def ring(step, kind, sides=(0, 1)):
        far = (ahead if kind == AD else behind)(step - 1)
        to = (behind if kind == AD else ahead)(1)
        for side in sides:
            view = piece(shard(far, side), kind)
            send(
                view, view, ring_send.at[step, kind, side], ring_recv.at[step, kind, side],
                {"fsdp": 2 * to + core},
            )

    def to_twin(view, step, kind, side):
        send(
            view, view, twin_send.at[step, kind, side], twin_recv.at[step, kind, side],
            {"fsdp": twin},
        )

    def ring_in(step, kind, sides=(0, 1)):
        for side in sides:
            view = piece(shard((ahead if kind == AD else behind)(step), side), kind)
            arrived(view, ring_send.at[step, kind, side], ring_recv.at[step, kind, side])
            to_twin(view, step, kind, side)
            if kind == A:
                send(
                    view, view, row_send.at[step, side], row_recv.at[step, side],
                    {"dp": other_row},
                )

    def row_in(step, sides=(0, 1)):
        for side in sides:
            view = piece(shard(behind(step), side), Y)
            arrived(view, row_send.at[step, side], row_recv.at[step, side])
            to_twin(view, step, Y, side)

    def twin_in(step, *kinds, sides=(0, 1)):
        for kind in kinds:
            for side in sides:
                far = (behind if kind == AD else ahead)(step) if step else chip
                arrived(
                    piece(shard(far, 1 - side), kind), twin_send.at[step, kind, side],
                    twin_recv.at[step, kind, side],
                )

    own_rows = rows_of(me)
    groups = factor.shape[0]
    span = SCALE_GROUP * QBLOCK
    shape = (3 * SCALE_GROUP, span)
    spread = (
        lax.broadcasted_iota(jnp.int32, shape, 0) % SCALE_GROUP
        == lax.broadcasted_iota(jnp.int32, shape, 1) // QBLOCK
    ).astype(jnp.bfloat16)

    def dequantize_group(g):
        eight = pl.ds(pl.multiple_of(SCALE_GROUP * g, SCALE_GROUP), SCALE_GROUP)
        absmax = (
            factor[pl.ds(g, 1), :] * (codes[eight, :].astype(jnp.float32) + 1.0) / 256.0
            + offset[pl.ds(g, 1), :]
        )
        high = absmax.astype(jnp.bfloat16).astype(jnp.float32)
        middle = (absmax - high).astype(jnp.bfloat16).astype(jnp.float32)
        parts = jnp.concatenate([high, middle, absmax - high - middle], axis=0)
        columns = pl.ds(pl.multiple_of(span * g, span), span)
        base[own_rows, columns] = (
            weight[:, columns].astype(jnp.float32)
            * dot(parts.astype(jnp.bfloat16), spread, (0, 0))
        ).astype(base.dtype)

    for load in loads[:4]:
        load.wait()
    ahead_groups = -(-a_tiles * TILE // span)
    for i in range(ahead_groups):
        dequantize_group(row * (a_tiles * TILE // span) + i)
    pl.semaphore_wait(barrier, len(peers))
    ring(1, A, (0,))
    def eye(rows, columns):
        return (
            lax.broadcasted_iota(jnp.int32, (rows, columns), 0)
            == lax.broadcasted_iota(jnp.int32, (rows, columns), 1)
        ).astype(jnp.bfloat16)

    square = eye(width, width)
    for load in loads[4:6]:
        load.wait()
    up_low = jnp.concatenate([up[...], jnp.zeros((LANES - rank, width), up.dtype)], axis=0)
    down_high = jnp.concatenate(
        [jnp.zeros((LANES - rank, down_width), down.dtype), down[...]], axis=0
    )
    adapters[own_rows, :] = (
        dot(square, up_low, (1, 1)) + dot(eye(width, down_width), down_high, (1, 1))
    ).astype(adapters.dtype)
    own_ad, own_base = adapters.at[own_rows], base.at[own_rows]
    ring(1, AD, (0,))
    to_twin(own_ad, 0, AD, 0)

    for i in range(groups - ahead_groups):
        lead = row * (a_tiles * TILE // span)
        dequantize_group(jnp.where(i < lead, i, i + ahead_groups))
    to_twin(own_base, 0, WHOLE, 0)

    ends = []
    for j in range(lengths.shape[2]):
        ends.append(lengths[0, row, j] + (ends[-1] if ends else 0))
    at = lax.broadcasted_iota(jnp.int32, (tokens, tokens), 0)
    to = lax.broadcasted_iota(jnp.int32, (tokens, tokens), 1)
    segment_at = sum((at >= end).astype(jnp.int32) for end in ends)
    segment_to = sum((to >= end).astype(jnp.int32) for end in ends)
    bias[...] = jnp.where((segment_at == segment_to) & (to <= at), 0.0, -jnp.inf)
    for load in loads[6:9]:
        load.wait()

    head_count = features // HEAD_SIZE
    per_loop = 2

    def heads(first, count):
        @pl.loop(first // per_loop, (first + count) // per_loop)
        def _(i):
            for j in range(per_loop):
                columns = pl.ds(
                    pl.multiple_of((i * per_loop + j) * HEAD_SIZE, HEAD_SIZE), HEAD_SIZE
                )
                scores = dot(q[:, columns], k[:, columns], (1, 1)) * HEAD_SIZE ** (-0.5)
                scores = scores + bias[...]
                weights = jnp.exp(scores - jnp.max(scores, axis=-1, keepdims=True))
                total = jnp.sum(weights, axis=-1, keepdims=True)
                summed = dot(weights.astype(jnp.bfloat16), v[:, columns], (1, 0))
                attended[:, columns] = (summed / total).astype(attended.dtype)

    def accumulate(there, *kinds):
        columns = pl.ds(pl.multiple_of(there * pair, LANES), pair)
        for first, count in kinds:
            @pl.loop(first, first + count)
            def _(i):
                some = pl.ds(pl.multiple_of(i * TILE, TILE), TILE)
                rows = base[columns, some]
                gradient[:, some] += dot(cot[:, columns], rows, (1, 0))
                product[:, columns] += dot(attended[:, some], rows, (1, 1))

    share = head_count // 10 * 2
    arrived(adapters.at[rows_of(twin)], twin_send.at[0, AD, 0], twin_recv.at[0, AD, 0])
    ring(1, AD, (1,))
    arrived(base.at[rows_of(twin)], twin_send.at[0, WHOLE, 0], twin_recv.at[0, WHOLE, 0])
    ring(1, A, (1,))
    ring(1, RA)
    heads(0, share)
    ring_in(1, AD)
    ring(2, AD)
    heads(share, share)
    ring_in(1, A)
    ring(2, A)
    ring(1, RB)
    ring_in(2, AD)
    ring(3, AD)
    heads(2 * share, share)
    ring_in(3, AD)
    ring(4, AD, (0,))
    heads(3 * share, head_count - 3 * share)
    ring_in(1, RA)
    ring_in(4, AD, (0,))
    for step in range(1, half):
        twin_in(step, AD)
    twin_in(half, AD, sides=(0,))
    loads[9].wait()

    for f in range(n):
        down_rows[f * down_width : (f + 1) * down_width, :] = adapters[
            f * width : f * width + down_width, :
        ]
    lane = lax.broadcasted_iota(jnp.int32, (tokens, LANES), 1)
    activation = dot(attended[...], down_rows[...], (1, 0))
    grads = adapter_scale * dot(cot[...], adapters[...], (1, 0))
    both = jnp.where(lane < rank, pltpu.roll(activation, rank, 1), pltpu.roll(grads, rank, 1))
    both = both.astype(jnp.bfloat16)
    mixed[...] = both
    nothing = jnp.zeros_like(both)
    low_rank[...] = jnp.where(lane < rank, both * jnp.bfloat16(adapter_scale), nothing)
    low_grad[...] = jnp.where(lane < rank, nothing, both)
    chunk = pair

    @pl.loop(0, model // chunk)
    def _(i):
        columns = pl.ds(pl.multiple_of(i * chunk, LANES), chunk)
        both = mixed[...]
        part[:, columns] = (
            adapter_scale * dot(both, cot[:, columns], (0, 0))[:rank]
        ).astype(part.dtype)

    @pl.loop(0, features // chunk)
    def _(i):
        columns = pl.ds(pl.multiple_of(i * chunk, LANES), chunk)
        there = pl.ds(pl.multiple_of(model + i * chunk, LANES), chunk)
        both = mixed[...]
        part[:, there] = dot(both, attended[:, columns], (0, 0))[rank:].astype(part.dtype)

    per_core = rank // 2
    per_row = per_core // 2
    theirs = pl.ds(pl.multiple_of((1 - core) * per_core, per_core), per_core)
    send(part.at[theirs], part_twin, sum_send.at[0], sum_recv.at[0], {"fsdp": twin})

    ring_in(2, A)
    ring(3, A)
    ring(2, RA)
    row_in(1)

    @pl.loop(0, model // pair)
    def _(i):
        columns = pl.ds(pl.multiple_of(i * pair, LANES), pair)
        product[:, columns] = dot(low_rank[...], adapters[columns, :], (1, 1))

    @pl.loop(0, tiles)
    def _(i):
        some = pl.ds(pl.multiple_of(i * TILE, TILE), TILE)
        gradient[:, some] = dot(low_grad[...], down_rows[some, :], (1, 1))

    arrived(part_twin, sum_send.at[0], sum_recv.at[0])
    away = pl.ds(pl.multiple_of(core * per_core + (1 - row) * per_row, per_row), per_row)
    away_twin = pl.ds(pl.multiple_of((1 - row) * per_row, per_row), per_row)
    kept = pl.ds(pl.multiple_of(core * per_core + row * per_row, per_row), per_row)
    kept_twin = pl.ds(pl.multiple_of(row * per_row, per_row), per_row)

    @pl.loop(0, (model + features) // chunk)
    def _(i):
        columns = pl.ds(pl.multiple_of(i * chunk, LANES), chunk)
        part_row[:, columns] = (
            part[away, columns].astype(jnp.float32)
            + part_twin[away_twin, columns].astype(jnp.float32)
        ).astype(part_row.dtype)

    send(part_row, landed_row, sum_send.at[1], sum_recv.at[1], {"dp": other_row})

    accumulate(chip, (0, tiles))
    ring_in(1, RB)
    accumulate(behind(1), (0, tiles))
    twin_in(1, A, RA, RB, Y)
    accumulate(ahead(1), (0, tiles))

    arrived(landed_row, sum_send.at[1], sum_recv.at[1])

    def row_sum(columns):
        return (
            part[kept, columns].astype(jnp.float32)
            + part_twin[kept_twin, columns].astype(jnp.float32)
            + landed_row[:, columns].astype(jnp.float32)
        ).astype(part_chip.dtype)

    side, line = chip % 2, chip // 2

    @pl.loop(0, chips)
    def _(i):
        part_chip[i % 2, i // 2, :, :pair] = row_sum(
            pl.ds(pl.multiple_of(i * pair, LANES), pair)
        )
        part_chip[i % 2, i // 2, :, pair:] = row_sum(
            pl.ds(pl.multiple_of(model + i // 2 * quad, LANES), quad)
        )

    beside = 2 * (2 * line + 1 - side) + core
    send(part_chip.at[1 - side], landed_side, sum_send.at[2], sum_recv.at[2], {"fsdp": beside})

    ring_in(3, A)
    ring(4, A, (0,))
    ring(2, RB)
    ring_in(2, RA)
    ring(3, RA)
    row_in(2)
    most = (0, 2 * a_tiles + r_tiles)
    accumulate(behind(2), most)
    twin_in(2, A, RA, Y)
    accumulate(ahead(2), most)
    ring_in(4, A, (0,))

    arrived(landed_side, sum_send.at[2], sum_recv.at[2])

    @pl.loop(0, half)
    def _(i):
        part_line[i] = (
            part_chip[side, i].astype(jnp.float32) + landed_side[i].astype(jnp.float32)
        ).astype(part_line.dtype)

    for d in range(1, half):
        there = (line + d) % half
        send(
            part_line.at[there], landed_line.at[d], sum_send.at[2 + d], sum_recv.at[2 + d],
            {"fsdp": 2 * (2 * there + side) + core},
        )
    ring_in(2, RB)
    ring(3, RB)

    accumulate(behind(2), tiles_of(RB))
    twin_in(2, RB)
    accumulate(ahead(2), tiles_of(RB))
    total = part_chip[side, line].astype(jnp.float32) + landed_side[line].astype(jnp.float32)
    for d in range(1, half):
        arrived(landed_line.at[d], sum_send.at[2 + d], sum_recv.at[2 + d])
        total = total + landed_line[d].astype(jnp.float32)
    own = 2 * core + row
    final[own] = total
    targets = ({"fsdp": twin}, {"dp": other_row}, {"dp": other_row, "fsdp": twin})
    for i, target in enumerate(targets):
        send(
            final.at[own], final.at[own], sum_send.at[2 + half + i],
            sum_recv.at[2 + half + i], target,
        )

    ring_in(3, RA)
    ring(4, RA, (0,))
    row_in(3)
    accumulate(behind(3), most)
    twin_in(3, A, RA, Y)
    accumulate(ahead(3), most)
    ring_in(3, RB)
    ring(4, RB, (0,))
    accumulate(behind(3), tiles_of(RB))
    twin_in(3, RB)
    accumulate(ahead(3), tiles_of(RB))
    row_in(4, (0,))
    ring_in(4, RA, (0,))
    twin_in(4, A, Y, RA, sides=(0,))
    accumulate(behind(4), most)

    owners = (2 * (1 - core) + row, 2 * core + 1 - row, 2 * (1 - core) + 1 - row)
    for i, owner in enumerate(owners):
        arrived(final.at[owner], sum_send.at[2 + half + i], sum_recv.at[2 + half + i])
    ranks = final[...].reshape(rank, block)
    up_cols, down_cols = ranks[:, :pair], ranks[:, pair:]
    up_cols = jnp.where(core == 0, up_cols, pltpu.roll(up_cols, pair - width, 1))
    up_out[...] = up_cols[:, :width]
    turned = down_cols
    for j in range(1, 4):
        turned = jnp.where(me % 4 == j, pltpu.roll(down_cols, quad - j * down_width, 1), turned)
    down_out[...] = turned[:, :down_width]

    stores = []

    def store(source, target):
        copy = pltpu.make_async_copy(source, target, out_sem.at[len(stores)])
        copy.start()
        stores.append(copy)

    store(up_out, up_hbm_out)
    store(down_out, down_hbm_out)

    def project(there):
        columns = pl.ds(pl.multiple_of(there * pair, LANES), pair)
        projection_output[:, columns] = product[:, columns].astype(projection_output.dtype)
        return columns

    first, count = tiles_of(RB)
    last = pl.ds(first * TILE, count * TILE)

    def convert(i):
        some = pl.ds(pl.multiple_of(i * TILE, TILE), TILE)
        attention_gradient[:, some] = gradient[:, some].astype(attention_gradient.dtype)

    @pl.loop(1, chips)
    def _(i):
        project((behind(half) + i) % chips)

    pl.loop(0, first)(convert)
    for i in range(1, chips):
        columns = pl.ds(pl.multiple_of((behind(half) + i) % chips * pair, LANES), pair)
        store(projection_output.at[:, columns], projection_hbm.at[:, columns])
    most_columns = pl.ds(0, first * TILE)
    store(attention_gradient.at[:, most_columns], gradient_hbm.at[:, most_columns])

    ring_in(4, RB, (0,))
    twin_in(4, RB, sides=(0,))
    accumulate(behind(4), tiles_of(RB))
    columns = project(behind(half))
    store(projection_output.at[:, columns], projection_hbm.at[:, columns])
    pl.loop(first, first + count)(convert)
    store(attention_gradient.at[:, last], gradient_hbm.at[:, last])
    for copy in stores:
        copy.wait()
    for copy in sent:
        copy.wait_send()


def finish_kernel(count, *refs):
    sources, results, held = refs[:count], refs[count : 2 * count], refs[2 * count : 3 * count]
    in_sem, out_sem = refs[3 * count :]
    ins, outs = [], []
    for i in range(count):
        rows, columns = sources[i].shape
        cuts = 4 if i < 2 else 1
        for j in range(cuts):
            some = pl.ds(rows // cuts * j, rows // cuts)
            place = len(ins)
            ins.append(
                pltpu.make_async_copy(sources[i].at[some], held[i].at[some], in_sem.at[place])
            )
            outs.append(
                pltpu.make_async_copy(held[i].at[some], results[i].at[some], out_sem.at[place])
            )
    for copy in ins:
        copy.start()
    for arrival, copy in zip(ins, outs):
        arrival.wait()
        copy.start()
    for copy in outs:
        copy.wait()


def finish(*results):
    anywhere = [pl.BlockSpec(memory_space=pl.ANY)] * len(results)
    dma = pltpu.SemaphoreType.DMA
    return pl.pallas_call(
        functools.partial(finish_kernel, len(results)),
        out_shape=[jax.ShapeDtypeStruct(x.shape, x.dtype) for x in results],
        in_specs=anywhere,
        out_specs=anywhere,
        scratch_shapes=[pltpu.VMEM(x.shape, x.dtype) for x in results] + [dma((12,)), dma((12,))],
        compiler_params=pltpu.CompilerParams(vmem_limit_bytes=62 * 2**20),
    )(*results)


def fused_per_device(
    queries,
    keys,
    values,
    lengths,
    normalized_weight,
    block_scale_codes,
    scale_group_factor,
    scale_group_offset,
    adapter_down_weight,
    adapter_up_weight,
    cotangent,
):
    n = lax.axis_size("fsdp")
    chips = n // 2
    half = chips // 2
    tokens, features = queries.shape
    model = cotangent.shape[1]
    rank, width = adapter_up_weight.shape
    down_width = adapter_down_weight.shape[1]
    block = 2 * width + 4 * down_width
    low, full = jnp.bfloat16, jnp.float32
    dma = pltpu.SemaphoreType.DMA
    hbm = pl.BlockSpec(memory_space=pl.ANY)
    shapes = lambda *s: pltpu.VMEM(s[:-1], s[-1])
    sums = 2 + half + 4
    return tuple(
        pl.pallas_call(
            fused_kernel,
            out_shape=[
                jax.ShapeDtypeStruct((tokens, model), low),
                jax.ShapeDtypeStruct((tokens, features), low),
                jax.ShapeDtypeStruct((rank, width), full),
                jax.ShapeDtypeStruct((rank, down_width), full),
            ],
            in_specs=[pl.BlockSpec(memory_space=pltpu.SMEM)] + [hbm] * 10,
            out_specs=[hbm] * 4,
            scratch_shapes=[
                shapes(n * width, features, low),
                shapes(n * width, LANES, low),
                shapes(features, LANES, low),
                shapes(width, features, low),
                shapes(features // QBLOCK, width, jnp.int32),
                shapes(features // (QBLOCK * SCALE_GROUP), width, full),
                shapes(features // (QBLOCK * SCALE_GROUP), width, full),
                shapes(rank, down_width, low),
                shapes(rank, width, low),
                shapes(tokens, features, low),
                shapes(tokens, features, low),
                shapes(tokens, features, low),
                shapes(tokens, model, low),
                shapes(tokens, features, low),
                shapes(tokens, tokens, full),
                shapes(tokens, LANES, low),
                shapes(tokens, LANES, low),
                shapes(tokens, LANES, low),
                shapes(tokens, model, full),
                shapes(tokens, features, full),
                shapes(rank, model + features, low),
                shapes(rank // 2, model + features, low),
                shapes(rank // 4, model + features, low),
                shapes(rank // 4, model + features, low),
                shapes(2, half, rank // 4, block, low),
                shapes(half, rank // 4, block, low),
                shapes(half, rank // 4, block, low),
                shapes(half, rank // 4, block, low),
                shapes(tokens, model, low),
                shapes(tokens, features, low),
                shapes(rank, width, full),
                shapes(rank, down_width, full),
                shapes(4, rank // 4, block, full),
                dma((10,)),
                dma((chips + 4,)),
                dma((half + 1, 4, 2)),
                dma((half + 1, 4, 2)),
                dma((half + 1, 2)),
                dma((half + 1, 2)),
                dma((half + 1, 5, 2)),
                dma((half + 1, 5, 2)),
                dma((sums,)),
                dma((sums,)),
            ],
            compiler_params=pltpu.CompilerParams(
                collective_id=3, has_side_effects=True, vmem_limit_bytes=60 * 2**20
            ),
        )(
            lengths, normalized_weight.T, block_scale_codes, scale_group_factor,
            scale_group_offset, adapter_down_weight, adapter_up_weight, queries, keys, values,
            cotangent,
        )
    )


def per_device(*operands):
    projection_output, attention_gradient, up_gradient, down_gradient = finish(
        *fused_per_device(*operands)
    )
    return projection_output, attention_gradient, down_gradient, up_gradient


def fused_fits(mesh):
    return mesh.shape["dp"] == 2 and mesh.shape["fsdp"] == 16


def solution(mesh):
    return jax.shard_map(
        per_device if fused_fits(mesh) else general_per_device,
        mesh=mesh,
        in_specs=(
            P(("dp", "fsdp"), None),
            P(("dp", "fsdp"), None),
            P(("dp", "fsdp"), None),
            P("fsdp", None, None),
            P(None, "fsdp"),
            P(None, "fsdp"),
            P(None, "fsdp"),
            P(None, "fsdp"),
            P(None, "fsdp"),
            P(None, "fsdp"),
            P(("dp", "fsdp"), None),
        ),
        out_specs=(
            P(("dp", "fsdp"), None),
            P(("dp", "fsdp"), None),
            P(None, "fsdp"),
            P(None, "fsdp"),
        ),
        check_vma=False,
    )
```

```python
import functools

import jax
import jax.numpy as jnp
from jax import lax
from jax.experimental import pallas as pl
from jax.experimental.pallas import tpu as pltpu
from jax.sharding import PartitionSpec as P

HEAD_SIZE = 128
QBLOCK = 64
SCALE_GROUP = 8


adapter_scale = 0.25


def dequantize_kernel(weight, absmax, out):
    rows, features = out.shape
    lane = lax.broadcasted_iota(jnp.int32, (rows, 2 * QBLOCK), 1)
    for i in range(features // (2 * QBLOCK)):
        columns = slice(2 * QBLOCK * i, 2 * QBLOCK * (i + 1))
        scale = jnp.where(
            lane < QBLOCK, absmax[:, 2 * i : 2 * i + 1], absmax[:, 2 * i + 1 : 2 * i + 2]
        )
        out[:, columns] = (weight[:, columns].astype(jnp.float32) * scale).astype(out.dtype)


def dequantize(normalized_weight, block_scale_codes, scale_group_factor, scale_group_offset):
    spread_scale = jnp.repeat(scale_group_factor, SCALE_GROUP, axis=0)
    spread_offset = jnp.repeat(scale_group_offset, SCALE_GROUP, axis=0)
    absmax = spread_scale * (block_scale_codes.astype(jnp.float32) + 1.0) / 256.0 + spread_offset
    weight = normalized_weight.T
    return pl.pallas_call(
        dequantize_kernel,
        out_shape=jax.ShapeDtypeStruct(weight.shape, jnp.bfloat16),
        compiler_params=pltpu.CompilerParams(vmem_limit_bytes=16 * 2**20),
    )(weight, absmax.T)


def attend(queries, keys, values, doc_lengths):
    tokens = queries.shape[0]
    head_count = queries.shape[1] // HEAD_SIZE
    query_heads = queries.reshape(tokens, head_count, HEAD_SIZE)
    key_heads = keys.reshape(tokens, head_count, HEAD_SIZE)
    value_heads = values.reshape(tokens, head_count, HEAD_SIZE)
    doc_ends = jnp.cumsum(doc_lengths)
    places = jnp.arange(tokens, dtype=jnp.int32)
    segment = jnp.sum((doc_ends[None, :] <= places[:, None]).astype(jnp.int32), axis=1)
    allowed = (segment[:, None] == segment[None, :]) & (places[None, :] <= places[:, None])
    scores = jnp.einsum(
        "qhe,khe->hqk", query_heads, key_heads, preferred_element_type=jnp.float32
    ) * HEAD_SIZE ** (-0.5)
    scores = jnp.where(allowed[None], scores, -jnp.inf)
    row_max = jnp.max(scores, axis=-1, keepdims=True)
    weights = jnp.exp(scores - row_max)
    total = jnp.sum(weights, axis=-1)
    summed = jnp.einsum(
        "hqk,khe->qhe",
        weights.astype(jnp.bfloat16),
        value_heads,
        preferred_element_type=jnp.float32,
    )
    return (
        (summed / jnp.transpose(total)[:, :, None])
        .astype(jnp.bfloat16)
        .reshape(tokens, head_count * HEAD_SIZE)
    )


MESH = pl.DeviceIdType.MESH


def ring_kernel(scatter, third, *refs):
    if scatter:
        block, parts, out, mine, sems, ring_send, ring_recv, row_send, row_recv = refs[:9]
        core_send, core_recv, part_send, part_recv = refs[9:]
    else:
        block, out, sems, ring_send, ring_recv, row_send, row_recv, core_send, core_recv = refs
    n = lax.axis_size("fsdp")
    chips = n // 2
    half = chips // 2
    row = lax.axis_index("dp")
    me = lax.axis_index("fsdp")
    chip, core = me // 2, me % 2
    place = jnp.where(chip % 2 == 0, chip // 2, chips - 1 - chip // 2)

    def device_at(where):
        where = (where + chips) % chips
        there = jnp.where(where < half, 2 * where, 2 * (chips - 1 - where) + 1)
        return 2 * there + core

    neighbour = (device_at(place + 1), device_at(place - 1))
    twin = 2 * chip + 1 - core
    other_row = row + 1 - 2 * (row % 2)
    parity = row % 2
    size = block.shape[0]
    own = (pl.ds(pl.multiple_of(parity * third, 16), third))
    others = (pl.ds(pl.multiple_of((1 - parity) * third, 16), third))
    rest = pl.ds(2 * third, size - 2 * third)
    segments = (own, rest)

    barrier = pltpu.get_barrier_semaphore()
    if scatter:
        for k in range(1, n):
            pl.semaphore_signal(barrier, inc=1, device_id={"fsdp": (me + k) % n}, device_id_type=MESH)
        pl.semaphore_signal(barrier, inc=1, device_id={"dp": other_row}, device_id_type=MESH)
        pl.semaphore_wait(barrier, n)
    else:
        for peer in (*neighbour, twin):
            pl.semaphore_signal(barrier, inc=1, device_id={"fsdp": peer}, device_id_type=MESH)
        pl.semaphore_signal(barrier, inc=1, device_id={"dp": other_row}, device_id_type=MESH)
        pl.semaphore_wait(barrier, 4)

    sent = []

    def send(src, dst, send_sem, recv_sem, target):
        copy = pltpu.make_async_remote_copy(
            src_ref=src, dst_ref=dst, send_sem=send_sem, recv_sem=recv_sem,
            device_id=target, device_id_type=MESH,
        )
        copy.start()
        sent.append(copy)

    def arrived(dst, recv_sem, send_sem):
        pltpu.make_async_remote_copy(
            src_ref=dst, dst_ref=dst, send_sem=send_sem, recv_sem=recv_sem,
            device_id={"fsdp": twin}, device_id_type=MESH,
        ).wait_recv()

    hops = ((half, half - 1), (half - 1, half))

    def ring(src, origin, way, seg, step):
        send(
            src, out.at[origin, segments[seg]], ring_send.at[way, seg, step],
            ring_recv.at[way, seg, step], {"fsdp": neighbour[way]},
        )

    for seg in range(2):
        for way in range(2):
            if hops[way][seg] >= 1:
                ring(block.at[segments[seg]], me, way, seg, 0)
    send(block, out.at[me], core_send.at[0, 0, 2], core_recv.at[0, 0, 2], {"fsdp": twin})
    if scatter:
        for k in range(1, n):
            to = (me + k) % n
            send(parts.at[to], mine.at[me], part_send.at[k], part_recv.at[k], {"fsdp": to})
    keep = pltpu.make_async_copy(block, out.at[me], sems.at[0])
    keep.start()
    if scatter:
        keep_part = pltpu.make_async_copy(parts.at[me], mine.at[me], sems.at[1])
        keep_part.start()

    def origin_of(way, step):
        return device_at(place - step if way == 0 else place + step)

    def to_twin(origin, rows, way, step, kind):
        send(
            out.at[origin, rows], out.at[origin, rows], core_send.at[way, step, kind],
            core_recv.at[way, step, kind], {"fsdp": twin},
        )

    def from_row(way, step):
        origin = origin_of(way, step)
        arrived(out.at[origin, others], row_recv.at[way, step], row_send.at[way, step])
        to_twin(origin, others, way, step, 2)

    for step in range(1, half + 1):
        for seg in range(2):
            for way in range(2):
                if step <= hops[way][seg]:
                    origin = origin_of(way, step)
                    rows = segments[seg]
                    view = out.at[origin, rows]
                    arrived(view, ring_recv.at[way, seg, step - 1], ring_send.at[way, seg, step - 1])
                    if step < hops[way][seg]:
                        ring(view, origin, way, seg, step)
                    if seg == 0:
                        send(
                            view, view, row_send.at[way, step], row_recv.at[way, step],
                            {"dp": other_row},
                        )
                    to_twin(origin, rows, way, step, seg)
        for way in range(2):
            if 1 <= step - 1 <= hops[way][0]:
                from_row(way, step - 1)
    for way in range(2):
        if 1 <= half <= hops[way][0]:
            from_row(way, half)

    arrived(out.at[twin], core_recv.at[0, 0, 2], core_send.at[0, 0, 2])
    for way in range(2):
        for step in range(1, half + 1):
            there = origin_of(way, step)
            origin = there + 1 - 2 * core
            for seg in range(2):
                if step <= hops[way][seg]:
                    arrived(
                        out.at[origin, segments[seg]], core_recv.at[way, step, seg],
                        core_send.at[way, step, seg],
                    )
            if step <= hops[way][0]:
                arrived(out.at[origin, others], core_recv.at[way, step, 2], core_send.at[way, step, 2])
    if scatter:
        for k in range(1, n):
            arrived(mine.at[(me + n - k) % n], part_recv.at[k], part_send.at[k])
        keep_part.wait()
    keep.wait()
    for copy in sent:
        copy.wait_send()


def ring_gather(block, collective_id, parts=None):
    n = lax.axis_size("fsdp")
    half = n // 4
    rows, width = block.shape
    third = (rows // 16 + 2) // 3 * 16
    scatter = parts is not None
    out_shape = [jax.ShapeDtypeStruct((n, rows, width), block.dtype)]
    any_spec = pl.BlockSpec(memory_space=pl.ANY)
    dma = pltpu.SemaphoreType.DMA
    scratch = [
        dma((2,)),
        dma((2, 2, half + 1)), dma((2, 2, half + 1)),
        dma((2, half + 1)), dma((2, half + 1)),
        dma((2, half + 1, 3)), dma((2, half + 1, 3)),
    ]
    operands = [block]
    if scatter:
        out_shape.append(jax.ShapeDtypeStruct(parts.shape, parts.dtype))
        scratch += [dma((n,)), dma((n,))]
        operands.append(parts)
    return pl.pallas_call(
        functools.partial(ring_kernel, scatter, third),
        out_shape=out_shape,
        in_specs=[pl.BlockSpec(memory_space=pltpu.VMEM)] * len(operands),
        out_specs=[any_spec] * len(out_shape),
        scratch_shapes=scratch,
        compiler_params=pltpu.CompilerParams(
            collective_id=collective_id, has_side_effects=True, vmem_limit_bytes=24 * 2**20
        ),
    )(*operands)


def row_sum_kernel(rows, share, out, landed, send_sems, recv_sems):
    me = lax.axis_index("dp")
    barrier = pltpu.get_barrier_semaphore()
    for k in range(1, rows):
        pl.semaphore_signal(barrier, inc=1, device_id={"dp": (me + k) % rows}, device_id_type=MESH)
    pl.semaphore_wait(barrier, rows - 1)
    copies = []
    for k in range(1, rows):
        copy = pltpu.make_async_remote_copy(
            src_ref=share, dst_ref=landed.at[me], send_sem=send_sems.at[k],
            recv_sem=recv_sems.at[k], device_id={"dp": (me + k) % rows}, device_id_type=MESH,
        )
        copy.start()
        copies.append(copy)
    keep = pltpu.make_async_copy(share, landed.at[me], send_sems.at[0])
    keep.start()
    for k in range(1, rows):
        pltpu.make_async_remote_copy(
            src_ref=share, dst_ref=landed.at[(me + rows - k) % rows], send_sem=send_sems.at[k],
            recv_sem=recv_sems.at[k], device_id={"dp": (me + k) % rows}, device_id_type=MESH,
        ).wait_recv()
    keep.wait()
    for copy in copies:
        copy.wait_send()
    total = landed[0]
    for k in range(1, rows):
        total = total + landed[k]
    out[...] = total


def sum_over_rows(share):
    rows = lax.axis_size("dp")
    vmem = pl.BlockSpec(memory_space=pltpu.VMEM)
    return pl.pallas_call(
        functools.partial(row_sum_kernel, rows),
        out_shape=jax.ShapeDtypeStruct(share.shape, share.dtype),
        in_specs=[vmem],
        out_specs=vmem,
        scratch_shapes=[
            pltpu.VMEM((rows, *share.shape), share.dtype),
            pltpu.SemaphoreType.DMA((rows,)),
            pltpu.SemaphoreType.DMA((rows,)),
        ],
        compiler_params=pltpu.CompilerParams(
            collective_id=2, has_side_effects=True, vmem_limit_bytes=16 * 2**20
        ),
    )(share)


def general_per_device(
    queries,
    keys,
    values,
    lengths,
    normalized_weight,
    block_scale_codes,
    scale_group_factor,
    scale_group_offset,
    adapter_down_weight,
    adapter_up_weight,
    cotangent,
):
    n = lax.axis_size("fsdp")
    row_index = lax.axis_index("dp")
    rank, down_width = adapter_down_weight.shape
    up_width = adapter_up_weight.shape[1]
    own_rows = down_width + up_width
    packed_rows = own_rows * rank // 128
    padded_rows = -(-packed_rows // 16) * 16

    def pack(x):
        x = x.reshape(*x.shape[:-2], packed_rows, 128)
        pad = [(0, 0)] * (x.ndim - 2) + [(0, padded_rows - packed_rows), (0, 0)]
        return jnp.pad(x, pad)

    def unpack(x):
        return x[..., :packed_rows, :].reshape(*x.shape[:-2], own_rows, rank)

    own_lengths = lax.dynamic_index_in_dim(lengths[0], row_index, 0, keepdims=False)
    own_adapters = jnp.concatenate([adapter_up_weight.T, adapter_down_weight.T], axis=0)
    (adapters,) = ring_gather(pack(own_adapters), 0)
    adapters = unpack(adapters)
    up_rows = adapters[:, :up_width].reshape(n * up_width, rank)
    down_rows = adapters[:, up_width:].reshape(n * down_width, rank)

    attention_output = attend(queries, keys, values, own_lengths)
    reduced_activation = jnp.dot(
        attention_output, down_rows, preferred_element_type=jnp.float32
    ).astype(jnp.bfloat16)
    reduced_gradient = (
        adapter_scale * jnp.dot(cotangent, up_rows, preferred_element_type=jnp.float32)
    ).astype(jnp.bfloat16)
    down_part = jnp.dot(attention_output.T, reduced_gradient, preferred_element_type=jnp.float32)
    up_part = adapter_scale * jnp.dot(
        cotangent.T, reduced_activation, preferred_element_type=jnp.float32
    )
    parts = jnp.concatenate(
        [up_part.reshape(n, up_width, rank), down_part.reshape(n, down_width, rank)], axis=1
    ).astype(jnp.bfloat16)

    local_base = dequantize(
        normalized_weight, block_scale_codes, scale_group_factor, scale_group_offset
    )
    gathered, shares = ring_gather(local_base, 1, pack(parts))
    base_rows = gathered.reshape(-1, gathered.shape[2])
    share = unpack(sum_over_rows(jnp.sum(shares.astype(jnp.float32), axis=0)))

    product = lax.dot_general(
        attention_output, base_rows, (((1,), (1,)), ((), ())), preferred_element_type=jnp.float32
    )
    projection_output = (
        product
        + adapter_scale
        * lax.dot_general(
            reduced_activation, up_rows, (((1,), (1,)), ((), ())),
            preferred_element_type=jnp.float32,
        )
    ).astype(jnp.bfloat16)
    attention_gradient = (
        jnp.dot(cotangent, base_rows, preferred_element_type=jnp.float32)
        + lax.dot_general(
            reduced_gradient, down_rows, (((1,), (1,)), ((), ())),
            preferred_element_type=jnp.float32,
        )
    ).astype(jnp.bfloat16)
    return (projection_output, attention_gradient, share[up_width:].T, share[:up_width].T)


LANES = 128
TILE = 256
A, RA, RB, AD, Y = range(5)
WHOLE = A


def dot(a, b, contract):
    return lax.dot_general(
        a, b, ((contract[:1], contract[1:]), ((), ())), preferred_element_type=jnp.float32
    )


def down_window(down_width):
    step = 2 * down_width // LANES * LANES
    return 4 * down_width - step, step


def fused_kernel(
    lengths, weight_hbm, codes_hbm, factor_hbm, offset_hbm, down_hbm, up_hbm, queries, keys,
    values, cotangent_hbm,
    projection_output, attention_gradient, up_out, down_out,
    base, packed, adapters, down_rows, weight, codes, factor, offset, down, up, q, k, v, cot, attended, bias, mixed, low_rank,
    low_grad, product, gradient, part, part_twin, part_row, landed_row, part_chip,
    landed_side, part_line, landed_line,
    final, local_sem, ring_send, ring_recv, row_send, row_recv, twin_send, twin_recv, sum_send,
    sum_recv,
):
    n = lax.axis_size("fsdp")
    chips = n // 2
    half = chips // 2
    row = lax.axis_index("dp")
    me = lax.axis_index("fsdp")
    chip, core = me // 2, me % 2
    tokens, features = attended.shape
    model = cot.shape[1]
    rank, width = up.shape
    down_width = down.shape[1]
    pair = 2 * width
    quad = 4 * down_width
    window, window_step = down_window(down_width)
    block = pair + window
    tiles = features // TILE
    a_tiles = 3 * tiles // 10
    r_tiles = (tiles - 2 * a_tiles) // 2
    place = jnp.where(chip % 2 == 0, chip // 2, chips - 1 - chip // 2)
    twin = 2 * chip + 1 - core
    other_row = 1 - row
    sense = 1 - 2 * core

    def chip_at(where):
        where = (where + 2 * chips) % chips
        return jnp.where(where < half, 2 * where, 2 * (chips - 1 - where) + 1)

    def behind(step):
        return chip_at(place - sense * step)

    def ahead(step):
        return chip_at(place + sense * step)

    barrier = pltpu.get_barrier_semaphore()
    peers = (
        {"fsdp": 2 * ahead(1) + core}, {"fsdp": 2 * behind(1) + core}, {"fsdp": twin},
        {"dp": other_row},
    )
    for peer in peers:
        pl.semaphore_signal(barrier, inc=1, device_id=peer, device_id_type=MESH)

    loads = [
        pltpu.make_async_copy(src, dst, local_sem.at[i])
        for i, (src, dst) in enumerate(
            (
                (codes_hbm, codes), (factor_hbm, factor), (offset_hbm, offset),
                (weight_hbm, weight), (up_hbm, up), (down_hbm, down), (queries, q), (keys, k),
                (values, v), (cotangent_hbm, cot),
            )
        )
    ]
    for load in loads:
        load.start()

    sent = []

    def send(src, dst, send_sem, recv_sem, target):
        copy = pltpu.make_async_remote_copy(
            src_ref=src, dst_ref=dst, send_sem=send_sem, recv_sem=recv_sem,
            device_id=target, device_id_type=MESH,
        )
        copy.start()
        sent.append(copy)

    def arrived(dst, send_sem, recv_sem):
        pltpu.make_async_remote_copy(
            src_ref=dst, dst_ref=dst, send_sem=send_sem, recv_sem=recv_sem,
            device_id={"fsdp": twin}, device_id_type=MESH,
        ).wait_recv()

    def rows_of(origin):
        return pl.ds(pl.multiple_of(origin * width, 64), width)

    packed_width = (width + down_width) // 2

    def packed_rows_of(origin):
        return pl.ds(pl.multiple_of(origin * packed_width, 16), packed_width)

    def tiles_of(kind):
        if kind == A:
            return row * a_tiles, a_tiles
        if kind == Y:
            return (1 - row) * a_tiles, a_tiles
        if kind == RA:
            return 2 * a_tiles, r_tiles
        return 2 * a_tiles + r_tiles, tiles - 2 * a_tiles - r_tiles

    def piece(origin, kind):
        if kind == AD:
            return packed.at[packed_rows_of(origin)]
        first, count = tiles_of(kind)
        return base.at[rows_of(origin), pl.ds(pl.multiple_of(first * TILE, TILE), count * TILE)]

    def shard(origin_chip, side):
        return 2 * origin_chip + (core if side == 0 else 1 - core)

    def ring(step, kind, sides=(0, 1)):
        far = (ahead if kind == AD else behind)(step - 1)
        to = (behind if kind == AD else ahead)(1)
        for side in sides:
            view = piece(shard(far, side), kind)
            send(
                view, view, ring_send.at[step, kind, side], ring_recv.at[step, kind, side],
                {"fsdp": 2 * to + core},
            )

    def to_twin(view, step, kind, side):
        send(
            view, view, twin_send.at[step, kind, side], twin_recv.at[step, kind, side],
            {"fsdp": twin},
        )

    def ring_in(step, kind, sides=(0, 1)):
        for side in sides:
            view = piece(shard((ahead if kind == AD else behind)(step), side), kind)
            arrived(view, ring_send.at[step, kind, side], ring_recv.at[step, kind, side])
            to_twin(view, step, kind, side)
            if kind == A:
                send(
                    view, view, row_send.at[step, side], row_recv.at[step, side],
                    {"dp": other_row},
                )

    def row_in(step, sides=(0, 1)):
        for side in sides:
            view = piece(shard(behind(step), side), Y)
            arrived(view, row_send.at[step, side], row_recv.at[step, side])
            to_twin(view, step, Y, side)

    def twin_in(step, *kinds, sides=(0, 1)):
        for kind in kinds:
            for side in sides:
                far = (behind if kind == AD else ahead)(step) if step else chip
                arrived(
                    piece(shard(far, 1 - side), kind), twin_send.at[step, kind, side],
                    twin_recv.at[step, kind, side],
                )

    own_rows = rows_of(me)
    groups = factor.shape[0]
    span = SCALE_GROUP * QBLOCK
    shape = (3 * SCALE_GROUP, span)
    spread = (
        lax.broadcasted_iota(jnp.int32, shape, 0) % SCALE_GROUP
        == lax.broadcasted_iota(jnp.int32, shape, 1) // QBLOCK
    ).astype(jnp.bfloat16)

    def dequantize_group(g):
        eight = pl.ds(pl.multiple_of(SCALE_GROUP * g, SCALE_GROUP), SCALE_GROUP)
        absmax = (
            factor[pl.ds(g, 1), :] * (codes[eight, :].astype(jnp.float32) + 1.0) / 256.0
            + offset[pl.ds(g, 1), :]
        )
        high = absmax.astype(jnp.bfloat16).astype(jnp.float32)
        middle = (absmax - high).astype(jnp.bfloat16).astype(jnp.float32)
        parts = jnp.concatenate([high, middle, absmax - high - middle], axis=0)
        columns = pl.ds(pl.multiple_of(span * g, span), span)
        base[own_rows, columns] = (
            weight[:, columns].astype(jnp.float32)
            * dot(parts.astype(jnp.bfloat16), spread, (0, 0))
        ).astype(base.dtype)

    for load in loads[:4]:
        load.wait()
    ahead_groups = -(-a_tiles * TILE // span)
    for i in range(ahead_groups):
        dequantize_group(row * (a_tiles * TILE // span) + i)
    pl.semaphore_wait(barrier, len(peers))
    ring(1, A, (0,))
    def picked(columns, shift):
        shape = (packed_width, columns)
        return (
            lax.broadcasted_iota(jnp.int32, shape, 0) + shift
            == lax.broadcasted_iota(jnp.int32, shape, 1)
        ).astype(jnp.bfloat16)

    for load in loads[4:6]:
        load.wait()
    up_low = jnp.concatenate([up[...], jnp.zeros((LANES - rank, width), up.dtype)], axis=0)
    up_high = jnp.concatenate([jnp.zeros((LANES - rank, width), up.dtype), up[...]], axis=0)
    down_high = jnp.concatenate(
        [jnp.zeros((LANES - rank, down_width), down.dtype), down[...]], axis=0
    )
    left = width - packed_width
    own_ad, own_base = packed.at[packed_rows_of(me)], base.at[own_rows]
    own_ad[...] = (
        dot(picked(width, 0), up_low, (1, 1))
        + dot(picked(width, packed_width), up_high, (1, 1))
        + dot(picked(down_width, -left), down_high, (1, 1))
    ).astype(packed.dtype)
    ring(1, AD, (0,))
    to_twin(own_ad, 0, AD, 0)

    for i in range(groups - ahead_groups):
        lead = row * (a_tiles * TILE // span)
        dequantize_group(jnp.where(i < lead, i, i + ahead_groups))
    to_twin(own_base, 0, WHOLE, 0)

    ends = []
    for j in range(lengths.shape[2]):
        ends.append(lengths[0, row, j] + (ends[-1] if ends else 0))
    at = lax.broadcasted_iota(jnp.int32, (tokens, tokens), 0)
    to = lax.broadcasted_iota(jnp.int32, (tokens, tokens), 1)
    segment_at = sum((at >= end).astype(jnp.int32) for end in ends)
    segment_to = sum((to >= end).astype(jnp.int32) for end in ends)
    bias[...] = jnp.where((segment_at == segment_to) & (to <= at), 0.0, -jnp.inf)
    for load in loads[6:9]:
        load.wait()

    head_count = features // HEAD_SIZE
    per_loop = 2

    def heads(first, count):
        @pl.loop(first // per_loop, (first + count) // per_loop)
        def _(i):
            for j in range(per_loop):
                columns = pl.ds(
                    pl.multiple_of((i * per_loop + j) * HEAD_SIZE, HEAD_SIZE), HEAD_SIZE
                )
                scores = dot(q[:, columns], k[:, columns], (1, 1)) * HEAD_SIZE ** (-0.5)
                scores = scores + bias[...]
                weights = jnp.exp(scores - jnp.max(scores, axis=-1, keepdims=True))
                total = jnp.sum(weights, axis=-1, keepdims=True)
                summed = dot(weights.astype(jnp.bfloat16), v[:, columns], (1, 0))
                attended[:, columns] = (summed / total).astype(attended.dtype)

    def accumulate(there, *kinds):
        columns = pl.ds(pl.multiple_of(there * pair, LANES), pair)
        for first, count in kinds:
            @pl.loop(first, first + count)
            def _(i):
                some = pl.ds(pl.multiple_of(i * TILE, TILE), TILE)
                rows = base[columns, some]
                gradient[:, some] += dot(cot[:, columns], rows, (1, 0))
                product[:, columns] += dot(attended[:, some], rows, (1, 1))

    share = head_count // 10 * 2
    arrived(packed.at[packed_rows_of(twin)], twin_send.at[0, AD, 0], twin_recv.at[0, AD, 0])
    ring(1, AD, (1,))
    arrived(base.at[rows_of(twin)], twin_send.at[0, WHOLE, 0], twin_recv.at[0, WHOLE, 0])
    ring(1, A, (1,))
    ring(1, RA)
    heads(0, share)
    ring_in(1, AD)
    ring(2, AD)
    heads(share, share)
    ring_in(1, A)
    ring(2, A)
    ring(1, RB)
    ring_in(2, AD)
    ring(3, AD)
    heads(2 * share, share)
    ring_in(3, AD)
    ring(4, AD, (0,))
    heads(3 * share, head_count - 3 * share)
    ring_in(1, RA)
    ring_in(4, AD, (0,))
    for step in range(1, half):
        twin_in(step, AD)
    twin_in(half, AD, sides=(0,))
    loads[9].wait()

    @pl.loop(0, n)
    def _(f):
        both = packed[packed_rows_of(f), :]
        start = f * width
        adapters[pl.ds(pl.multiple_of(start, 16), packed_width), :] = both
        adapters[pl.ds(pl.multiple_of(start + packed_width, 16), left), :] = pltpu.roll(
            both[:left].astype(jnp.float32), rank, 1
        ).astype(adapters.dtype)
        down_rows[pl.ds(pl.multiple_of(f * down_width, 16), down_width), :] = both[left:]

    lane = lax.broadcasted_iota(jnp.int32, (tokens, LANES), 1)
    activation = dot(attended[...], down_rows[...], (1, 0))
    grads = adapter_scale * dot(cot[...], adapters[...], (1, 0))
    both = jnp.where(lane < rank, pltpu.roll(activation, rank, 1), pltpu.roll(grads, rank, 1))
    both = both.astype(jnp.bfloat16)
    mixed[...] = both
    nothing = jnp.zeros_like(both)
    low_rank[...] = jnp.where(lane < rank, both * jnp.bfloat16(adapter_scale), nothing)
    low_grad[...] = jnp.where(lane < rank, nothing, both)
    chunk = pair

    @pl.loop(0, model // chunk)
    def _(i):
        columns = pl.ds(pl.multiple_of(i * chunk, LANES), chunk)
        both = mixed[...]
        part[:, columns] = (
            adapter_scale * dot(both, cot[:, columns], (0, 0))[:rank]
        ).astype(part.dtype)

    @pl.loop(0, features // chunk)
    def _(i):
        columns = pl.ds(pl.multiple_of(i * chunk, LANES), chunk)
        there = pl.ds(pl.multiple_of(model + i * chunk, LANES), chunk)
        both = mixed[...]
        part[:, there] = dot(both, attended[:, columns], (0, 0))[rank:].astype(part.dtype)

    per_core = rank // 2
    per_row = per_core // 2
    theirs = pl.ds(pl.multiple_of((1 - core) * per_core, per_core), per_core)
    send(part.at[theirs], part_twin, sum_send.at[0], sum_recv.at[0], {"fsdp": twin})

    ring_in(2, A)
    ring(3, A)
    ring(2, RA)
    row_in(1)

    @pl.loop(0, model // pair)
    def _(i):
        columns = pl.ds(pl.multiple_of(i * pair, LANES), pair)
        product[:, columns] = dot(low_rank[...], adapters[columns, :], (1, 1))

    @pl.loop(0, tiles)
    def _(i):
        some = pl.ds(pl.multiple_of(i * TILE, TILE), TILE)
        gradient[:, some] = dot(low_grad[...], down_rows[some, :], (1, 1))

    arrived(part_twin, sum_send.at[0], sum_recv.at[0])
    away = pl.ds(pl.multiple_of(core * per_core + (1 - row) * per_row, per_row), per_row)
    away_twin = pl.ds(pl.multiple_of((1 - row) * per_row, per_row), per_row)
    kept = pl.ds(pl.multiple_of(core * per_core + row * per_row, per_row), per_row)
    kept_twin = pl.ds(pl.multiple_of(row * per_row, per_row), per_row)

    @pl.loop(0, (model + features) // chunk)
    def _(i):
        columns = pl.ds(pl.multiple_of(i * chunk, LANES), chunk)
        part_row[:, columns] = (
            part[away, columns].astype(jnp.float32)
            + part_twin[away_twin, columns].astype(jnp.float32)
        ).astype(part_row.dtype)

    send(part_row, landed_row, sum_send.at[1], sum_recv.at[1], {"dp": other_row})

    accumulate(chip, (0, tiles))
    ring_in(1, RB)
    accumulate(behind(1), (0, tiles))
    twin_in(1, A, RA, RB, Y)
    accumulate(ahead(1), (0, tiles))

    ring_in(3, A)
    ring(4, A, (0,))
    ring(2, RB)
    ring_in(2, RA)
    ring(3, RA)

    arrived(landed_row, sum_send.at[1], sum_recv.at[1])

    def row_sum(columns):
        return (
            part[kept, columns].astype(jnp.float32)
            + part_twin[kept_twin, columns].astype(jnp.float32)
            + landed_row[:, columns].astype(jnp.float32)
        ).astype(part_chip.dtype)

    side, line = chip % 2, chip // 2

    @pl.loop(0, chips)
    def _(i):
        part_chip[i % 2, i // 2, :, :pair] = row_sum(
            pl.ds(pl.multiple_of(i * pair, LANES), pair)
        )
        part_chip[i % 2, i // 2, :, pair:] = row_sum(
            pl.ds(
                pl.multiple_of(model + i // 2 * quad + i % 2 * window_step, LANES), window
            )
        )

    beside = 2 * (2 * line + 1 - side) + core
    send(part_chip.at[1 - side], landed_side, sum_send.at[2], sum_recv.at[2], {"fsdp": beside})

    row_in(2)
    most = (0, 2 * a_tiles + r_tiles)
    accumulate(behind(2), most)
    twin_in(2, A, RA, Y)
    accumulate(ahead(2), most)
    ring_in(4, A, (0,))

    ring_in(2, RB)
    ring(3, RB)

    arrived(landed_side, sum_send.at[2], sum_recv.at[2])

    @pl.loop(0, half)
    def _(i):
        part_line[i] = (
            part_chip[side, i].astype(jnp.float32) + landed_side[i].astype(jnp.float32)
        ).astype(part_line.dtype)

    for d in range(1, half):
        there = (line + d) % half
        send(
            part_line.at[there], landed_line.at[d], sum_send.at[2 + d], sum_recv.at[2 + d],
            {"fsdp": 2 * (2 * there + side) + core},
        )

    accumulate(behind(2), tiles_of(RB))
    twin_in(2, RB)
    accumulate(ahead(2), tiles_of(RB))
    ring_in(3, RA)
    ring(4, RA, (0,))
    accumulate(behind(3), tiles_of(A), tiles_of(RA))
    row_in(3)
    ring_in(3, RB)
    ring(4, RB, (0,))
    accumulate(behind(3), tiles_of(Y), tiles_of(RB))

    total = part_chip[side, line].astype(jnp.float32) + landed_side[line].astype(jnp.float32)
    for d in range(1, half):
        arrived(landed_line.at[d], sum_send.at[2 + d], sum_recv.at[2 + d])
        total = total + landed_line[d].astype(jnp.float32)
    own = 2 * core + row
    final[own] = total
    targets = ({"fsdp": twin}, {"dp": other_row}, {"dp": other_row, "fsdp": twin})
    for i, target in enumerate(targets):
        send(
            final.at[own], final.at[own], sum_send.at[2 + half + i],
            sum_recv.at[2 + half + i], target,
        )

    twin_in(3, A, RA, Y)
    accumulate(ahead(3), most)
    twin_in(3, RB)
    accumulate(ahead(3), tiles_of(RB))
    row_in(4, (0,))
    ring_in(4, RA, (0,))
    twin_in(4, A, Y, RA, sides=(0,))
    accumulate(behind(4), most)

    owners = (2 * (1 - core) + row, 2 * core + 1 - row, 2 * (1 - core) + 1 - row)
    for i, owner in enumerate(owners):
        arrived(final.at[owner], sum_send.at[2 + half + i], sum_recv.at[2 + half + i])
    ranks = final[...].reshape(rank, block)
    up_cols, down_cols = ranks[:, :pair], ranks[:, pair:]
    up_cols = jnp.where(core == 0, up_cols, pltpu.roll(up_cols, pair - width, 1))
    up_out[...] = up_cols[:, :width]
    turned = down_cols
    for j in range(1, 4):
        first = j * down_width - j // 2 * window_step
        turned = jnp.where(me % 4 == j, pltpu.roll(down_cols, window - first, 1), turned)
    down_out[...] = turned[:, :down_width]

    def project(there):
        columns = pl.ds(pl.multiple_of(there * pair, LANES), pair)
        projection_output[:, columns] = product[:, columns].astype(projection_output.dtype)

    first, count = tiles_of(RB)

    def convert(i):
        some = pl.ds(pl.multiple_of(i * TILE, TILE), TILE)
        attention_gradient[:, some] = gradient[:, some].astype(attention_gradient.dtype)

    @pl.loop(1, chips)
    def _(i):
        project((behind(half) + i) % chips)

    pl.loop(0, first)(convert)
    ring_in(4, RB, (0,))
    twin_in(4, RB, sides=(0,))
    accumulate(behind(4), tiles_of(RB))
    project(behind(half))
    pl.loop(first, first + count)(convert)
    for copy in sent:
        copy.wait_send()


def finish_kernel(count, *refs):
    copies = []
    for i in range(count):
        rows = refs[i].shape[0]
        cuts = 4 if i < 2 else 1
        for j in range(cuts):
            some = pl.ds(rows // cuts * j, rows // cuts)
            copies.append(
                pltpu.make_async_copy(
                    refs[i].at[some], refs[count + i].at[some], refs[-1].at[len(copies)]
                )
            )
    for copy in copies:
        copy.start()
    for copy in copies:
        copy.wait()


def finish(*results):
    return pl.pallas_call(
        functools.partial(finish_kernel, len(results)),
        out_shape=[jax.ShapeDtypeStruct(x.shape, x.dtype) for x in results],
        in_specs=[pl.BlockSpec(memory_space=pltpu.VMEM)] * len(results),
        out_specs=[pl.BlockSpec(memory_space=pl.ANY)] * len(results),
        scratch_shapes=[pltpu.SemaphoreType.DMA((12,))],
        compiler_params=pltpu.CompilerParams(vmem_limit_bytes=8 * 2**20),
    )(*results)


def fused_per_device(
    queries,
    keys,
    values,
    lengths,
    normalized_weight,
    block_scale_codes,
    scale_group_factor,
    scale_group_offset,
    adapter_down_weight,
    adapter_up_weight,
    cotangent,
):
    n = lax.axis_size("fsdp")
    chips = n // 2
    half = chips // 2
    tokens, features = queries.shape
    model = cotangent.shape[1]
    rank, width = adapter_up_weight.shape
    down_width = adapter_down_weight.shape[1]
    block = 2 * width + down_window(down_width)[0]
    low, full = jnp.bfloat16, jnp.float32
    dma = pltpu.SemaphoreType.DMA
    hbm = pl.BlockSpec(memory_space=pl.ANY)
    shapes = lambda *s: pltpu.VMEM(s[:-1], s[-1])
    sums = 2 + half + 4
    return tuple(
        pl.pallas_call(
            fused_kernel,
            out_shape=[
                shapes(tokens, model, low),
                shapes(tokens, features, low),
                shapes(rank, width, full),
                shapes(rank, down_width, full),
            ],
            in_specs=[pl.BlockSpec(memory_space=pltpu.SMEM)] + [hbm] * 10,
            out_specs=[pl.BlockSpec(memory_space=pltpu.VMEM)] * 4,
            scratch_shapes=[
                shapes(n * width, features, low),
                shapes(n * (width + down_width) // 2, LANES, low),
                shapes(n * width, LANES, low),
                shapes(features, LANES, low),
                shapes(width, features, low),
                shapes(features // QBLOCK, width, jnp.int32),
                shapes(features // (QBLOCK * SCALE_GROUP), width, full),
                shapes(features // (QBLOCK * SCALE_GROUP), width, full),
                shapes(rank, down_width, low),
                shapes(rank, width, low),
                shapes(tokens, features, low),
                shapes(tokens, features, low),
                shapes(tokens, features, low),
                shapes(tokens, model, low),
                shapes(tokens, features, low),
                shapes(tokens, tokens, full),
                shapes(tokens, LANES, low),
                shapes(tokens, LANES, low),
                shapes(tokens, LANES, low),
                shapes(tokens, model, full),
                shapes(tokens, features, full),
                shapes(rank, model + features, low),
                shapes(rank // 2, model + features, low),
                shapes(rank // 4, model + features, low),
                shapes(rank // 4, model + features, low),
                shapes(2, half, rank // 4, block, low),
                shapes(half, rank // 4, block, low),
                shapes(half, rank // 4, block, low),
                shapes(half, rank // 4, block, low),
                shapes(4, rank // 4, block, full),
                dma((10,)),
                dma((half + 1, 4, 2)),
                dma((half + 1, 4, 2)),
                dma((half + 1, 2)),
                dma((half + 1, 2)),
                dma((half + 1, 5, 2)),
                dma((half + 1, 5, 2)),
                dma((sums,)),
                dma((sums,)),
            ],
            compiler_params=pltpu.CompilerParams(
                collective_id=3, has_side_effects=True, vmem_limit_bytes=60 * 2**20
            ),
        )(
            lengths, normalized_weight.T, block_scale_codes, scale_group_factor,
            scale_group_offset, adapter_down_weight, adapter_up_weight, queries, keys, values,
            cotangent,
        )
    )


def per_device(*operands):
    projection_output, attention_gradient, up_gradient, down_gradient = finish(
        *fused_per_device(*operands)
    )
    return projection_output, attention_gradient, down_gradient, up_gradient


def fused_fits(mesh):
    return mesh.shape["dp"] == 2 and mesh.shape["fsdp"] == 16


def solution(mesh):
    return jax.shard_map(
        per_device if fused_fits(mesh) else general_per_device,
        mesh=mesh,
        in_specs=(
            P(("dp", "fsdp"), None),
            P(("dp", "fsdp"), None),
            P(("dp", "fsdp"), None),
            P("fsdp", None, None),
            P(None, "fsdp"),
            P(None, "fsdp"),
            P(None, "fsdp"),
            P(None, "fsdp"),
            P(None, "fsdp"),
            P(None, "fsdp"),
            P(("dp", "fsdp"), None),
        ),
        out_specs=(
            P(("dp", "fsdp"), None),
            P(("dp", "fsdp"), None),
            P(None, "fsdp"),
            P(None, "fsdp"),
        ),
        check_vma=False,
    )
```

```python
import functools

import jax
import jax.numpy as jnp
from jax import lax
from jax.experimental import pallas as pl
from jax.experimental.pallas import tpu as pltpu
from jax.sharding import PartitionSpec as P

HEAD_SIZE = 128
QBLOCK = 64
SCALE_GROUP = 8


adapter_scale = 0.25


def dequantize_kernel(weight, absmax, out):
    rows, features = out.shape
    lane = lax.broadcasted_iota(jnp.int32, (rows, 2 * QBLOCK), 1)
    for i in range(features // (2 * QBLOCK)):
        columns = slice(2 * QBLOCK * i, 2 * QBLOCK * (i + 1))
        scale = jnp.where(
            lane < QBLOCK, absmax[:, 2 * i : 2 * i + 1], absmax[:, 2 * i + 1 : 2 * i + 2]
        )
        out[:, columns] = (weight[:, columns].astype(jnp.float32) * scale).astype(out.dtype)


def dequantize(normalized_weight, block_scale_codes, scale_group_factor, scale_group_offset):
    spread_scale = jnp.repeat(scale_group_factor, SCALE_GROUP, axis=0)
    spread_offset = jnp.repeat(scale_group_offset, SCALE_GROUP, axis=0)
    absmax = spread_scale * (block_scale_codes.astype(jnp.float32) + 1.0) / 256.0 + spread_offset
    weight = normalized_weight.T
    return pl.pallas_call(
        dequantize_kernel,
        out_shape=jax.ShapeDtypeStruct(weight.shape, jnp.bfloat16),
        compiler_params=pltpu.CompilerParams(vmem_limit_bytes=16 * 2**20),
    )(weight, absmax.T)


def attend(queries, keys, values, doc_lengths):
    tokens = queries.shape[0]
    head_count = queries.shape[1] // HEAD_SIZE
    query_heads = queries.reshape(tokens, head_count, HEAD_SIZE)
    key_heads = keys.reshape(tokens, head_count, HEAD_SIZE)
    value_heads = values.reshape(tokens, head_count, HEAD_SIZE)
    doc_ends = jnp.cumsum(doc_lengths)
    places = jnp.arange(tokens, dtype=jnp.int32)
    segment = jnp.sum((doc_ends[None, :] <= places[:, None]).astype(jnp.int32), axis=1)
    allowed = (segment[:, None] == segment[None, :]) & (places[None, :] <= places[:, None])
    scores = jnp.einsum(
        "qhe,khe->hqk", query_heads, key_heads, preferred_element_type=jnp.float32
    ) * HEAD_SIZE ** (-0.5)
    scores = jnp.where(allowed[None], scores, -jnp.inf)
    row_max = jnp.max(scores, axis=-1, keepdims=True)
    weights = jnp.exp(scores - row_max)
    total = jnp.sum(weights, axis=-1)
    summed = jnp.einsum(
        "hqk,khe->qhe",
        weights.astype(jnp.bfloat16),
        value_heads,
        preferred_element_type=jnp.float32,
    )
    return (
        (summed / jnp.transpose(total)[:, :, None])
        .astype(jnp.bfloat16)
        .reshape(tokens, head_count * HEAD_SIZE)
    )


MESH = pl.DeviceIdType.MESH


def ring_kernel(scatter, third, *refs):
    if scatter:
        block, parts, out, mine, sems, ring_send, ring_recv, row_send, row_recv = refs[:9]
        core_send, core_recv, part_send, part_recv = refs[9:]
    else:
        block, out, sems, ring_send, ring_recv, row_send, row_recv, core_send, core_recv = refs
    n = lax.axis_size("fsdp")
    chips = n // 2
    half = chips // 2
    row = lax.axis_index("dp")
    me = lax.axis_index("fsdp")
    chip, core = me // 2, me % 2
    place = jnp.where(chip % 2 == 0, chip // 2, chips - 1 - chip // 2)

    def device_at(where):
        where = (where + chips) % chips
        there = jnp.where(where < half, 2 * where, 2 * (chips - 1 - where) + 1)
        return 2 * there + core

    neighbour = (device_at(place + 1), device_at(place - 1))
    twin = 2 * chip + 1 - core
    other_row = row + 1 - 2 * (row % 2)
    parity = row % 2
    size = block.shape[0]
    own = (pl.ds(pl.multiple_of(parity * third, 16), third))
    others = (pl.ds(pl.multiple_of((1 - parity) * third, 16), third))
    rest = pl.ds(2 * third, size - 2 * third)
    segments = (own, rest)

    barrier = pltpu.get_barrier_semaphore()
    if scatter:
        for k in range(1, n):
            pl.semaphore_signal(barrier, inc=1, device_id={"fsdp": (me + k) % n}, device_id_type=MESH)
        pl.semaphore_signal(barrier, inc=1, device_id={"dp": other_row}, device_id_type=MESH)
        pl.semaphore_wait(barrier, n)
    else:
        for peer in (*neighbour, twin):
            pl.semaphore_signal(barrier, inc=1, device_id={"fsdp": peer}, device_id_type=MESH)
        pl.semaphore_signal(barrier, inc=1, device_id={"dp": other_row}, device_id_type=MESH)
        pl.semaphore_wait(barrier, 4)

    sent = []

    def send(src, dst, send_sem, recv_sem, target):
        copy = pltpu.make_async_remote_copy(
            src_ref=src, dst_ref=dst, send_sem=send_sem, recv_sem=recv_sem,
            device_id=target, device_id_type=MESH,
        )
        copy.start()
        sent.append(copy)

    def arrived(dst, recv_sem, send_sem):
        pltpu.make_async_remote_copy(
            src_ref=dst, dst_ref=dst, send_sem=send_sem, recv_sem=recv_sem,
            device_id={"fsdp": twin}, device_id_type=MESH,
        ).wait_recv()

    hops = ((half, half - 1), (half - 1, half))

    def ring(src, origin, way, seg, step):
        send(
            src, out.at[origin, segments[seg]], ring_send.at[way, seg, step],
            ring_recv.at[way, seg, step], {"fsdp": neighbour[way]},
        )

    for seg in range(2):
        for way in range(2):
            if hops[way][seg] >= 1:
                ring(block.at[segments[seg]], me, way, seg, 0)
    send(block, out.at[me], core_send.at[0, 0, 2], core_recv.at[0, 0, 2], {"fsdp": twin})
    if scatter:
        for k in range(1, n):
            to = (me + k) % n
            send(parts.at[to], mine.at[me], part_send.at[k], part_recv.at[k], {"fsdp": to})
    keep = pltpu.make_async_copy(block, out.at[me], sems.at[0])
    keep.start()
    if scatter:
        keep_part = pltpu.make_async_copy(parts.at[me], mine.at[me], sems.at[1])
        keep_part.start()

    def origin_of(way, step):
        return device_at(place - step if way == 0 else place + step)

    def to_twin(origin, rows, way, step, kind):
        send(
            out.at[origin, rows], out.at[origin, rows], core_send.at[way, step, kind],
            core_recv.at[way, step, kind], {"fsdp": twin},
        )

    def from_row(way, step):
        origin = origin_of(way, step)
        arrived(out.at[origin, others], row_recv.at[way, step], row_send.at[way, step])
        to_twin(origin, others, way, step, 2)

    for step in range(1, half + 1):
        for seg in range(2):
            for way in range(2):
                if step <= hops[way][seg]:
                    origin = origin_of(way, step)
                    rows = segments[seg]
                    view = out.at[origin, rows]
                    arrived(view, ring_recv.at[way, seg, step - 1], ring_send.at[way, seg, step - 1])
                    if step < hops[way][seg]:
                        ring(view, origin, way, seg, step)
                    if seg == 0:
                        send(
                            view, view, row_send.at[way, step], row_recv.at[way, step],
                            {"dp": other_row},
                        )
                    to_twin(origin, rows, way, step, seg)
        for way in range(2):
            if 1 <= step - 1 <= hops[way][0]:
                from_row(way, step - 1)
    for way in range(2):
        if 1 <= half <= hops[way][0]:
            from_row(way, half)

    arrived(out.at[twin], core_recv.at[0, 0, 2], core_send.at[0, 0, 2])
    for way in range(2):
        for step in range(1, half + 1):
            there = origin_of(way, step)
            origin = there + 1 - 2 * core
            for seg in range(2):
                if step <= hops[way][seg]:
                    arrived(
                        out.at[origin, segments[seg]], core_recv.at[way, step, seg],
                        core_send.at[way, step, seg],
                    )
            if step <= hops[way][0]:
                arrived(out.at[origin, others], core_recv.at[way, step, 2], core_send.at[way, step, 2])
    if scatter:
        for k in range(1, n):
            arrived(mine.at[(me + n - k) % n], part_recv.at[k], part_send.at[k])
        keep_part.wait()
    keep.wait()
    for copy in sent:
        copy.wait_send()


def ring_gather(block, collective_id, parts=None):
    n = lax.axis_size("fsdp")
    half = n // 4
    rows, width = block.shape
    third = (rows // 16 + 2) // 3 * 16
    scatter = parts is not None
    out_shape = [jax.ShapeDtypeStruct((n, rows, width), block.dtype)]
    any_spec = pl.BlockSpec(memory_space=pl.ANY)
    dma = pltpu.SemaphoreType.DMA
    scratch = [
        dma((2,)),
        dma((2, 2, half + 1)), dma((2, 2, half + 1)),
        dma((2, half + 1)), dma((2, half + 1)),
        dma((2, half + 1, 3)), dma((2, half + 1, 3)),
    ]
    operands = [block]
    if scatter:
        out_shape.append(jax.ShapeDtypeStruct(parts.shape, parts.dtype))
        scratch += [dma((n,)), dma((n,))]
        operands.append(parts)
    return pl.pallas_call(
        functools.partial(ring_kernel, scatter, third),
        out_shape=out_shape,
        in_specs=[pl.BlockSpec(memory_space=pltpu.VMEM)] * len(operands),
        out_specs=[any_spec] * len(out_shape),
        scratch_shapes=scratch,
        compiler_params=pltpu.CompilerParams(
            collective_id=collective_id, has_side_effects=True, vmem_limit_bytes=24 * 2**20
        ),
    )(*operands)


def row_sum_kernel(rows, share, out, landed, send_sems, recv_sems):
    me = lax.axis_index("dp")
    barrier = pltpu.get_barrier_semaphore()
    for k in range(1, rows):
        pl.semaphore_signal(barrier, inc=1, device_id={"dp": (me + k) % rows}, device_id_type=MESH)
    pl.semaphore_wait(barrier, rows - 1)
    copies = []
    for k in range(1, rows):
        copy = pltpu.make_async_remote_copy(
            src_ref=share, dst_ref=landed.at[me], send_sem=send_sems.at[k],
            recv_sem=recv_sems.at[k], device_id={"dp": (me + k) % rows}, device_id_type=MESH,
        )
        copy.start()
        copies.append(copy)
    keep = pltpu.make_async_copy(share, landed.at[me], send_sems.at[0])
    keep.start()
    for k in range(1, rows):
        pltpu.make_async_remote_copy(
            src_ref=share, dst_ref=landed.at[(me + rows - k) % rows], send_sem=send_sems.at[k],
            recv_sem=recv_sems.at[k], device_id={"dp": (me + k) % rows}, device_id_type=MESH,
        ).wait_recv()
    keep.wait()
    for copy in copies:
        copy.wait_send()
    total = landed[0]
    for k in range(1, rows):
        total = total + landed[k]
    out[...] = total


def sum_over_rows(share):
    rows = lax.axis_size("dp")
    vmem = pl.BlockSpec(memory_space=pltpu.VMEM)
    return pl.pallas_call(
        functools.partial(row_sum_kernel, rows),
        out_shape=jax.ShapeDtypeStruct(share.shape, share.dtype),
        in_specs=[vmem],
        out_specs=vmem,
        scratch_shapes=[
            pltpu.VMEM((rows, *share.shape), share.dtype),
            pltpu.SemaphoreType.DMA((rows,)),
            pltpu.SemaphoreType.DMA((rows,)),
        ],
        compiler_params=pltpu.CompilerParams(
            collective_id=2, has_side_effects=True, vmem_limit_bytes=16 * 2**20
        ),
    )(share)


def general_per_device(
    queries,
    keys,
    values,
    lengths,
    normalized_weight,
    block_scale_codes,
    scale_group_factor,
    scale_group_offset,
    adapter_down_weight,
    adapter_up_weight,
    cotangent,
):
    n = lax.axis_size("fsdp")
    row_index = lax.axis_index("dp")
    rank, down_width = adapter_down_weight.shape
    up_width = adapter_up_weight.shape[1]
    own_rows = down_width + up_width
    packed_rows = own_rows * rank // 128
    padded_rows = -(-packed_rows // 16) * 16

    def pack(x):
        x = x.reshape(*x.shape[:-2], packed_rows, 128)
        pad = [(0, 0)] * (x.ndim - 2) + [(0, padded_rows - packed_rows), (0, 0)]
        return jnp.pad(x, pad)

    def unpack(x):
        return x[..., :packed_rows, :].reshape(*x.shape[:-2], own_rows, rank)

    own_lengths = lax.dynamic_index_in_dim(lengths[0], row_index, 0, keepdims=False)
    own_adapters = jnp.concatenate([adapter_up_weight.T, adapter_down_weight.T], axis=0)
    (adapters,) = ring_gather(pack(own_adapters), 0)
    adapters = unpack(adapters)
    up_rows = adapters[:, :up_width].reshape(n * up_width, rank)
    down_rows = adapters[:, up_width:].reshape(n * down_width, rank)

    attention_output = attend(queries, keys, values, own_lengths)
    reduced_activation = jnp.dot(
        attention_output, down_rows, preferred_element_type=jnp.float32
    ).astype(jnp.bfloat16)
    reduced_gradient = (
        adapter_scale * jnp.dot(cotangent, up_rows, preferred_element_type=jnp.float32)
    ).astype(jnp.bfloat16)
    down_part = jnp.dot(attention_output.T, reduced_gradient, preferred_element_type=jnp.float32)
    up_part = adapter_scale * jnp.dot(
        cotangent.T, reduced_activation, preferred_element_type=jnp.float32
    )
    parts = jnp.concatenate(
        [up_part.reshape(n, up_width, rank), down_part.reshape(n, down_width, rank)], axis=1
    ).astype(jnp.bfloat16)

    local_base = dequantize(
        normalized_weight, block_scale_codes, scale_group_factor, scale_group_offset
    )
    gathered, shares = ring_gather(local_base, 1, pack(parts))
    base_rows = gathered.reshape(-1, gathered.shape[2])
    share = unpack(sum_over_rows(jnp.sum(shares.astype(jnp.float32), axis=0)))

    product = lax.dot_general(
        attention_output, base_rows, (((1,), (1,)), ((), ())), preferred_element_type=jnp.float32
    )
    projection_output = (
        product
        + adapter_scale
        * lax.dot_general(
            reduced_activation, up_rows, (((1,), (1,)), ((), ())),
            preferred_element_type=jnp.float32,
        )
    ).astype(jnp.bfloat16)
    attention_gradient = (
        jnp.dot(cotangent, base_rows, preferred_element_type=jnp.float32)
        + lax.dot_general(
            reduced_gradient, down_rows, (((1,), (1,)), ((), ())),
            preferred_element_type=jnp.float32,
        )
    ).astype(jnp.bfloat16)
    return (projection_output, attention_gradient, share[up_width:].T, share[:up_width].T)


LANES = 128
TILE = 256
A, RA, RB, AD, Y = range(5)
WHOLE = A


def dot(a, b, contract):
    return lax.dot_general(
        a, b, ((contract[:1], contract[1:]), ((), ())), preferred_element_type=jnp.float32
    )


def down_window(down_width):
    step = 2 * down_width // LANES * LANES
    return 4 * down_width - step, step


def fused_kernel(
    lengths, weight_hbm, codes_hbm, factor_hbm, offset_hbm, down_hbm, up_hbm, queries, keys,
    values, cotangent_hbm,
    projection_output, attention_gradient, up_out, down_out,
    base, packed, adapters, down_rows, weight, codes, factor, offset, down, up, q, k, v, cot, attended, bias, mixed, low_rank,
    low_grad, product, gradient, part, part_twin, part_row, landed_row, part_chip,
    landed_side, part_line, landed_line,
    final, local_sem, ring_send, ring_recv, row_send, row_recv, twin_send, twin_recv, sum_send,
    sum_recv,
):
    n = lax.axis_size("fsdp")
    chips = n // 2
    half = chips // 2
    row = lax.axis_index("dp")
    me = lax.axis_index("fsdp")
    chip, core = me // 2, me % 2
    tokens, features = attended.shape
    model = cot.shape[1]
    rank, width = up.shape
    down_width = down.shape[1]
    pair = 2 * width
    quad = 4 * down_width
    window, window_step = down_window(down_width)
    block = pair + window
    tiles = features // TILE
    a_tiles = 3 * tiles // 10
    r_tiles = (tiles - 2 * a_tiles) // 2
    place = jnp.where(chip % 2 == 0, chip // 2, chips - 1 - chip // 2)
    twin = 2 * chip + 1 - core
    other_row = 1 - row
    sense = 1 - 2 * core

    def chip_at(where):
        where = (where + 2 * chips) % chips
        return jnp.where(where < half, 2 * where, 2 * (chips - 1 - where) + 1)

    def behind(step):
        return chip_at(place - sense * step)

    def ahead(step):
        return chip_at(place + sense * step)

    barrier = pltpu.get_barrier_semaphore()
    peers = (
        {"fsdp": 2 * ahead(1) + core}, {"fsdp": 2 * behind(1) + core}, {"fsdp": twin},
        {"dp": other_row},
    )
    for peer in peers:
        pl.semaphore_signal(barrier, inc=1, device_id=peer, device_id_type=MESH)

    loads = [
        pltpu.make_async_copy(src, dst, local_sem.at[i])
        for i, (src, dst) in enumerate(
            (
                (codes_hbm, codes), (factor_hbm, factor), (offset_hbm, offset),
                (weight_hbm, weight), (up_hbm, up), (down_hbm, down), (queries, q), (keys, k),
                (values, v), (cotangent_hbm, cot),
            )
        )
    ]
    for load in loads:
        load.start()

    sent = []

    def send(src, dst, send_sem, recv_sem, target):
        copy = pltpu.make_async_remote_copy(
            src_ref=src, dst_ref=dst, send_sem=send_sem, recv_sem=recv_sem,
            device_id=target, device_id_type=MESH,
        )
        copy.start()
        sent.append(copy)

    def arrived(dst, send_sem, recv_sem):
        pltpu.make_async_remote_copy(
            src_ref=dst, dst_ref=dst, send_sem=send_sem, recv_sem=recv_sem,
            device_id={"fsdp": twin}, device_id_type=MESH,
        ).wait_recv()

    def rows_of(origin):
        return pl.ds(pl.multiple_of(origin * width, 64), width)

    packed_width = (width + down_width) // 2

    def packed_rows_of(origin):
        return pl.ds(pl.multiple_of(origin * packed_width, 16), packed_width)

    def tiles_of(kind):
        if kind == A:
            return row * a_tiles, a_tiles
        if kind == Y:
            return (1 - row) * a_tiles, a_tiles
        if kind == RA:
            return 2 * a_tiles, r_tiles
        return 2 * a_tiles + r_tiles, tiles - 2 * a_tiles - r_tiles

    def piece(origin, kind):
        if kind == AD:
            return packed.at[packed_rows_of(origin)]
        first, count = tiles_of(kind)
        return base.at[rows_of(origin), pl.ds(pl.multiple_of(first * TILE, TILE), count * TILE)]

    def shard(origin_chip, side):
        return 2 * origin_chip + (core if side == 0 else 1 - core)

    def ring(step, kind, sides=(0, 1)):
        far = (ahead if kind == AD else behind)(step - 1)
        to = (behind if kind == AD else ahead)(1)
        for side in sides:
            view = piece(shard(far, side), kind)
            send(
                view, view, ring_send.at[step, kind, side], ring_recv.at[step, kind, side],
                {"fsdp": 2 * to + core},
            )

    def to_twin(view, step, kind, side):
        send(
            view, view, twin_send.at[step, kind, side], twin_recv.at[step, kind, side],
            {"fsdp": twin},
        )

    def ring_in(step, kind, sides=(0, 1)):
        for side in sides:
            view = piece(shard((ahead if kind == AD else behind)(step), side), kind)
            arrived(view, ring_send.at[step, kind, side], ring_recv.at[step, kind, side])
            to_twin(view, step, kind, side)
            if kind == A:
                send(
                    view, view, row_send.at[step, side], row_recv.at[step, side],
                    {"dp": other_row},
                )

    def row_in(step, sides=(0, 1)):
        for side in sides:
            view = piece(shard(behind(step), side), Y)
            arrived(view, row_send.at[step, side], row_recv.at[step, side])
            to_twin(view, step, Y, side)

    def twin_in(step, *kinds, sides=(0, 1)):
        for kind in kinds:
            for side in sides:
                far = (behind if kind == AD else ahead)(step) if step else chip
                arrived(
                    piece(shard(far, 1 - side), kind), twin_send.at[step, kind, side],
                    twin_recv.at[step, kind, side],
                )

    own_rows = rows_of(me)
    groups = factor.shape[0]
    span = SCALE_GROUP * QBLOCK
    shape = (3 * SCALE_GROUP, span)
    spread = (
        lax.broadcasted_iota(jnp.int32, shape, 0) % SCALE_GROUP
        == lax.broadcasted_iota(jnp.int32, shape, 1) // QBLOCK
    ).astype(jnp.bfloat16)

    def dequantize_group(g):
        eight = pl.ds(pl.multiple_of(SCALE_GROUP * g, SCALE_GROUP), SCALE_GROUP)
        absmax = (
            factor[pl.ds(g, 1), :] * (codes[eight, :].astype(jnp.float32) + 1.0) / 256.0
            + offset[pl.ds(g, 1), :]
        )
        high = absmax.astype(jnp.bfloat16).astype(jnp.float32)
        middle = (absmax - high).astype(jnp.bfloat16).astype(jnp.float32)
        parts = jnp.concatenate([high, middle, absmax - high - middle], axis=0)
        columns = pl.ds(pl.multiple_of(span * g, span), span)
        base[own_rows, columns] = (
            weight[:, columns].astype(jnp.float32)
            * dot(parts.astype(jnp.bfloat16), spread, (0, 0))
        ).astype(base.dtype)

    for load in loads[:4]:
        load.wait()
    ahead_groups = -(-a_tiles * TILE // span)
    for i in range(ahead_groups):
        dequantize_group(row * (a_tiles * TILE // span) + i)
    pl.semaphore_wait(barrier, len(peers))
    ring(1, A, (0,))
    def picked(columns, shift):
        shape = (packed_width, columns)
        return (
            lax.broadcasted_iota(jnp.int32, shape, 0) + shift
            == lax.broadcasted_iota(jnp.int32, shape, 1)
        ).astype(jnp.bfloat16)

    for load in loads[4:6]:
        load.wait()
    up_low = jnp.concatenate([up[...], jnp.zeros((LANES - rank, width), up.dtype)], axis=0)
    up_high = jnp.concatenate([jnp.zeros((LANES - rank, width), up.dtype), up[...]], axis=0)
    down_high = jnp.concatenate(
        [jnp.zeros((LANES - rank, down_width), down.dtype), down[...]], axis=0
    )
    left = width - packed_width
    own_ad, own_base = packed.at[packed_rows_of(me)], base.at[own_rows]
    own_ad[...] = (
        dot(picked(width, 0), up_low, (1, 1))
        + dot(picked(width, packed_width), up_high, (1, 1))
        + dot(picked(down_width, -left), down_high, (1, 1))
    ).astype(packed.dtype)
    ring(1, AD, (0,))
    to_twin(own_ad, 0, AD, 0)

    for i in range(groups - ahead_groups):
        lead = row * (a_tiles * TILE // span)
        dequantize_group(jnp.where(i < lead, i, i + ahead_groups))
    to_twin(own_base, 0, WHOLE, 0)

    ends = []
    for j in range(lengths.shape[2]):
        ends.append(lengths[0, row, j] + (ends[-1] if ends else 0))
    at = lax.broadcasted_iota(jnp.int32, (tokens, tokens), 0)
    to = lax.broadcasted_iota(jnp.int32, (tokens, tokens), 1)
    segment_at = sum((at >= end).astype(jnp.int32) for end in ends)
    segment_to = sum((to >= end).astype(jnp.int32) for end in ends)
    bias[...] = jnp.where((segment_at == segment_to) & (to <= at), 0.0, -jnp.inf)
    for load in loads[6:9]:
        load.wait()

    head_count = features // HEAD_SIZE
    per_loop = 2

    def heads(first, count):
        @pl.loop(first // per_loop, (first + count) // per_loop)
        def _(i):
            for j in range(per_loop):
                columns = pl.ds(
                    pl.multiple_of((i * per_loop + j) * HEAD_SIZE, HEAD_SIZE), HEAD_SIZE
                )
                scores = dot(q[:, columns], k[:, columns], (1, 1)) * HEAD_SIZE ** (-0.5)
                scores = scores + bias[...]
                weights = jnp.exp(scores - jnp.max(scores, axis=-1, keepdims=True))
                total = jnp.sum(weights, axis=-1, keepdims=True)
                summed = dot(weights.astype(jnp.bfloat16), v[:, columns], (1, 0))
                attended[:, columns] = (summed / total).astype(attended.dtype)

    def accumulate(there, *kinds):
        columns = pl.ds(pl.multiple_of(there * pair, LANES), pair)
        for first, count in kinds:
            @pl.loop(first, first + count)
            def _(i):
                some = pl.ds(pl.multiple_of(i * TILE, TILE), TILE)
                rows = base[columns, some]
                gradient[:, some] += dot(cot[:, columns], rows, (1, 0))
                product[:, columns] += dot(attended[:, some], rows, (1, 1))

    share = head_count // 10 * 2
    arrived(packed.at[packed_rows_of(twin)], twin_send.at[0, AD, 0], twin_recv.at[0, AD, 0])
    ring(1, AD, (1,))
    arrived(base.at[rows_of(twin)], twin_send.at[0, WHOLE, 0], twin_recv.at[0, WHOLE, 0])
    ring(1, A, (1,))
    ring(1, RA)
    heads(0, share)
    ring_in(1, AD)
    ring(2, AD)
    heads(share, share)
    ring_in(1, A)
    ring(2, A)
    ring(1, RB)
    ring_in(2, AD)
    ring(3, AD)
    heads(2 * share, share)
    ring_in(3, AD)
    ring(4, AD, (0,))
    heads(3 * share, head_count - 3 * share)
    ring_in(1, RA)
    ring_in(4, AD, (0,))
    for step in range(1, half):
        twin_in(step, AD)
    twin_in(half, AD, sides=(0,))
    loads[9].wait()

    @pl.loop(0, n)
    def _(f):
        both = packed[packed_rows_of(f), :]
        start = f * width
        adapters[pl.ds(pl.multiple_of(start, 16), packed_width), :] = both
        adapters[pl.ds(pl.multiple_of(start + packed_width, 16), left), :] = pltpu.roll(
            both[:left].astype(jnp.float32), rank, 1
        ).astype(adapters.dtype)
        down_rows[pl.ds(pl.multiple_of(f * down_width, 16), down_width), :] = both[left:]

    lane = lax.broadcasted_iota(jnp.int32, (tokens, LANES), 1)
    activation = dot(attended[...], down_rows[...], (1, 0))
    grads = adapter_scale * dot(cot[...], adapters[...], (1, 0))
    both = jnp.where(lane < rank, pltpu.roll(activation, rank, 1), pltpu.roll(grads, rank, 1))
    both = both.astype(jnp.bfloat16)
    mixed[...] = both
    nothing = jnp.zeros_like(both)
    low_rank[...] = jnp.where(lane < rank, both * jnp.bfloat16(adapter_scale), nothing)
    low_grad[...] = jnp.where(lane < rank, nothing, both)
    chunk = pair

    @pl.loop(0, model // chunk)
    def _(i):
        columns = pl.ds(pl.multiple_of(i * chunk, LANES), chunk)
        both = mixed[...]
        part[:, columns] = (
            adapter_scale * dot(both, cot[:, columns], (0, 0))[:rank]
        ).astype(part.dtype)

    @pl.loop(0, features // chunk)
    def _(i):
        columns = pl.ds(pl.multiple_of(i * chunk, LANES), chunk)
        there = pl.ds(pl.multiple_of(model + i * chunk, LANES), chunk)
        both = mixed[...]
        part[:, there] = dot(both, attended[:, columns], (0, 0))[rank:].astype(part.dtype)

    per_core = rank // 2
    per_row = per_core // 2
    theirs = pl.ds(pl.multiple_of((1 - core) * per_core, per_core), per_core)
    send(part.at[theirs], part_twin, sum_send.at[0], sum_recv.at[0], {"fsdp": twin})

    ring_in(2, A)
    ring(3, A)
    ring(2, RA)
    row_in(1)

    @pl.loop(0, model // pair)
    def _(i):
        columns = pl.ds(pl.multiple_of(i * pair, LANES), pair)
        product[:, columns] = dot(low_rank[...], adapters[columns, :], (1, 1))

    @pl.loop(0, tiles)
    def _(i):
        some = pl.ds(pl.multiple_of(i * TILE, TILE), TILE)
        gradient[:, some] = dot(low_grad[...], down_rows[some, :], (1, 1))

    arrived(part_twin, sum_send.at[0], sum_recv.at[0])
    away = pl.ds(pl.multiple_of(core * per_core + (1 - row) * per_row, per_row), per_row)
    away_twin = pl.ds(pl.multiple_of((1 - row) * per_row, per_row), per_row)
    kept = pl.ds(pl.multiple_of(core * per_core + row * per_row, per_row), per_row)
    kept_twin = pl.ds(pl.multiple_of(row * per_row, per_row), per_row)

    @pl.loop(0, (model + features) // chunk)
    def _(i):
        columns = pl.ds(pl.multiple_of(i * chunk, LANES), chunk)
        part_row[:, columns] = (
            part[away, columns].astype(jnp.float32)
            + part_twin[away_twin, columns].astype(jnp.float32)
        ).astype(part_row.dtype)

    send(part_row, landed_row, sum_send.at[1], sum_recv.at[1], {"dp": other_row})

    accumulate(chip, (0, tiles))
    ring_in(1, RB)
    accumulate(behind(1), (0, tiles))
    twin_in(1, A, RA, RB, Y)
    accumulate(ahead(1), (0, tiles))

    ring_in(3, A)
    ring(4, A, (0,))
    ring(2, RB)
    ring_in(2, RA)
    ring(3, RA)

    arrived(landed_row, sum_send.at[1], sum_recv.at[1])

    def row_sum(columns):
        return (
            part[kept, columns].astype(jnp.float32)
            + part_twin[kept_twin, columns].astype(jnp.float32)
            + landed_row[:, columns].astype(jnp.float32)
        ).astype(part_chip.dtype)

    side, line = chip % 2, chip // 2

    @pl.loop(0, chips)
    def _(i):
        part_chip[i % 2, i // 2, :, :pair] = row_sum(
            pl.ds(pl.multiple_of(i * pair, LANES), pair)
        )
        part_chip[i % 2, i // 2, :, pair:] = row_sum(
            pl.ds(
                pl.multiple_of(model + i // 2 * quad + i % 2 * window_step, LANES), window
            )
        )

    beside = 2 * (2 * line + 1 - side) + core
    send(part_chip.at[1 - side], landed_side, sum_send.at[2], sum_recv.at[2], {"fsdp": beside})

    row_in(2)
    most = (0, 2 * a_tiles + r_tiles)
    accumulate(behind(2), most)
    twin_in(2, A, RA, Y)
    accumulate(ahead(2), most)
    ring_in(4, A, (0,))

    ring_in(2, RB)
    ring(3, RB)

    arrived(landed_side, sum_send.at[2], sum_recv.at[2])

    @pl.loop(0, half)
    def _(i):
        part_line[i] = (
            part_chip[side, i].astype(jnp.float32) + landed_side[i].astype(jnp.float32)
        ).astype(part_line.dtype)

    for d in range(1, half):
        there = (line + d) % half
        send(
            part_line.at[there], landed_line.at[d], sum_send.at[2 + d], sum_recv.at[2 + d],
            {"fsdp": 2 * (2 * there + side) + core},
        )

    accumulate(behind(2), tiles_of(RB))
    twin_in(2, RB)
    accumulate(ahead(2), tiles_of(RB))
    accumulate(behind(3), tiles_of(A))
    twin_in(3, A)
    accumulate(ahead(3), tiles_of(A))
    twin_in(4, A, sides=(0,))
    accumulate(behind(4), tiles_of(A))
    ring_in(3, RA)
    ring(4, RA, (0,))
    accumulate(behind(3), tiles_of(RA))
    twin_in(3, RA)
    accumulate(ahead(3), tiles_of(RA))

    def project(there):
        columns = pl.ds(pl.multiple_of(there * pair, LANES), pair)
        projection_output[:, columns] = product[:, columns].astype(projection_output.dtype)

    @pl.loop(0, chips - 3)
    def _(i):
        project(chip_at(place + 2 - i))

    ring_in(3, RB)
    ring(4, RB, (0,))
    accumulate(behind(3), tiles_of(RB))
    row_in(3)
    accumulate(behind(3), tiles_of(Y))

    total = part_chip[side, line].astype(jnp.float32) + landed_side[line].astype(jnp.float32)
    for d in range(1, half):
        arrived(landed_line.at[d], sum_send.at[2 + d], sum_recv.at[2 + d])
        total = total + landed_line[d].astype(jnp.float32)
    own = 2 * core + row
    final[own] = total
    targets = ({"fsdp": twin}, {"dp": other_row}, {"dp": other_row, "fsdp": twin})
    for i, target in enumerate(targets):
        send(
            final.at[own], final.at[own], sum_send.at[2 + half + i],
            sum_recv.at[2 + half + i], target,
        )

    twin_in(3, RB, Y)
    accumulate(ahead(3), tiles_of(RB), tiles_of(Y))
    project(behind(3))
    project(ahead(3))
    row_in(4, (0,))
    ring_in(4, RA, (0,))
    twin_in(4, Y, RA, sides=(0,))
    accumulate(behind(4), tiles_of(Y), tiles_of(RA))

    first, count = tiles_of(RB)

    def convert(i):
        some = pl.ds(pl.multiple_of(i * TILE, TILE), TILE)
        attention_gradient[:, some] = gradient[:, some].astype(attention_gradient.dtype)

    pl.loop(0, first)(convert)
    ring_in(4, RB, (0,))
    twin_in(4, RB, sides=(0,))
    accumulate(behind(4), tiles_of(RB))
    project(behind(half))
    pl.loop(first, first + count)(convert)
    owners = (2 * (1 - core) + row, 2 * core + 1 - row, 2 * (1 - core) + 1 - row)
    for i, owner in enumerate(owners):
        arrived(final.at[owner], sum_send.at[2 + half + i], sum_recv.at[2 + half + i])
    ranks = final[...].reshape(rank, block)
    up_cols, down_cols = ranks[:, :pair], ranks[:, pair:]
    up_cols = jnp.where(core == 0, up_cols, pltpu.roll(up_cols, pair - width, 1))
    up_out[...] = up_cols[:, :width]
    turned = down_cols
    for j in range(1, 4):
        first = j * down_width - j // 2 * window_step
        turned = jnp.where(me % 4 == j, pltpu.roll(down_cols, window - first, 1), turned)
    down_out[...] = turned[:, :down_width]
    for copy in sent:
        copy.wait_send()


def finish_kernel(count, *refs):
    copies = []
    for i in range(count):
        rows = refs[i].shape[0]
        cuts = 4 if i < 2 else 1
        for j in range(cuts):
            some = pl.ds(rows // cuts * j, rows // cuts)
            copies.append(
                pltpu.make_async_copy(
                    refs[i].at[some], refs[count + i].at[some], refs[-1].at[len(copies)]
                )
            )
    for copy in copies:
        copy.start()
    for copy in copies:
        copy.wait()


def finish(*results):
    return pl.pallas_call(
        functools.partial(finish_kernel, len(results)),
        out_shape=[jax.ShapeDtypeStruct(x.shape, x.dtype) for x in results],
        in_specs=[pl.BlockSpec(memory_space=pltpu.VMEM)] * len(results),
        out_specs=[pl.BlockSpec(memory_space=pl.ANY)] * len(results),
        scratch_shapes=[pltpu.SemaphoreType.DMA((12,))],
        compiler_params=pltpu.CompilerParams(vmem_limit_bytes=8 * 2**20),
    )(*results)


def fused_per_device(
    queries,
    keys,
    values,
    lengths,
    normalized_weight,
    block_scale_codes,
    scale_group_factor,
    scale_group_offset,
    adapter_down_weight,
    adapter_up_weight,
    cotangent,
):
    n = lax.axis_size("fsdp")
    chips = n // 2
    half = chips // 2
    tokens, features = queries.shape
    model = cotangent.shape[1]
    rank, width = adapter_up_weight.shape
    down_width = adapter_down_weight.shape[1]
    block = 2 * width + down_window(down_width)[0]
    low, full = jnp.bfloat16, jnp.float32
    dma = pltpu.SemaphoreType.DMA
    hbm = pl.BlockSpec(memory_space=pl.ANY)
    shapes = lambda *s: pltpu.VMEM(s[:-1], s[-1])
    sums = 2 + half + 4
    return tuple(
        pl.pallas_call(
            fused_kernel,
            out_shape=[
                shapes(tokens, model, low),
                shapes(tokens, features, low),
                shapes(rank, width, full),
                shapes(rank, down_width, full),
            ],
            in_specs=[pl.BlockSpec(memory_space=pltpu.SMEM)] + [hbm] * 10,
            out_specs=[pl.BlockSpec(memory_space=pltpu.VMEM)] * 4,
            scratch_shapes=[
                shapes(n * width, features, low),
                shapes(n * (width + down_width) // 2, LANES, low),
                shapes(n * width, LANES, low),
                shapes(features, LANES, low),
                shapes(width, features, low),
                shapes(features // QBLOCK, width, jnp.int32),
                shapes(features // (QBLOCK * SCALE_GROUP), width, full),
                shapes(features // (QBLOCK * SCALE_GROUP), width, full),
                shapes(rank, down_width, low),
                shapes(rank, width, low),
                shapes(tokens, features, low),
                shapes(tokens, features, low),
                shapes(tokens, features, low),
                shapes(tokens, model, low),
                shapes(tokens, features, low),
                shapes(tokens, tokens, full),
                shapes(tokens, LANES, low),
                shapes(tokens, LANES, low),
                shapes(tokens, LANES, low),
                shapes(tokens, model, full),
                shapes(tokens, features, full),
                shapes(rank, model + features, low),
                shapes(rank // 2, model + features, low),
                shapes(rank // 4, model + features, low),
                shapes(rank // 4, model + features, low),
                shapes(2, half, rank // 4, block, low),
                shapes(half, rank // 4, block, low),
                shapes(half, rank // 4, block, low),
                shapes(half, rank // 4, block, low),
                shapes(4, rank // 4, block, full),
                dma((10,)),
                dma((half + 1, 4, 2)),
                dma((half + 1, 4, 2)),
                dma((half + 1, 2)),
                dma((half + 1, 2)),
                dma((half + 1, 5, 2)),
                dma((half + 1, 5, 2)),
                dma((sums,)),
                dma((sums,)),
            ],
            compiler_params=pltpu.CompilerParams(
                collective_id=3, has_side_effects=True, vmem_limit_bytes=60 * 2**20
            ),
        )(
            lengths, normalized_weight.T, block_scale_codes, scale_group_factor,
            scale_group_offset, adapter_down_weight, adapter_up_weight, queries, keys, values,
            cotangent,
        )
    )


def per_device(*operands):
    projection_output, attention_gradient, up_gradient, down_gradient = finish(
        *fused_per_device(*operands)
    )
    return projection_output, attention_gradient, down_gradient, up_gradient


def fused_fits(mesh):
    return mesh.shape["dp"] == 2 and mesh.shape["fsdp"] == 16


def solution(mesh):
    return jax.shard_map(
        per_device if fused_fits(mesh) else general_per_device,
        mesh=mesh,
        in_specs=(
            P(("dp", "fsdp"), None),
            P(("dp", "fsdp"), None),
            P(("dp", "fsdp"), None),
            P("fsdp", None, None),
            P(None, "fsdp"),
            P(None, "fsdp"),
            P(None, "fsdp"),
            P(None, "fsdp"),
            P(None, "fsdp"),
            P(None, "fsdp"),
            P(("dp", "fsdp"), None),
        ),
        out_specs=(
            P(("dp", "fsdp"), None),
            P(("dp", "fsdp"), None),
            P(None, "fsdp"),
            P(None, "fsdp"),
        ),
        check_vma=False,
    )
```

```python
import functools

import jax
import jax.numpy as jnp
from jax import lax
from jax.experimental import pallas as pl
from jax.experimental.pallas import tpu as pltpu
from jax.sharding import PartitionSpec as P

HEAD_SIZE = 128
QBLOCK = 64
SCALE_GROUP = 8


adapter_scale = 0.25


def dequantize_kernel(weight, absmax, out):
    rows, features = out.shape
    lane = lax.broadcasted_iota(jnp.int32, (rows, 2 * QBLOCK), 1)
    for i in range(features // (2 * QBLOCK)):
        columns = slice(2 * QBLOCK * i, 2 * QBLOCK * (i + 1))
        scale = jnp.where(
            lane < QBLOCK, absmax[:, 2 * i : 2 * i + 1], absmax[:, 2 * i + 1 : 2 * i + 2]
        )
        out[:, columns] = (weight[:, columns].astype(jnp.float32) * scale).astype(out.dtype)


def dequantize(normalized_weight, block_scale_codes, scale_group_factor, scale_group_offset):
    spread_scale = jnp.repeat(scale_group_factor, SCALE_GROUP, axis=0)
    spread_offset = jnp.repeat(scale_group_offset, SCALE_GROUP, axis=0)
    absmax = spread_scale * (block_scale_codes.astype(jnp.float32) + 1.0) / 256.0 + spread_offset
    weight = normalized_weight.T
    return pl.pallas_call(
        dequantize_kernel,
        out_shape=jax.ShapeDtypeStruct(weight.shape, jnp.bfloat16),
        compiler_params=pltpu.CompilerParams(vmem_limit_bytes=16 * 2**20),
    )(weight, absmax.T)


def attend(queries, keys, values, doc_lengths):
    tokens = queries.shape[0]
    head_count = queries.shape[1] // HEAD_SIZE
    query_heads = queries.reshape(tokens, head_count, HEAD_SIZE)
    key_heads = keys.reshape(tokens, head_count, HEAD_SIZE)
    value_heads = values.reshape(tokens, head_count, HEAD_SIZE)
    doc_ends = jnp.cumsum(doc_lengths)
    places = jnp.arange(tokens, dtype=jnp.int32)
    segment = jnp.sum((doc_ends[None, :] <= places[:, None]).astype(jnp.int32), axis=1)
    allowed = (segment[:, None] == segment[None, :]) & (places[None, :] <= places[:, None])
    scores = jnp.einsum(
        "qhe,khe->hqk", query_heads, key_heads, preferred_element_type=jnp.float32
    ) * HEAD_SIZE ** (-0.5)
    scores = jnp.where(allowed[None], scores, -jnp.inf)
    row_max = jnp.max(scores, axis=-1, keepdims=True)
    weights = jnp.exp(scores - row_max)
    total = jnp.sum(weights, axis=-1)
    summed = jnp.einsum(
        "hqk,khe->qhe",
        weights.astype(jnp.bfloat16),
        value_heads,
        preferred_element_type=jnp.float32,
    )
    return (
        (summed / jnp.transpose(total)[:, :, None])
        .astype(jnp.bfloat16)
        .reshape(tokens, head_count * HEAD_SIZE)
    )


MESH = pl.DeviceIdType.MESH


def ring_kernel(scatter, third, *refs):
    if scatter:
        block, parts, out, mine, sems, ring_send, ring_recv, row_send, row_recv = refs[:9]
        core_send, core_recv, part_send, part_recv = refs[9:]
    else:
        block, out, sems, ring_send, ring_recv, row_send, row_recv, core_send, core_recv = refs
    n = lax.axis_size("fsdp")
    chips = n // 2
    half = chips // 2
    row = lax.axis_index("dp")
    me = lax.axis_index("fsdp")
    chip, core = me // 2, me % 2
    place = jnp.where(chip % 2 == 0, chip // 2, chips - 1 - chip // 2)

    def device_at(where):
        where = (where + chips) % chips
        there = jnp.where(where < half, 2 * where, 2 * (chips - 1 - where) + 1)
        return 2 * there + core

    neighbour = (device_at(place + 1), device_at(place - 1))
    twin = 2 * chip + 1 - core
    other_row = row + 1 - 2 * (row % 2)
    parity = row % 2
    size = block.shape[0]
    own = (pl.ds(pl.multiple_of(parity * third, 16), third))
    others = (pl.ds(pl.multiple_of((1 - parity) * third, 16), third))
    rest = pl.ds(2 * third, size - 2 * third)
    segments = (own, rest)

    barrier = pltpu.get_barrier_semaphore()
    if scatter:
        for k in range(1, n):
            pl.semaphore_signal(barrier, inc=1, device_id={"fsdp": (me + k) % n}, device_id_type=MESH)
        pl.semaphore_signal(barrier, inc=1, device_id={"dp": other_row}, device_id_type=MESH)
        pl.semaphore_wait(barrier, n)
    else:
        for peer in (*neighbour, twin):
            pl.semaphore_signal(barrier, inc=1, device_id={"fsdp": peer}, device_id_type=MESH)
        pl.semaphore_signal(barrier, inc=1, device_id={"dp": other_row}, device_id_type=MESH)
        pl.semaphore_wait(barrier, 4)

    sent = []

    def send(src, dst, send_sem, recv_sem, target):
        copy = pltpu.make_async_remote_copy(
            src_ref=src, dst_ref=dst, send_sem=send_sem, recv_sem=recv_sem,
            device_id=target, device_id_type=MESH,
        )
        copy.start()
        sent.append(copy)

    def arrived(dst, recv_sem, send_sem):
        pltpu.make_async_remote_copy(
            src_ref=dst, dst_ref=dst, send_sem=send_sem, recv_sem=recv_sem,
            device_id={"fsdp": twin}, device_id_type=MESH,
        ).wait_recv()

    hops = ((half, half - 1), (half - 1, half))

    def ring(src, origin, way, seg, step):
        send(
            src, out.at[origin, segments[seg]], ring_send.at[way, seg, step],
            ring_recv.at[way, seg, step], {"fsdp": neighbour[way]},
        )

    for seg in range(2):
        for way in range(2):
            if hops[way][seg] >= 1:
                ring(block.at[segments[seg]], me, way, seg, 0)
    send(block, out.at[me], core_send.at[0, 0, 2], core_recv.at[0, 0, 2], {"fsdp": twin})
    if scatter:
        for k in range(1, n):
            to = (me + k) % n
            send(parts.at[to], mine.at[me], part_send.at[k], part_recv.at[k], {"fsdp": to})
    keep = pltpu.make_async_copy(block, out.at[me], sems.at[0])
    keep.start()
    if scatter:
        keep_part = pltpu.make_async_copy(parts.at[me], mine.at[me], sems.at[1])
        keep_part.start()

    def origin_of(way, step):
        return device_at(place - step if way == 0 else place + step)

    def to_twin(origin, rows, way, step, kind):
        send(
            out.at[origin, rows], out.at[origin, rows], core_send.at[way, step, kind],
            core_recv.at[way, step, kind], {"fsdp": twin},
        )

    def from_row(way, step):
        origin = origin_of(way, step)
        arrived(out.at[origin, others], row_recv.at[way, step], row_send.at[way, step])
        to_twin(origin, others, way, step, 2)

    for step in range(1, half + 1):
        for seg in range(2):
            for way in range(2):
                if step <= hops[way][seg]:
                    origin = origin_of(way, step)
                    rows = segments[seg]
                    view = out.at[origin, rows]
                    arrived(view, ring_recv.at[way, seg, step - 1], ring_send.at[way, seg, step - 1])
                    if step < hops[way][seg]:
                        ring(view, origin, way, seg, step)
                    if seg == 0:
                        send(
                            view, view, row_send.at[way, step], row_recv.at[way, step],
                            {"dp": other_row},
                        )
                    to_twin(origin, rows, way, step, seg)
        for way in range(2):
            if 1 <= step - 1 <= hops[way][0]:
                from_row(way, step - 1)
    for way in range(2):
        if 1 <= half <= hops[way][0]:
            from_row(way, half)

    arrived(out.at[twin], core_recv.at[0, 0, 2], core_send.at[0, 0, 2])
    for way in range(2):
        for step in range(1, half + 1):
            there = origin_of(way, step)
            origin = there + 1 - 2 * core
            for seg in range(2):
                if step <= hops[way][seg]:
                    arrived(
                        out.at[origin, segments[seg]], core_recv.at[way, step, seg],
                        core_send.at[way, step, seg],
                    )
            if step <= hops[way][0]:
                arrived(out.at[origin, others], core_recv.at[way, step, 2], core_send.at[way, step, 2])
    if scatter:
        for k in range(1, n):
            arrived(mine.at[(me + n - k) % n], part_recv.at[k], part_send.at[k])
        keep_part.wait()
    keep.wait()
    for copy in sent:
        copy.wait_send()


def ring_gather(block, collective_id, parts=None):
    n = lax.axis_size("fsdp")
    half = n // 4
    rows, width = block.shape
    third = (rows // 16 + 2) // 3 * 16
    scatter = parts is not None
    out_shape = [jax.ShapeDtypeStruct((n, rows, width), block.dtype)]
    any_spec = pl.BlockSpec(memory_space=pl.ANY)
    dma = pltpu.SemaphoreType.DMA
    scratch = [
        dma((2,)),
        dma((2, 2, half + 1)), dma((2, 2, half + 1)),
        dma((2, half + 1)), dma((2, half + 1)),
        dma((2, half + 1, 3)), dma((2, half + 1, 3)),
    ]
    operands = [block]
    if scatter:
        out_shape.append(jax.ShapeDtypeStruct(parts.shape, parts.dtype))
        scratch += [dma((n,)), dma((n,))]
        operands.append(parts)
    return pl.pallas_call(
        functools.partial(ring_kernel, scatter, third),
        out_shape=out_shape,
        in_specs=[pl.BlockSpec(memory_space=pltpu.VMEM)] * len(operands),
        out_specs=[any_spec] * len(out_shape),
        scratch_shapes=scratch,
        compiler_params=pltpu.CompilerParams(
            collective_id=collective_id, has_side_effects=True, vmem_limit_bytes=24 * 2**20
        ),
    )(*operands)


def row_sum_kernel(rows, share, out, landed, send_sems, recv_sems):
    me = lax.axis_index("dp")
    barrier = pltpu.get_barrier_semaphore()
    for k in range(1, rows):
        pl.semaphore_signal(barrier, inc=1, device_id={"dp": (me + k) % rows}, device_id_type=MESH)
    pl.semaphore_wait(barrier, rows - 1)
    copies = []
    for k in range(1, rows):
        copy = pltpu.make_async_remote_copy(
            src_ref=share, dst_ref=landed.at[me], send_sem=send_sems.at[k],
            recv_sem=recv_sems.at[k], device_id={"dp": (me + k) % rows}, device_id_type=MESH,
        )
        copy.start()
        copies.append(copy)
    keep = pltpu.make_async_copy(share, landed.at[me], send_sems.at[0])
    keep.start()
    for k in range(1, rows):
        pltpu.make_async_remote_copy(
            src_ref=share, dst_ref=landed.at[(me + rows - k) % rows], send_sem=send_sems.at[k],
            recv_sem=recv_sems.at[k], device_id={"dp": (me + k) % rows}, device_id_type=MESH,
        ).wait_recv()
    keep.wait()
    for copy in copies:
        copy.wait_send()
    total = landed[0]
    for k in range(1, rows):
        total = total + landed[k]
    out[...] = total


def sum_over_rows(share):
    rows = lax.axis_size("dp")
    vmem = pl.BlockSpec(memory_space=pltpu.VMEM)
    return pl.pallas_call(
        functools.partial(row_sum_kernel, rows),
        out_shape=jax.ShapeDtypeStruct(share.shape, share.dtype),
        in_specs=[vmem],
        out_specs=vmem,
        scratch_shapes=[
            pltpu.VMEM((rows, *share.shape), share.dtype),
            pltpu.SemaphoreType.DMA((rows,)),
            pltpu.SemaphoreType.DMA((rows,)),
        ],
        compiler_params=pltpu.CompilerParams(
            collective_id=2, has_side_effects=True, vmem_limit_bytes=16 * 2**20
        ),
    )(share)


def general_per_device(
    queries,
    keys,
    values,
    lengths,
    normalized_weight,
    block_scale_codes,
    scale_group_factor,
    scale_group_offset,
    adapter_down_weight,
    adapter_up_weight,
    cotangent,
):
    n = lax.axis_size("fsdp")
    row_index = lax.axis_index("dp")
    rank, down_width = adapter_down_weight.shape
    up_width = adapter_up_weight.shape[1]
    own_rows = down_width + up_width
    packed_rows = own_rows * rank // 128
    padded_rows = -(-packed_rows // 16) * 16

    def pack(x):
        x = x.reshape(*x.shape[:-2], packed_rows, 128)
        pad = [(0, 0)] * (x.ndim - 2) + [(0, padded_rows - packed_rows), (0, 0)]
        return jnp.pad(x, pad)

    def unpack(x):
        return x[..., :packed_rows, :].reshape(*x.shape[:-2], own_rows, rank)

    own_lengths = lax.dynamic_index_in_dim(lengths[0], row_index, 0, keepdims=False)
    own_adapters = jnp.concatenate([adapter_up_weight.T, adapter_down_weight.T], axis=0)
    (adapters,) = ring_gather(pack(own_adapters), 0)
    adapters = unpack(adapters)
    up_rows = adapters[:, :up_width].reshape(n * up_width, rank)
    down_rows = adapters[:, up_width:].reshape(n * down_width, rank)

    attention_output = attend(queries, keys, values, own_lengths)
    reduced_activation = jnp.dot(
        attention_output, down_rows, preferred_element_type=jnp.float32
    ).astype(jnp.bfloat16)
    reduced_gradient = (
        adapter_scale * jnp.dot(cotangent, up_rows, preferred_element_type=jnp.float32)
    ).astype(jnp.bfloat16)
    down_part = jnp.dot(attention_output.T, reduced_gradient, preferred_element_type=jnp.float32)
    up_part = adapter_scale * jnp.dot(
        cotangent.T, reduced_activation, preferred_element_type=jnp.float32
    )
    parts = jnp.concatenate(
        [up_part.reshape(n, up_width, rank), down_part.reshape(n, down_width, rank)], axis=1
    ).astype(jnp.bfloat16)

    local_base = dequantize(
        normalized_weight, block_scale_codes, scale_group_factor, scale_group_offset
    )
    gathered, shares = ring_gather(local_base, 1, pack(parts))
    base_rows = gathered.reshape(-1, gathered.shape[2])
    share = unpack(sum_over_rows(jnp.sum(shares.astype(jnp.float32), axis=0)))

    product = lax.dot_general(
        attention_output, base_rows, (((1,), (1,)), ((), ())), preferred_element_type=jnp.float32
    )
    projection_output = (
        product
        + adapter_scale
        * lax.dot_general(
            reduced_activation, up_rows, (((1,), (1,)), ((), ())),
            preferred_element_type=jnp.float32,
        )
    ).astype(jnp.bfloat16)
    attention_gradient = (
        jnp.dot(cotangent, base_rows, preferred_element_type=jnp.float32)
        + lax.dot_general(
            reduced_gradient, down_rows, (((1,), (1,)), ((), ())),
            preferred_element_type=jnp.float32,
        )
    ).astype(jnp.bfloat16)
    return (projection_output, attention_gradient, share[up_width:].T, share[:up_width].T)


LANES = 128
TILE = 256
A, RA, RB, AD, Y = range(5)


def dot(a, b, contract):
    return lax.dot_general(
        a, b, ((contract[:1], contract[1:]), ((), ())), preferred_element_type=jnp.float32
    )


def down_window(down_width):
    step = 2 * down_width // LANES * LANES
    return 4 * down_width - step, step


def fused_kernel(
    lengths, weight_hbm, codes_hbm, factor_hbm, offset_hbm, down_hbm, up_hbm, queries, keys,
    values, cotangent_hbm,
    projection_output, attention_gradient, up_out, down_out,
    base, packed, adapters, down_rows, weight, codes, factor, offset, down, up, q, k, v, cot, attended, bias, mixed, low_rank,
    low_grad, product, gradient, part, part_twin, part_row, landed_row, part_chip,
    landed_side, part_line, landed_line,
    final, local_sem, ring_send, ring_recv, row_send, row_recv, twin_send, twin_recv, sum_send,
    sum_recv,
):
    n = lax.axis_size("fsdp")
    chips = n // 2
    half = chips // 2
    row = lax.axis_index("dp")
    me = lax.axis_index("fsdp")
    chip, core = me // 2, me % 2
    tokens, features = attended.shape
    model = cot.shape[1]
    rank, width = up.shape
    down_width = down.shape[1]
    pair = 2 * width
    quad = 4 * down_width
    window, window_step = down_window(down_width)
    block = pair + window
    tiles = features // TILE
    a_tiles = 3 * tiles // 10
    r_tiles = (tiles - 2 * a_tiles) // 2
    place = jnp.where(chip % 2 == 0, chip // 2, chips - 1 - chip // 2)
    twin = 2 * chip + 1 - core
    other_row = 1 - row
    sense = 1 - 2 * core

    def chip_at(where):
        where = (where + 2 * chips) % chips
        return jnp.where(where < half, 2 * where, 2 * (chips - 1 - where) + 1)

    def behind(step):
        return chip_at(place - sense * step)

    def ahead(step):
        return chip_at(place + sense * step)

    barrier = pltpu.get_barrier_semaphore()
    peers = (
        {"fsdp": 2 * ahead(1) + core}, {"fsdp": 2 * behind(1) + core}, {"fsdp": twin},
        {"dp": other_row},
    )
    for peer in peers:
        pl.semaphore_signal(barrier, inc=1, device_id=peer, device_id_type=MESH)

    loads = [
        pltpu.make_async_copy(src, dst, local_sem.at[i])
        for i, (src, dst) in enumerate(
            (
                (codes_hbm, codes), (factor_hbm, factor), (offset_hbm, offset),
                (weight_hbm, weight), (up_hbm, up), (down_hbm, down), (queries, q), (keys, k),
                (values, v), (cotangent_hbm, cot),
            )
        )
    ]
    for load in loads:
        load.start()

    sent = []

    def send(src, dst, send_sem, recv_sem, target):
        copy = pltpu.make_async_remote_copy(
            src_ref=src, dst_ref=dst, send_sem=send_sem, recv_sem=recv_sem,
            device_id=target, device_id_type=MESH,
        )
        copy.start()
        sent.append(copy)

    def arrived(dst, send_sem, recv_sem):
        pltpu.make_async_remote_copy(
            src_ref=dst, dst_ref=dst, send_sem=send_sem, recv_sem=recv_sem,
            device_id={"fsdp": twin}, device_id_type=MESH,
        ).wait_recv()

    def rows_of(origin):
        return pl.ds(pl.multiple_of(origin * width, 64), width)

    packed_width = (width + down_width) // 2

    def packed_rows_of(origin):
        return pl.ds(pl.multiple_of(origin * packed_width, 16), packed_width)

    def tiles_of(kind):
        if kind == A:
            return row * a_tiles, a_tiles
        if kind == Y:
            return (1 - row) * a_tiles, a_tiles
        if kind == RA:
            return 2 * a_tiles, r_tiles
        return 2 * a_tiles + r_tiles, tiles - 2 * a_tiles - r_tiles

    def piece(origin, kind):
        if kind == AD:
            return packed.at[packed_rows_of(origin)]
        first, count = tiles_of(kind)
        return base.at[rows_of(origin), pl.ds(pl.multiple_of(first * TILE, TILE), count * TILE)]

    def shard(origin_chip, side):
        return 2 * origin_chip + (core if side == 0 else 1 - core)

    def ring(step, kind, sides=(0, 1)):
        far = (ahead if kind == AD else behind)(step - 1)
        to = (behind if kind == AD else ahead)(1)
        for side in sides:
            view = piece(shard(far, side), kind)
            send(
                view, view, ring_send.at[step, kind, side], ring_recv.at[step, kind, side],
                {"fsdp": 2 * to + core},
            )

    def to_twin(view, step, kind, side):
        send(
            view, view, twin_send.at[step, kind, side], twin_recv.at[step, kind, side],
            {"fsdp": twin},
        )

    def ring_in(step, kind, sides=(0, 1)):
        for side in sides:
            view = piece(shard((ahead if kind == AD else behind)(step), side), kind)
            arrived(view, ring_send.at[step, kind, side], ring_recv.at[step, kind, side])
            to_twin(view, step, kind, side)
            if kind == A:
                send(
                    view, view, row_send.at[step, side], row_recv.at[step, side],
                    {"dp": other_row},
                )

    def row_in(step, sides=(0, 1)):
        for side in sides:
            view = piece(shard(behind(step), side), Y)
            arrived(view, row_send.at[step, side], row_recv.at[step, side])
            to_twin(view, step, Y, side)

    def twin_in(step, *kinds, sides=(0, 1)):
        for kind in kinds:
            for side in sides:
                far = (behind if kind == AD else ahead)(step) if step else chip
                arrived(
                    piece(shard(far, 1 - side), kind), twin_send.at[step, kind, side],
                    twin_recv.at[step, kind, side],
                )

    own_rows = rows_of(me)
    groups = factor.shape[0]
    span = SCALE_GROUP * QBLOCK
    shape = (3 * SCALE_GROUP, span)
    spread = (
        lax.broadcasted_iota(jnp.int32, shape, 0) % SCALE_GROUP
        == lax.broadcasted_iota(jnp.int32, shape, 1) // QBLOCK
    ).astype(jnp.bfloat16)

    def dequantize_group(g):
        eight = pl.ds(pl.multiple_of(SCALE_GROUP * g, SCALE_GROUP), SCALE_GROUP)
        absmax = (
            factor[pl.ds(g, 1), :] * (codes[eight, :].astype(jnp.float32) + 1.0) / 256.0
            + offset[pl.ds(g, 1), :]
        )
        high = absmax.astype(jnp.bfloat16).astype(jnp.float32)
        middle = (absmax - high).astype(jnp.bfloat16).astype(jnp.float32)
        parts = jnp.concatenate([high, middle, absmax - high - middle], axis=0)
        columns = pl.ds(pl.multiple_of(span * g, span), span)
        base[own_rows, columns] = (
            weight[:, columns].astype(jnp.float32)
            * dot(parts.astype(jnp.bfloat16), spread, (0, 0))
        ).astype(base.dtype)

    for load in loads[:4]:
        load.wait()
    ahead_groups = -(-a_tiles * TILE // span)
    for i in range(ahead_groups):
        dequantize_group(row * (a_tiles * TILE // span) + i)
    pl.semaphore_wait(barrier, len(peers))
    ring(1, A, (0,))
    to_twin(piece(me, A), 0, A, 0)
    def picked(columns, shift):
        shape = (packed_width, columns)
        return (
            lax.broadcasted_iota(jnp.int32, shape, 0) + shift
            == lax.broadcasted_iota(jnp.int32, shape, 1)
        ).astype(jnp.bfloat16)

    for load in loads[4:6]:
        load.wait()
    up_low = jnp.concatenate([up[...], jnp.zeros((LANES - rank, width), up.dtype)], axis=0)
    up_high = jnp.concatenate([jnp.zeros((LANES - rank, width), up.dtype), up[...]], axis=0)
    down_high = jnp.concatenate(
        [jnp.zeros((LANES - rank, down_width), down.dtype), down[...]], axis=0
    )
    left = width - packed_width
    own_ad = packed.at[packed_rows_of(me)]
    own_ad[...] = (
        dot(picked(width, 0), up_low, (1, 1))
        + dot(picked(width, packed_width), up_high, (1, 1))
        + dot(picked(down_width, -left), down_high, (1, 1))
    ).astype(packed.dtype)
    ring(1, AD, (0,))
    to_twin(own_ad, 0, AD, 0)

    for i in range(groups - ahead_groups):
        lead = row * (a_tiles * TILE // span)
        dequantize_group(jnp.where(i < lead, i, i + ahead_groups))
    for kind in (RA, RB, Y):
        to_twin(piece(me, kind), 0, kind, 0)
    twin_in(0, A, sides=(0,))
    ring(1, A, (1,))
    ring(1, RA, (0,))

    ends = []
    for j in range(lengths.shape[2]):
        ends.append(lengths[0, row, j] + (ends[-1] if ends else 0))
    at = lax.broadcasted_iota(jnp.int32, (tokens, tokens), 0)
    to = lax.broadcasted_iota(jnp.int32, (tokens, tokens), 1)
    segment_at = sum((at >= end).astype(jnp.int32) for end in ends)
    segment_to = sum((to >= end).astype(jnp.int32) for end in ends)
    bias[...] = jnp.where((segment_at == segment_to) & (to <= at), 0.0, -jnp.inf)
    for load in loads[6:9]:
        load.wait()

    head_count = features // HEAD_SIZE
    per_loop = 2

    def heads(first, count):
        @pl.loop(first // per_loop, (first + count) // per_loop)
        def _(i):
            for j in range(per_loop):
                columns = pl.ds(
                    pl.multiple_of((i * per_loop + j) * HEAD_SIZE, HEAD_SIZE), HEAD_SIZE
                )
                scores = dot(q[:, columns], k[:, columns], (1, 1)) * HEAD_SIZE ** (-0.5)
                scores = scores + bias[...]
                weights = jnp.exp(scores - jnp.max(scores, axis=-1, keepdims=True))
                total = jnp.sum(weights, axis=-1, keepdims=True)
                summed = dot(weights.astype(jnp.bfloat16), v[:, columns], (1, 0))
                attended[:, columns] = (summed / total).astype(attended.dtype)

    def accumulate(there, *kinds):
        columns = pl.ds(pl.multiple_of(there * pair, LANES), pair)
        for first, count in kinds:
            @pl.loop(first, first + count)
            def _(i):
                some = pl.ds(pl.multiple_of(i * TILE, TILE), TILE)
                rows = base[columns, some]
                gradient[:, some] += dot(cot[:, columns], rows, (1, 0))
                product[:, columns] += dot(attended[:, some], rows, (1, 1))

    share = head_count // 10 * 2
    arrived(packed.at[packed_rows_of(twin)], twin_send.at[0, AD, 0], twin_recv.at[0, AD, 0])
    ring(1, AD, (1,))
    twin_in(0, RA, RB, Y, sides=(0,))
    ring(1, RA, (1,))
    heads(0, share)
    ring_in(1, AD)
    ring(2, AD)
    heads(share, share)
    ring_in(1, A)
    ring(2, A)
    ring(1, RB)
    ring_in(2, AD)
    ring(3, AD)
    heads(2 * share, share)
    ring_in(3, AD)
    ring(4, AD, (0,))
    heads(3 * share, head_count - 3 * share)
    ring_in(1, RA)
    ring_in(4, AD, (0,))
    for step in range(1, half):
        twin_in(step, AD)
    twin_in(half, AD, sides=(0,))
    loads[9].wait()

    @pl.loop(0, n)
    def _(f):
        both = packed[packed_rows_of(f), :]
        start = f * width
        adapters[pl.ds(pl.multiple_of(start, 16), packed_width), :] = both
        adapters[pl.ds(pl.multiple_of(start + packed_width, 16), left), :] = pltpu.roll(
            both[:left].astype(jnp.float32), rank, 1
        ).astype(adapters.dtype)
        down_rows[pl.ds(pl.multiple_of(f * down_width, 16), down_width), :] = both[left:]

    lane = lax.broadcasted_iota(jnp.int32, (tokens, LANES), 1)
    activation = dot(attended[...], down_rows[...], (1, 0))
    grads = adapter_scale * dot(cot[...], adapters[...], (1, 0))
    both = jnp.where(lane < rank, pltpu.roll(activation, rank, 1), pltpu.roll(grads, rank, 1))
    both = both.astype(jnp.bfloat16)
    mixed[...] = both
    nothing = jnp.zeros_like(both)
    low_rank[...] = jnp.where(lane < rank, both * jnp.bfloat16(adapter_scale), nothing)
    low_grad[...] = jnp.where(lane < rank, nothing, both)
    chunk = pair

    @pl.loop(0, model // chunk)
    def _(i):
        columns = pl.ds(pl.multiple_of(i * chunk, LANES), chunk)
        both = mixed[...]
        part[:, columns] = (
            adapter_scale * dot(both, cot[:, columns], (0, 0))[:rank]
        ).astype(part.dtype)

    @pl.loop(0, features // chunk)
    def _(i):
        columns = pl.ds(pl.multiple_of(i * chunk, LANES), chunk)
        there = pl.ds(pl.multiple_of(model + i * chunk, LANES), chunk)
        both = mixed[...]
        part[:, there] = dot(both, attended[:, columns], (0, 0))[rank:].astype(part.dtype)

    per_core = rank // 2
    per_row = per_core // 2
    theirs = pl.ds(pl.multiple_of((1 - core) * per_core, per_core), per_core)
    send(part.at[theirs], part_twin, sum_send.at[0], sum_recv.at[0], {"fsdp": twin})

    ring_in(2, A)
    ring(3, A)
    ring(2, RA)
    row_in(1)

    @pl.loop(0, model // pair)
    def _(i):
        columns = pl.ds(pl.multiple_of(i * pair, LANES), pair)
        product[:, columns] = dot(low_rank[...], adapters[columns, :], (1, 1))

    @pl.loop(0, tiles)
    def _(i):
        some = pl.ds(pl.multiple_of(i * TILE, TILE), TILE)
        gradient[:, some] = dot(low_grad[...], down_rows[some, :], (1, 1))

    arrived(part_twin, sum_send.at[0], sum_recv.at[0])
    away = pl.ds(pl.multiple_of(core * per_core + (1 - row) * per_row, per_row), per_row)
    away_twin = pl.ds(pl.multiple_of((1 - row) * per_row, per_row), per_row)
    kept = pl.ds(pl.multiple_of(core * per_core + row * per_row, per_row), per_row)
    kept_twin = pl.ds(pl.multiple_of(row * per_row, per_row), per_row)

    @pl.loop(0, (model + features) // chunk)
    def _(i):
        columns = pl.ds(pl.multiple_of(i * chunk, LANES), chunk)
        part_row[:, columns] = (
            part[away, columns].astype(jnp.float32)
            + part_twin[away_twin, columns].astype(jnp.float32)
        ).astype(part_row.dtype)

    send(part_row, landed_row, sum_send.at[1], sum_recv.at[1], {"dp": other_row})

    accumulate(chip, (0, tiles))
    ring_in(1, RB)
    accumulate(behind(1), (0, tiles))
    twin_in(1, A, RA, RB, Y)
    accumulate(ahead(1), (0, tiles))

    ring_in(3, A)
    ring(4, A, (0,))
    ring(2, RB)
    ring_in(2, RA)
    ring(3, RA)

    arrived(landed_row, sum_send.at[1], sum_recv.at[1])

    def row_sum(columns):
        return (
            part[kept, columns].astype(jnp.float32)
            + part_twin[kept_twin, columns].astype(jnp.float32)
            + landed_row[:, columns].astype(jnp.float32)
        ).astype(part_chip.dtype)

    side, line = chip % 2, chip // 2

    @pl.loop(0, chips)
    def _(i):
        part_chip[i % 2, i // 2, :, :pair] = row_sum(
            pl.ds(pl.multiple_of(i * pair, LANES), pair)
        )
        part_chip[i % 2, i // 2, :, pair:] = row_sum(
            pl.ds(
                pl.multiple_of(model + i // 2 * quad + i % 2 * window_step, LANES), window
            )
        )

    beside = 2 * (2 * line + 1 - side) + core
    send(part_chip.at[1 - side], landed_side, sum_send.at[2], sum_recv.at[2], {"fsdp": beside})

    row_in(2)
    most = (0, 2 * a_tiles + r_tiles)
    accumulate(behind(2), most)
    twin_in(2, A, RA, Y)
    accumulate(ahead(2), most)
    ring_in(4, A, (0,))

    ring_in(2, RB)
    ring(3, RB)

    arrived(landed_side, sum_send.at[2], sum_recv.at[2])

    @pl.loop(0, half)
    def _(i):
        part_line[i] = (
            part_chip[side, i].astype(jnp.float32) + landed_side[i].astype(jnp.float32)
        ).astype(part_line.dtype)

    for d in range(1, half):
        there = (line + d) % half
        send(
            part_line.at[there], landed_line.at[d], sum_send.at[2 + d], sum_recv.at[2 + d],
            {"fsdp": 2 * (2 * there + side) + core},
        )

    accumulate(behind(2), tiles_of(RB))
    twin_in(2, RB)
    accumulate(ahead(2), tiles_of(RB))
    accumulate(behind(3), tiles_of(A))
    twin_in(3, A)
    accumulate(ahead(3), tiles_of(A))
    twin_in(4, A, sides=(0,))
    accumulate(behind(4), tiles_of(A))
    ring_in(3, RA)
    ring(4, RA, (0,))
    accumulate(behind(3), tiles_of(RA))
    twin_in(3, RA)
    accumulate(ahead(3), tiles_of(RA))

    def project(there):
        columns = pl.ds(pl.multiple_of(there * pair, LANES), pair)
        projection_output[:, columns] = product[:, columns].astype(projection_output.dtype)

    @pl.loop(0, chips - 3)
    def _(i):
        project(chip_at(place + 2 - i))

    ring_in(3, RB)
    ring(4, RB, (0,))
    accumulate(behind(3), tiles_of(RB))
    row_in(3)
    accumulate(behind(3), tiles_of(Y))

    total = part_chip[side, line].astype(jnp.float32) + landed_side[line].astype(jnp.float32)
    for d in range(1, half):
        arrived(landed_line.at[d], sum_send.at[2 + d], sum_recv.at[2 + d])
        total = total + landed_line[d].astype(jnp.float32)
    own = 2 * core + row
    final[own] = total
    targets = ({"fsdp": twin}, {"dp": other_row}, {"dp": other_row, "fsdp": twin})
    for i, target in enumerate(targets):
        send(
            final.at[own], final.at[own], sum_send.at[2 + half + i],
            sum_recv.at[2 + half + i], target,
        )

    twin_in(3, RB, Y)
    accumulate(ahead(3), tiles_of(RB), tiles_of(Y))
    project(behind(3))
    project(ahead(3))
    row_in(4, (0,))
    ring_in(4, RA, (0,))
    twin_in(4, Y, RA, sides=(0,))
    accumulate(behind(4), tiles_of(Y), tiles_of(RA))

    first, count = tiles_of(RB)

    def convert(i):
        some = pl.ds(pl.multiple_of(i * TILE, TILE), TILE)
        attention_gradient[:, some] = gradient[:, some].astype(attention_gradient.dtype)

    pl.loop(0, first)(convert)
    ring_in(4, RB, (0,))
    twin_in(4, RB, sides=(0,))
    accumulate(behind(4), tiles_of(RB))
    project(behind(half))
    pl.loop(first, first + count)(convert)
    owners = (2 * (1 - core) + row, 2 * core + 1 - row, 2 * (1 - core) + 1 - row)
    for i, owner in enumerate(owners):
        arrived(final.at[owner], sum_send.at[2 + half + i], sum_recv.at[2 + half + i])
    ranks = final[...].reshape(rank, block)
    up_cols, down_cols = ranks[:, :pair], ranks[:, pair:]
    up_cols = jnp.where(core == 0, up_cols, pltpu.roll(up_cols, pair - width, 1))
    up_out[...] = up_cols[:, :width]
    turned = down_cols
    for j in range(1, 4):
        first = j * down_width - j // 2 * window_step
        turned = jnp.where(me % 4 == j, pltpu.roll(down_cols, window - first, 1), turned)
    down_out[...] = turned[:, :down_width]
    for copy in sent:
        copy.wait_send()


def finish_kernel(count, *refs):
    copies = []
    for i in range(count):
        rows = refs[i].shape[0]
        cuts = 4 if i < 2 else 1
        for j in range(cuts):
            some = pl.ds(rows // cuts * j, rows // cuts)
            copies.append(
                pltpu.make_async_copy(
                    refs[i].at[some], refs[count + i].at[some], refs[-1].at[len(copies)]
                )
            )
    for copy in copies:
        copy.start()
    for copy in copies:
        copy.wait()


def finish(*results):
    return pl.pallas_call(
        functools.partial(finish_kernel, len(results)),
        out_shape=[jax.ShapeDtypeStruct(x.shape, x.dtype) for x in results],
        in_specs=[pl.BlockSpec(memory_space=pltpu.VMEM)] * len(results),
        out_specs=[pl.BlockSpec(memory_space=pl.ANY)] * len(results),
        scratch_shapes=[pltpu.SemaphoreType.DMA((12,))],
        compiler_params=pltpu.CompilerParams(vmem_limit_bytes=8 * 2**20),
    )(*results)


def fused_per_device(
    queries,
    keys,
    values,
    lengths,
    normalized_weight,
    block_scale_codes,
    scale_group_factor,
    scale_group_offset,
    adapter_down_weight,
    adapter_up_weight,
    cotangent,
):
    n = lax.axis_size("fsdp")
    chips = n // 2
    half = chips // 2
    tokens, features = queries.shape
    model = cotangent.shape[1]
    rank, width = adapter_up_weight.shape
    down_width = adapter_down_weight.shape[1]
    block = 2 * width + down_window(down_width)[0]
    low, full = jnp.bfloat16, jnp.float32
    dma = pltpu.SemaphoreType.DMA
    hbm = pl.BlockSpec(memory_space=pl.ANY)
    shapes = lambda *s: pltpu.VMEM(s[:-1], s[-1])
    sums = 2 + half + 4
    return tuple(
        pl.pallas_call(
            fused_kernel,
            out_shape=[
                shapes(tokens, model, low),
                shapes(tokens, features, low),
                shapes(rank, width, full),
                shapes(rank, down_width, full),
            ],
            in_specs=[pl.BlockSpec(memory_space=pltpu.SMEM)] + [hbm] * 10,
            out_specs=[pl.BlockSpec(memory_space=pltpu.VMEM)] * 4,
            scratch_shapes=[
                shapes(n * width, features, low),
                shapes(n * (width + down_width) // 2, LANES, low),
                shapes(n * width, LANES, low),
                shapes(features, LANES, low),
                shapes(width, features, low),
                shapes(features // QBLOCK, width, jnp.int32),
                shapes(features // (QBLOCK * SCALE_GROUP), width, full),
                shapes(features // (QBLOCK * SCALE_GROUP), width, full),
                shapes(rank, down_width, low),
                shapes(rank, width, low),
                shapes(tokens, features, low),
                shapes(tokens, features, low),
                shapes(tokens, features, low),
                shapes(tokens, model, low),
                shapes(tokens, features, low),
                shapes(tokens, tokens, full),
                shapes(tokens, LANES, low),
                shapes(tokens, LANES, low),
                shapes(tokens, LANES, low),
                shapes(tokens, model, full),
                shapes(tokens, features, full),
                shapes(rank, model + features, low),
                shapes(rank // 2, model + features, low),
                shapes(rank // 4, model + features, low),
                shapes(rank // 4, model + features, low),
                shapes(2, half, rank // 4, block, low),
                shapes(half, rank // 4, block, low),
                shapes(half, rank // 4, block, low),
                shapes(half, rank // 4, block, low),
                shapes(4, rank // 4, block, full),
                dma((10,)),
                dma((half + 1, 4, 2)),
                dma((half + 1, 4, 2)),
                dma((half + 1, 2)),
                dma((half + 1, 2)),
                dma((half + 1, 5, 2)),
                dma((half + 1, 5, 2)),
                dma((sums,)),
                dma((sums,)),
            ],
            compiler_params=pltpu.CompilerParams(
                collective_id=3, has_side_effects=True, vmem_limit_bytes=60 * 2**20
            ),
        )(
            lengths, normalized_weight.T, block_scale_codes, scale_group_factor,
            scale_group_offset, adapter_down_weight, adapter_up_weight, queries, keys, values,
            cotangent,
        )
    )


def per_device(*operands):
    projection_output, attention_gradient, up_gradient, down_gradient = finish(
        *fused_per_device(*operands)
    )
    return projection_output, attention_gradient, down_gradient, up_gradient


def fused_fits(mesh):
    return mesh.shape["dp"] == 2 and mesh.shape["fsdp"] == 16


def solution(mesh):
    return jax.shard_map(
        per_device if fused_fits(mesh) else general_per_device,
        mesh=mesh,
        in_specs=(
            P(("dp", "fsdp"), None),
            P(("dp", "fsdp"), None),
            P(("dp", "fsdp"), None),
            P("fsdp", None, None),
            P(None, "fsdp"),
            P(None, "fsdp"),
            P(None, "fsdp"),
            P(None, "fsdp"),
            P(None, "fsdp"),
            P(None, "fsdp"),
            P(("dp", "fsdp"), None),
        ),
        out_specs=(
            P(("dp", "fsdp"), None),
            P(("dp", "fsdp"), None),
            P(None, "fsdp"),
            P(None, "fsdp"),
        ),
        check_vma=False,
    )
```
